32 devices in a mesh: dp: 1 (over z), kv: 32 (over y, x, core).
Axes of the slice: x: 4, y: 4, z: 1, core: 2. Of those that a mesh axis runs over, the one named last changes fastest.
The devices are a block of a 4x4x8 slice.
Arguments:
- x_first: bfloat16 [16, 4096], P('dp')
- next_emb: bfloat16 [2, 16, 4096], P(None, 'dp')
- k_cache: bfloat16 [16, 8192, 8, 128], P('dp', 'kv')
- v_cache: bfloat16 [16, 8192, 8, 128], P('dp', 'kv')
- seq_len: int32 [16], P('dp')
- ln1_gain: float32 [4096], replicated
- ln1_bias: float32 [4096], replicated
- w_q: bfloat16 [4096, 4096], replicated
- b_q: float32 [4096], replicated
- w_k: bfloat16 [4096, 1024], replicated
- b_k: float32 [1024], replicated
- w_v: bfloat16 [4096, 1024], replicated
- b_v: float32 [1024], replicated
- w_o: bfloat16 [4096, 4096], replicated
- b_o: float32 [4096], replicated
- ln2_gain: float32 [4096], replicated
- ln2_bias: float32 [4096], replicated
- w_router: bfloat16 [4096, 16], replicated
- w_gate: bfloat16 [16, 4096, 960], P(None, None, 'kv')
- w_up: bfloat16 [16, 4096, 960], P(None, None, 'kv')
- w_down: bfloat16 [16, 960, 4096], P(None, 'kv')
- long_factor: float32 [64], replicated
- expert_idx: int32 [3, 16, 2], P(None, 'dp')
- route_mask: int32 [3, 16, 2, 16], P(None, 'dp')
Outputs:
- output 1: bfloat16 [3, 16, 4096], P(None, 'dp')
- output 2: bfloat16 [16, 3, 8, 128], P('dp')
- output 3: bfloat16 [16, 3, 8, 128], P('dp')
All inputs are finite; a program needn't handle non-finite values.
Results may differ from the reference program's by a relative error of at most 0.0117903.
Values sent between devices are 32-bit elements.
A program may use at most 768 MiB of HBM per device.

```python
import math
import jax
import jax.numpy as jnp
from jax import lax

BATCH_SIZE = 16
SHARD_LEN = 256
KV_GROUP = 32
CACHE_LEN = 8192
D_MODEL = 4096
Q_HEADS = 32
KV_HEADS = 8
HEAD_DIM = 128
NUM_EXPERTS = 16
TOP_K = 2
FF_DIM = 960
NUM_STEPS = 3
SEG_COUNT = 64

HALF_DIM = HEAD_DIM // 2
Q_GROUP = Q_HEADS // KV_HEADS
FF_SHARD = FF_DIM // KV_GROUP
ROPE_BASE = 10000.0
ROPE_MSCALE = math.sqrt(1.0 + math.log(32.0) / math.log(4096.0))
NORM_EPS = 1e-5
NEG_FILL = -1e30


def setup_inputs(seed: int = 0, part: int = 0) -> dict:
    base_key = jax.random.key(seed)
    shared_keys = jax.random.split(base_key, 17)
    part_keys = jax.random.split(jax.random.fold_in(base_key, part), 9)
    q_width = Q_HEADS * HEAD_DIM
    kv_width = KV_HEADS * HEAD_DIM
    d_scale = D_MODEL ** -0.5

    def normal(rand_key, arr_dims, factor):
        return jax.random.normal(rand_key, arr_dims, jnp.float32) * factor

    x_first = normal(part_keys[0], (BATCH_SIZE, D_MODEL), 1.0).astype(jnp.bfloat16)
    next_emb = normal(part_keys[1], (NUM_STEPS - 1, BATCH_SIZE, D_MODEL), 1.0).astype(jnp.bfloat16)
    seg_index = (jnp.arange(CACHE_LEN) * SEG_COUNT) // CACHE_LEN
    key_segs = normal(part_keys[2], (BATCH_SIZE, SEG_COUNT, KV_HEADS, HEAD_DIM), 1.0)
    value_segs = normal(part_keys[3], (BATCH_SIZE, SEG_COUNT, KV_HEADS, HEAD_DIM), 4.0)
    cache_dims = (BATCH_SIZE, CACHE_LEN, KV_HEADS, HEAD_DIM)
    k_cache = (normal(part_keys[4], cache_dims, 1.0) + key_segs[:, seg_index]).astype(jnp.bfloat16)
    v_cache = (normal(part_keys[5], cache_dims, 1.0) + value_segs[:, seg_index]).astype(jnp.bfloat16)
    drawn_lens = jax.random.randint(part_keys[6], (BATCH_SIZE,), CACHE_LEN // 4, CACHE_LEN + 1)
    seq_len = jnp.where(jnp.arange(BATCH_SIZE) == 0, CACHE_LEN, drawn_lens).astype(jnp.int32)
    rank_scores = jax.random.randint(part_keys[7], (NUM_STEPS, BATCH_SIZE, NUM_EXPERTS), 0, 1 << 20)
    expert_order = jnp.argsort(rank_scores * NUM_EXPERTS + jnp.arange(NUM_EXPERTS), axis=-1)
    expert_idx = expert_order[..., :TOP_K].astype(jnp.int32)
    chosen = (expert_idx[..., None] == jnp.arange(NUM_EXPERTS)).astype(jnp.int32)
    earlier = jnp.cumsum(chosen, axis=2) - chosen
    coin_flip = jax.random.randint(part_keys[8], (NUM_STEPS, BATCH_SIZE, TOP_K, NUM_EXPERTS), 0, 2)
    route_mask = jnp.where(chosen == 1, 1, jnp.where(earlier > 0, 0, coin_flip)).astype(jnp.int32)
    return {
        'x_first': x_first,
        'next_emb': next_emb,
        'k_cache': k_cache,
        'v_cache': v_cache,
        'seq_len': seq_len,
        'ln1_gain': 1.0 + normal(shared_keys[0], (D_MODEL,), 0.3),
        'ln1_bias': normal(shared_keys[1], (D_MODEL,), 0.3),
        'w_q': normal(shared_keys[2], (D_MODEL, q_width), d_scale).astype(jnp.bfloat16),
        'b_q': normal(shared_keys[3], (q_width,), 0.5),
        'w_k': normal(shared_keys[4], (D_MODEL, kv_width), d_scale).astype(jnp.bfloat16),
        'b_k': normal(shared_keys[5], (kv_width,), 0.5),
        'w_v': normal(shared_keys[6], (D_MODEL, kv_width), d_scale).astype(jnp.bfloat16),
        'b_v': normal(shared_keys[7], (kv_width,), 0.5),
        'w_o': normal(shared_keys[8], (q_width, D_MODEL), q_width ** -0.5).astype(jnp.bfloat16),
        'b_o': normal(shared_keys[9], (D_MODEL,), 0.3),
        'ln2_gain': 1.0 + normal(shared_keys[10], (D_MODEL,), 0.3),
        'ln2_bias': normal(shared_keys[11], (D_MODEL,), 0.3),
        'w_router': normal(shared_keys[12], (D_MODEL, NUM_EXPERTS), 1.5 * d_scale).astype(jnp.bfloat16),
        'w_gate': normal(shared_keys[13], (NUM_EXPERTS, D_MODEL, FF_DIM), d_scale).astype(jnp.bfloat16),
        'w_up': normal(shared_keys[14], (NUM_EXPERTS, D_MODEL, FF_DIM), d_scale).astype(jnp.bfloat16),
        'w_down': normal(shared_keys[15], (NUM_EXPERTS, FF_DIM, D_MODEL), FF_DIM ** -0.5).astype(jnp.bfloat16),
        'long_factor': jnp.exp(jax.random.uniform(shared_keys[16], (HALF_DIM,), jnp.float32, 0.0, 3.5)),
        'expert_idx': expert_idx,
        'route_mask': route_mask,
    }


def layer_norm(x_in, gain_vec, bias_vec):
    x_f32 = x_in.astype(jnp.float32)
    mean_val = jnp.mean(x_f32, axis=-1, keepdims=True)
    centered = x_f32 - mean_val
    var_val = jnp.mean(centered * centered, axis=-1, keepdims=True)
    return (centered * lax.rsqrt(var_val + NORM_EPS) * gain_vec + bias_vec).astype(jnp.bfloat16)


def rotate_heads(x_in, angles):
    cos_half = jnp.cos(angles) * ROPE_MSCALE
    sin_half = jnp.sin(angles) * ROPE_MSCALE
    cos_full = jnp.concatenate([cos_half, cos_half], axis=-1)[:, None, :]
    sin_full = jnp.concatenate([sin_half, sin_half], axis=-1)[:, None, :]
    x_f32 = x_in.astype(jnp.float32)
    rotated = jnp.concatenate([-x_f32[..., HALF_DIM:], x_f32[..., :HALF_DIM]], axis=-1)
    return (x_f32 * cos_full + rotated * sin_full).astype(jnp.bfloat16)


def partial_stats(q_grp, keys, values, keep_mask):
    scores = jnp.einsum('bkgd,btkd->bkgt', q_grp.astype(jnp.float32), keys.astype(jnp.float32)) * (HEAD_DIM ** -0.5)
    keep_full = keep_mask[:, None, None, :]
    scores = jnp.where(keep_full, scores, NEG_FILL)
    run_max = jnp.max(scores, axis=-1)
    weights = jnp.where(keep_full, jnp.exp(scores - run_max[..., None]), 0.0)
    run_sum = jnp.sum(weights, axis=-1)
    out_part = jnp.einsum('bkgt,btkd->bkgd', weights.astype(jnp.bfloat16).astype(jnp.float32), values.astype(jnp.float32))
    return run_max, run_sum, out_part


def reference(x_first, next_emb, k_cache, v_cache, seq_len, ln1_gain, ln1_bias, w_q, b_q, w_k, b_k, w_v, b_v, w_o, b_o, ln2_gain, ln2_bias, w_router, w_gate, w_up, w_down, long_factor, expert_idx, route_mask):
    inv_freq = 1.0 / (long_factor * ROPE_BASE ** (jnp.arange(HALF_DIM, dtype=jnp.float32) * 2.0 / HEAD_DIM))
    step_inputs = jnp.concatenate([x_first[None], next_emb], axis=0)
    shard_ids = jnp.arange(KV_GROUP)
    tail_slots = jnp.arange(NUM_STEPS)

    def decode_step(step_carry, step_in):
        tail_k, tail_v = step_carry
        x_in, idx_step, mask_step, step_idx = step_in
        h_norm = layer_norm(x_in, ln1_gain, ln1_bias)
        q_new = (jnp.dot(h_norm, w_q, preferred_element_type=jnp.float32) + b_q).astype(jnp.bfloat16).reshape(BATCH_SIZE, Q_HEADS, HEAD_DIM)
        k_new = (jnp.dot(h_norm, w_k, preferred_element_type=jnp.float32) + b_k).astype(jnp.bfloat16).reshape(BATCH_SIZE, KV_HEADS, HEAD_DIM)
        v_new = (jnp.dot(h_norm, w_v, preferred_element_type=jnp.float32) + b_v).astype(jnp.bfloat16).reshape(BATCH_SIZE, KV_HEADS, HEAD_DIM)
        angles = (seq_len + step_idx).astype(jnp.float32)[:, None] * inv_freq[None, :]
        q_grp = rotate_heads(q_new, angles).reshape(BATCH_SIZE, KV_HEADS, Q_GROUP, HEAD_DIM)
        k_rot = rotate_heads(k_new, angles)
        tail_k = lax.dynamic_update_slice_in_dim(tail_k, k_rot[:, None], step_idx, axis=1)
        tail_v = lax.dynamic_update_slice_in_dim(tail_v, v_new[:, None], step_idx, axis=1)

        def one_shard(shard_id):
            k_blk = lax.dynamic_slice_in_dim(k_cache, shard_id * SHARD_LEN, SHARD_LEN, axis=1)
            v_blk = lax.dynamic_slice_in_dim(v_cache, shard_id * SHARD_LEN, SHARD_LEN, axis=1)
            positions = shard_id * SHARD_LEN + jnp.arange(SHARD_LEN)
            keep_mask = positions[None, :] < seq_len[:, None]
            return partial_stats(q_grp, k_blk, v_blk, keep_mask)

        cache_max, cache_sum, cache_out = lax.map(one_shard, shard_ids)
        tail_keep = jnp.broadcast_to(tail_slots[None, :] <= step_idx, (BATCH_SIZE, NUM_STEPS))
        tail_max, tail_sum, tail_out = partial_stats(q_grp, tail_k, tail_v, tail_keep)
        max_all = jnp.concatenate([cache_max, tail_max[None]], axis=0)
        sum_all = jnp.concatenate([cache_sum, tail_sum[None]], axis=0)
        out_all = jnp.concatenate([cache_out, tail_out[None]], axis=0)
        top_max = jnp.max(max_all, axis=0, keepdims=True)
        factor = jnp.exp(max_all - top_max)
        total_sum = jnp.sum(sum_all * factor, axis=0)
        merged = jnp.sum(out_all * factor[..., None], axis=0) / total_sum[..., None]
        attn_out = merged.reshape(BATCH_SIZE, Q_HEADS * HEAD_DIM).astype(jnp.bfloat16)
        x_mid = (x_in.astype(jnp.float32) + jnp.dot(attn_out, w_o, preferred_element_type=jnp.float32) + b_o).astype(jnp.bfloat16)
        h_moe = layer_norm(x_mid, ln2_gain, ln2_bias)
        logits = jnp.dot(h_moe, w_router, preferred_element_type=jnp.float32)
        masked = jnp.where(mask_step == 1, logits[:, None, :], NEG_FILL)
        gate_probs = jax.nn.softmax(masked, axis=-1)
        chosen = idx_step[..., None] == jnp.arange(NUM_EXPERTS)[None, None, :]
        gate_mat = jnp.sum(jnp.where(chosen, gate_probs, 0.0), axis=1)

        def expert_body(part_acc, expert_in):
            gate_w, up_w, down_w, gate_col = expert_in
            act_gate = jnp.dot(h_moe, gate_w, preferred_element_type=jnp.float32)
            act_up = jnp.dot(h_moe, up_w, preferred_element_type=jnp.float32)
            mixed_act = (gate_col[:, None] * jax.nn.silu(act_gate) * act_up).astype(jnp.bfloat16)
            blocks = mixed_act.reshape(BATCH_SIZE, KV_GROUP, FF_SHARD).astype(jnp.float32)
            down_blocks = down_w.reshape(KV_GROUP, FF_SHARD, D_MODEL).astype(jnp.float32)
            return part_acc + jnp.einsum('bjf,jfd->bjd', blocks, down_blocks), None

        part_init = jnp.zeros((BATCH_SIZE, KV_GROUP, D_MODEL), jnp.float32)
        part_acc = lax.scan(expert_body, part_init, (w_gate, w_up, w_down, gate_mat.T))[0]
        moe_out = jnp.sum(part_acc.astype(jnp.bfloat16).astype(jnp.float32), axis=1)
        x_out = (x_mid.astype(jnp.float32) + moe_out).astype(jnp.bfloat16)
        return (tail_k, tail_v), x_out

    tail_init = jnp.zeros((BATCH_SIZE, NUM_STEPS, KV_HEADS, HEAD_DIM), jnp.bfloat16)
    final_carry, hidden = lax.scan(decode_step, (tail_init, tail_init), (step_inputs, expert_idx, route_mask, jnp.arange(NUM_STEPS)))
    return hidden, final_carry[0], final_carry[1]
```

```python
import math
import jax
import jax.numpy as jnp
from jax import lax
from jax.sharding import PartitionSpec as P

ROPE_BASE = 10000.0
ROPE_MSCALE = math.sqrt(1.0 + math.log(32.0) / math.log(4096.0))
NORM_EPS = 1e-5
NEG_FILL = -1e30


def layer_norm(x_in, gain_vec, bias_vec):
    x_f32 = x_in.astype(jnp.float32)
    mean_val = jnp.mean(x_f32, axis=-1, keepdims=True)
    centered = x_f32 - mean_val
    var_val = jnp.mean(centered * centered, axis=-1, keepdims=True)
    return (centered * lax.rsqrt(var_val + NORM_EPS) * gain_vec + bias_vec).astype(jnp.bfloat16)


def rotate_heads(x_in, angles):
    half_dim = x_in.shape[-1] // 2
    cos_half = jnp.cos(angles) * ROPE_MSCALE
    sin_half = jnp.sin(angles) * ROPE_MSCALE
    cos_full = jnp.concatenate([cos_half, cos_half], axis=-1)[:, None, :]
    sin_full = jnp.concatenate([sin_half, sin_half], axis=-1)[:, None, :]
    x_f32 = x_in.astype(jnp.float32)
    rotated = jnp.concatenate([-x_f32[..., half_dim:], x_f32[..., :half_dim]], axis=-1)
    return (x_f32 * cos_full + rotated * sin_full).astype(jnp.bfloat16)


def inverse_freq(long_factor, head_dim):
    half_dim = head_dim // 2
    return 1.0 / (long_factor * ROPE_BASE ** (jnp.arange(half_dim, dtype=jnp.float32) * 2.0 / head_dim))


def partial_stats(q_grp, keys, values, keep_mask):
    scores = jnp.einsum('bkgd,btkd->bkgt', q_grp, keys, preferred_element_type=jnp.float32) * (q_grp.shape[-1] ** -0.5)
    keep_full = keep_mask
    scores = jnp.where(keep_full, scores, NEG_FILL)
    run_max = jnp.max(scores, axis=-1)
    weights = jnp.where(keep_full, jnp.exp(scores - run_max[..., None]), 0.0)
    run_sum = jnp.sum(weights, axis=-1)
    out_part = jnp.einsum('bkgt,btkd->bkgd', weights.astype(jnp.bfloat16), values, preferred_element_type=jnp.float32)
    return run_max, run_sum, out_part


def combine_stats(max_all, sum_all, out_all):
    top_max = jnp.max(max_all, axis=0, keepdims=True)
    factor = jnp.exp(max_all - top_max)
    total_sum = jnp.sum(sum_all * factor, axis=0)
    merged = jnp.sum(out_all * factor[..., None], axis=0)
    return merged / total_sum[..., None]


def gate_matrix(h_moe, w_router, idx_step, mask_step):
    logits = jnp.dot(h_moe, w_router, preferred_element_type=jnp.float32)
    masked = jnp.where(mask_step == 1, logits[:, None, :], NEG_FILL)
    gate_probs = jax.nn.softmax(masked, axis=-1)
    chosen = idx_step[..., None] == jnp.arange(logits.shape[-1])[None, None, :]
    return jnp.sum(jnp.where(chosen, gate_probs, 0.0), axis=1)


def expert_part(h_moe, gate_mat, w_gate, w_up, w_down):
    act_gate = jnp.einsum('bd,edf->bef', h_moe, w_gate, preferred_element_type=jnp.float32)
    act_up = jnp.einsum('bd,edf->bef', h_moe, w_up, preferred_element_type=jnp.float32)
    mixed_act = (gate_mat[:, :, None] * jax.nn.silu(act_gate) * act_up).astype(jnp.bfloat16)
    return jnp.einsum('bef,efd->bd', mixed_act, w_down, preferred_element_type=jnp.float32).astype(jnp.bfloat16)


def solution(mesh):
    def layer_steps(x_first, next_emb, k_cache, v_cache, seq_len, ln1_gain, ln1_bias, w_q, b_q, w_k, b_k, w_v, b_v, w_o, b_o, ln2_gain, ln2_bias, w_router, w_gate, w_up, w_down, long_factor, expert_idx, route_mask):
        batch_rows, shard_len, kv_heads, head_dim = k_cache.shape
        q_heads = w_q.shape[1] // head_dim
        q_group = q_heads // kv_heads
        shard_id = lax.axis_index('kv')
        positions = shard_id * shard_len + jnp.arange(shard_len)
        cache_keep = positions[None, :] < seq_len[:, None]
        inv_freq = inverse_freq(long_factor, head_dim)
        num_steps = next_emb.shape[0] + 1
        x_all = jnp.concatenate([x_first[None], next_emb], axis=0)
        rows = num_steps * batch_rows
        h_norm = layer_norm(x_all, ln1_gain, ln1_bias).reshape(rows, -1)
        q_new = (jnp.dot(h_norm, w_q, preferred_element_type=jnp.float32) + b_q).astype(jnp.bfloat16).reshape(rows, q_heads, head_dim)
        k_new = (jnp.dot(h_norm, w_k, preferred_element_type=jnp.float32) + b_k).astype(jnp.bfloat16).reshape(rows, kv_heads, head_dim)
        v_new = (jnp.dot(h_norm, w_v, preferred_element_type=jnp.float32) + b_v).astype(jnp.bfloat16).reshape(num_steps, batch_rows, kv_heads, head_dim)
        steps = jnp.arange(num_steps)
        angles = ((seq_len[None, :] + steps[:, None]).astype(jnp.float32)[:, :, None] * inv_freq).reshape(rows, -1)
        q_rot = rotate_heads(q_new, angles).reshape(num_steps, batch_rows, kv_heads, q_group, head_dim)
        q_grp = q_rot.transpose(1, 2, 0, 3, 4).reshape(batch_rows, kv_heads, num_steps * q_group, head_dim)
        tail_k = rotate_heads(k_new, angles).reshape(num_steps, batch_rows, kv_heads, head_dim).transpose(1, 0, 2, 3)
        tail_v = v_new.transpose(1, 0, 2, 3)
        run_max, run_sum, out_part = partial_stats(q_grp, k_cache, v_cache, cache_keep[:, None, None, :])
        packed = jnp.concatenate([run_max[..., None], run_sum[..., None], out_part], axis=-1)
        gathered = lax.all_gather(packed, 'kv')
        tail_keep = jnp.repeat(steps[None, :] <= steps[:, None], q_group, axis=0)[None, None]
        tail_max, tail_sum, tail_out = partial_stats(q_grp, tail_k, tail_v, tail_keep)
        max_all = jnp.concatenate([gathered[..., 0], tail_max[None]], axis=0)
        sum_all = jnp.concatenate([gathered[..., 1], tail_sum[None]], axis=0)
        out_all = jnp.concatenate([gathered[..., 2:], tail_out[None]], axis=0)
        attn = combine_stats(max_all, sum_all, out_all).astype(jnp.bfloat16)
        attn = attn.reshape(batch_rows, kv_heads, num_steps, q_group, head_dim).transpose(2, 0, 1, 3, 4).reshape(rows, q_heads * head_dim)
        x_flat = x_all.reshape(rows, -1)
        x_mid = (x_flat.astype(jnp.float32) + jnp.dot(attn, w_o, preferred_element_type=jnp.float32) + b_o).astype(jnp.bfloat16)
        h_moe = layer_norm(x_mid, ln2_gain, ln2_bias)
        gate_mat = gate_matrix(h_moe, w_router, expert_idx.reshape(rows, -1), route_mask.reshape(rows, *route_mask.shape[2:]))
        moe_part = expert_part(h_moe, gate_mat, w_gate, w_up, w_down)
        moe_sum = lax.psum(moe_part.astype(jnp.float32), 'kv')
        hidden = (x_mid.astype(jnp.float32) + moe_sum).astype(jnp.bfloat16)
        return hidden.reshape(num_steps, batch_rows, -1), tail_k, tail_v

    replicated = P()
    in_specs = (P('dp'), P(None, 'dp'), P('dp', 'kv'), P('dp', 'kv'), P('dp')) + (replicated,) * 13 + (P(None, None, 'kv'), P(None, None, 'kv'), P(None, 'kv'), replicated, P(None, 'dp'), P(None, 'dp'))
    out_specs = (P(None, 'dp'), P('dp'), P('dp'))
    return jax.shard_map(layer_steps, mesh=mesh, in_specs=in_specs, out_specs=out_specs, check_vma=False)
```

```python
import functools
import math

import jax
import jax.numpy as jnp
import numpy as np
from jax import lax
from jax.experimental import pallas as pl
from jax.experimental.pallas import tpu as pltpu
from jax.sharding import PartitionSpec as P

ROPE_BASE = 10000.0
ROPE_MSCALE = math.sqrt(1.0 + math.log(32.0) / math.log(4096.0))
NORM_EPS = 1e-5
NEG_FILL = -1e30
MESH = pl.DeviceIdType.MESH
F32 = jnp.float32
BF16 = jnp.bfloat16
LANES = 128
WCOLS = 512
CORES = 2
VMEM_BYTES = 67043328
NT = (((1,), (1,)), ((), ()))


def iota(shape, dim):
    return lax.broadcasted_iota(jnp.int32, shape, dim)


def to_row(col):
    rows = col.shape[0]
    pick = iota((rows, LANES), 0) == iota((rows, LANES), 1)
    return jnp.sum(jnp.where(pick, jnp.broadcast_to(col, (rows, LANES)), 0.0), axis=0, keepdims=True)


def to_col(row, rows):
    pick = iota((rows, LANES), 0) == iota((rows, LANES), 1)
    return jnp.sum(jnp.where(pick, jnp.broadcast_to(row, (rows, LANES)), 0.0), axis=1, keepdims=True)


def stat_tile(m_row, l_row):
    r = iota((8, LANES), 0)
    return jnp.where(r == 0, jnp.broadcast_to(m_row, (8, LANES)), jnp.where(r == 1, jnp.broadcast_to(l_row, (8, LANES)), 0.0))


def softmax_part(s_raw, valid, scale):
    s = jnp.where(valid, s_raw * scale, NEG_FILL)
    m = jnp.max(s, axis=1, keepdims=True)
    w = jnp.where(valid, jnp.exp(s - m), 0.0)
    return m, jnp.sum(w, axis=1, keepdims=True), w.astype(BF16)


def round_bf16(x):
    return x.astype(BF16).astype(F32)


def kernel(dims, lens_ref, ei_ref, rm_ref,
           x_first, next_emb, k_hbm, v_hbm, g1, c1, w_q, b_q, w_k, b_k, w_v, b_v, w_o, b_o, g2, c2, w_r, w_g, w_u, w_d, lf, pw,
           out_ref, tk_ref, tv_ref,
           wring, kbuf, vbuf, wmoe, xin, x32, h, vg1, vc1, vg2, vc2, vbo, vbq, vbk, vbv, vlf, vpw, vwr,
           qbuf, cosb, sinb, kt, vt, tkv, psend, precv, omine, osend, orecv, oxs, lhs, xg, gs, ub, mine, mpsend, mprecv, mosend, morecv, yg, t32,
           wsem, ksem, vsem, msem, ssem, qx_s, qx_r, kx_s, kx_r, vx_s, vx_r, ps_s, ps_r, os_s, os_r, ox_s, ox_r,
           xa_s, xa_r, xf_s, mp_s, mp_r, mo_s, mo_r, ya_s, ya_r, yf_s):
    S, B, D, T, KH, HD, H, E, FE, chips = (dims[k] for k in ("S", "B", "D", "T", "KH", "HD", "H", "E", "FE", "chips"))
    R = S * B
    HH, KHH = H // CORES, KH // CORES
    half_cols = D // CORES
    QG = H // KH
    QR = S * HH
    MR = QR + 8
    PC = LANES * CORES
    FEP = wmoe.shape[1]
    scale = HD ** -0.5
    me = lax.axis_index("kv")
    chip = me // CORES
    c = lax.rem(me, CORES)
    partner = chip * CORES + (1 - c)

    def peer(ch):
        return ch * CORES + c

    bar = pltpu.get_barrier_semaphore()
    pl.semaphore_signal(bar, inc=1, device_id={"kv": partner}, device_id_type=MESH)

    def sig(i, _):
        pl.semaphore_signal(bar, inc=1, device_id={"kv": peer(lax.rem(chip + i, chips))}, device_id_type=MESH)
        return 0
    lax.fori_loop(1, chips, sig, 0)

    def wsrc(ci):
        if ci < 4:
            return w_q.at[:, pl.ds(pl.multiple_of(c * half_cols + ci * WCOLS, WCOLS), WCOLS)]
        if ci == 4:
            return w_k.at[:, pl.ds(pl.multiple_of(c * WCOLS, WCOLS), WCOLS)]
        if ci == 5:
            return w_v.at[:, pl.ds(pl.multiple_of(c * WCOLS, WCOLS), WCOLS)]
        return w_o.at[:, pl.ds(pl.multiple_of(c * half_cols + (ci - 6) * WCOLS, WCOLS), WCOLS)]

    def wcopy(ci):
        return pltpu.make_async_copy(wsrc(ci), wring.at[ci % 4], wsem.at[ci])

    smalls = [(x_first, xin.at[0]), (next_emb, xin.at[pl.ds(1, S - 1)]), (g1, vg1), (c1, vc1), (b_q, vbq), (b_k, vbk), (b_v, vbv),
              (lf, vlf), (pw, vpw), (g2, vg2), (c2, vc2), (b_o, vbo), (w_r, vwr)]
    small_copies = [pltpu.make_async_copy(a, b, ssem.at[i]) for i, (a, b) in enumerate(smalls)]
    for cp in small_copies[:9]:
        cp.start()
    for ci in range(4):
        wcopy(ci).start()
    for cp in small_copies[9:]:
        cp.start()

    def kcopy(b):
        return pltpu.make_async_copy(k_hbm.at[b], kbuf.at[b], ksem.at[b])

    def vcopy(b):
        return pltpu.make_async_copy(v_hbm.at[b], vbuf.at[b], vsem.at[b])

    moe_copies = [pltpu.make_async_copy(src, wmoe.at[i, pl.ds(0, FE)], msem.at[i]) for i, src in enumerate((w_g, w_u, w_d))]

    wmoe[2, FE:FEP, :] = jnp.zeros((FEP - FE, D), BF16)
    lhs[...] = jnp.zeros_like(lhs)
    gs[...] = jnp.zeros_like(gs)
    tkv[...] = jnp.zeros_like(tkv)

    row_b = lax.rem(iota((R, LANES), 0), B)
    pos = iota((R, LANES), 0) // B
    for b in range(B):
        pos = pos + jnp.where(row_b == b, lens_ref[b], 0)

    def layer_norm(s, gain, bias):
        x = x32[s * B:(s + 1) * B, :]
        mean = jnp.sum(x, axis=1, keepdims=True) / D
        cen = x - mean
        var = jnp.sum(cen * cen, axis=1, keepdims=True) / D
        h[s * B:(s + 1) * B, :] = (cen * lax.rsqrt(var + NORM_EPS) * gain[...] + bias[...]).astype(BF16)

    for cp in small_copies[:9]:
        cp.wait()
    for s in range(S):
        x32[s * B:(s + 1) * B, :] = xin[s].astype(F32)
        layer_norm(s, vg1, vc1)
    inv = 1.0 / (vlf[...] * vpw[...])
    ang = pos.astype(F32) * inv
    cosb[...] = jnp.cos(ang) * ROPE_MSCALE
    sn = jnp.sin(ang) * ROPE_MSCALE
    sinb[...] = jnp.where(iota((R, LANES), 1) < HD // 2, -sn, sn)

    def rotate(x):
        return round_bf16(x * cosb[...] + pltpu.roll(x, HD // 2, 1) * sinb[...])

    def q_chunk(ci, _):
        pltpu.make_async_copy(wsrc(0), wring.at[ci], wsem.at[ci]).wait()
        off = pl.multiple_of(c * half_cols + ci * WCOLS, WCOLS)
        y = jnp.dot(h[...], wring[ci], preferred_element_type=F32) + vbq[:, pl.ds(off, WCOLS)]
        y = round_bf16(y)
        for t in range(WCOLS // HD):
            r = rotate(y[:, t * HD:(t + 1) * HD])
            hh = ci * (WCOLS // HD) + t
            for s in range(S):
                qbuf[c, pl.ds(s * HH + hh, B, stride=QR), :] = r[s * B:(s + 1) * B, :]

        @pl.when(ci == 0)
        def _():
            wcopy(4).start()

        @pl.when(ci == 1)
        def _():
            wcopy(5).start()

            def kv_start(j, _):
                b = lax.rem(chip + 1 + j, chips)
                kcopy(b).start()
                vcopy(b).start()
                return 0
            lax.fori_loop(0, B, kv_start, 0)

        @pl.when(ci == 2)
        def _():
            wcopy(6).start()

        @pl.when(ci == 3)
        def _():
            wcopy(7).start()
        return 0
    lax.fori_loop(0, 4, q_chunk, 0)

    pl.semaphore_wait(bar, chips)

    def to_partner(src, dst, ss, rs):
        return pltpu.make_async_remote_copy(src, dst, ss, rs, device_id={"kv": partner}, device_id_type=MESH)

    q_x = to_partner(qbuf.at[c], qbuf.at[c], qx_s, qx_r)
    q_x.start()

    wcopy(4).wait()
    y = round_bf16(jnp.dot(h[...], wring[0], preferred_element_type=F32) + vbk[:, pl.ds(pl.multiple_of(c * WCOLS, WCOLS), WCOLS)])
    for t in range(KHH):
        kt[c, t, :, :] = rotate(y[:, t * HD:(t + 1) * HD])
    wcopy(8).start()
    wcopy(5).wait()
    y = round_bf16(jnp.dot(h[...], wring[1], preferred_element_type=F32) + vbv[:, pl.ds(pl.multiple_of(c * WCOLS, WCOLS), WCOLS)])
    for t in range(KHH):
        vt[c, t, :, :] = y[:, t * HD:(t + 1) * HD]
    wcopy(9).start()
    for cp in moe_copies:
        cp.start()
    k_x = to_partner(kt.at[c], kt.at[c], kx_s, kx_r)
    v_x = to_partner(vt.at[c], vt.at[c], vx_s, vx_r)
    k_x.start()
    v_x.start()

    q_x.wait_recv()
    row_hh = lax.rem(iota((QR, T * KH), 0), HH) // QG
    lane = iota((QR, T * KH), 1)
    lane_kh = lax.rem(lane, KH)

    def o_copy(b):
        return pltpu.make_async_remote_copy(osend.at[b], orecv.at[chip], os_s.at[b], os_r.at[chip],
                                            device_id={"kv": peer(b)}, device_id_type=MESH)

    def pair_combine(b, dst, di):
        to_partner(psend.at[b], precv.at[b], ps_s.at[b], ps_r.at[b]).wait_recv()
        m1, l1 = omine[b, QR:QR + 1, :], omine[b, QR + 1:QR + 2, :]
        m2, l2 = precv[b, QR:QR + 1, :], precv[b, QR + 1:QR + 2, :]
        top = jnp.maximum(m1, m2)
        f1, f2 = jnp.exp(m1 - top), jnp.exp(m2 - top)
        dst[di, 0:QR, :] = omine[b, 0:QR, :] * to_col(f1, QR) + precv[b, 0:QR, :] * to_col(f2, QR)
        dst[di, QR:MR, :] = stat_tile(top, l1 * f1 + l2 * f2)

    def attn_step(j, _):
        b = lax.rem(chip + 1 + j, chips)
        kcopy(b).wait()
        vcopy(b).wait()
        lim = (lens_ref[b] - me * T) * KH
        for which in range(2):
            half = 1 - c if which == 0 else c
            dst = psend if which == 0 else omine
            qb = qbuf[half, pl.ds(pl.multiple_of(b * QR, QR), QR), :].astype(BF16)
            sc = lax.dot_general(qb, kbuf[b], NT, preferred_element_type=F32)
            valid = (lane_kh == row_hh + half * KHH) & (lane < lim)
            m, l, w = softmax_part(sc, valid, scale)
            dst[b, 0:QR, :] = jnp.dot(w, vbuf[b], preferred_element_type=F32)
            dst[b, QR:MR, :] = stat_tile(to_row(m), to_row(l))
            if which == 0:
                to_partner(psend.at[b], precv.at[b], ps_s.at[b], ps_r.at[b]).start()

        @pl.when(j > 0)
        def _():
            pb = lax.rem(chip + j, chips)
            pair_combine(pb, osend, pb)
            o_copy(pb).start()
        return 0
    lax.fori_loop(0, B, attn_step, 0)
    pair_combine(chip, orecv, chip)

    for s in range(S):
        for t in range(KHH):
            tkv[0, s * KHH + t:s * KHH + t + 1, :] = kt[c, t, pl.ds(s * B + chip, 1), :]
            tkv[1, s * KHH + t:s * KHH + t + 1, :] = vt[c, t, pl.ds(s * B + chip, 1), :]
    TR = tkv.shape[1]
    qb = qbuf[c, pl.ds(pl.multiple_of(chip * QR, QR), QR), :].astype(BF16)
    sc = lax.dot_general(qb, tkv[0].astype(BF16), NT, preferred_element_type=F32)
    tr, tl = iota((QR, TR), 0), iota((QR, TR), 1)
    valid = (lax.rem(tl, KHH) == lax.rem(tr, HH) // QG) & (tl // KHH <= tr // HH) & (tl < S * KHH)
    m, l, w = softmax_part(sc, valid, scale)
    orecv[chips, 0:QR, :] = jnp.dot(w, tkv[1].astype(BF16), preferred_element_type=F32)
    orecv[chips, QR:MR, :] = stat_tile(to_row(m), to_row(l))

    def o_wait(i, _):
        src = lax.rem(chip + chips - i, chips)
        pltpu.make_async_remote_copy(osend.at[0], orecv.at[src], os_s.at[0], os_r.at[src],
                                     device_id={"kv": peer(src)}, device_id_type=MESH).wait_recv()
        return 0
    lax.fori_loop(1, chips, o_wait, 0)

    top = orecv[0, QR:QR + 1, :]
    for i in range(1, chips + 1):
        top = jnp.maximum(top, orecv[i, QR:QR + 1, :])
    tot = jnp.zeros((1, LANES), F32)
    acc = jnp.zeros((QR, LANES), F32)
    for i in range(chips + 1):
        f = jnp.exp(orecv[i, QR:QR + 1, :] - top)
        tot = tot + orecv[i, QR + 1:QR + 2, :] * f
        acc = acc + orecv[i, 0:QR, :] * to_col(f, QR)
    oxs[c, :, :] = round_bf16(acc / to_col(tot, QR))
    o_x = to_partner(oxs.at[c], oxs.at[c], ox_s, ox_r)
    o_x.start()
    o_x.wait_recv()
    for hf in range(CORES):
        for hh in range(HH):
            lhs[0:S, (hf * HH + hh) * HD:(hf * HH + hh + 1) * HD] = oxs[hf, pl.ds(hh, S, stride=HH), :]
    for cp in small_copies[9:]:
        cp.wait()

    ctiles = WCOLS // LANES
    my_slot = pl.multiple_of(me * QR, QR)

    def wo_chunk(jn, _):
        slot = lax.rem(jn + 2, 4)
        pltpu.make_async_copy(wsrc(0), wring.at[slot], wsem.at[jn + 6]).wait()
        off = pl.multiple_of(c * half_cols + jn * WCOLS, WCOLS)
        d = jnp.dot(lhs[...].astype(BF16), wring[slot], preferred_element_type=F32)
        for s in range(S):
            v = round_bf16(x32[pl.ds(s * B + chip, 1), pl.ds(off, WCOLS)] + d[s:s + 1, :] + vbo[:, pl.ds(off, WCOLS)])
            for t in range(ctiles):
                xg[pl.ds(my_slot + s * HH + jn * ctiles + t, 1), :] = v[:, t * LANES:(t + 1) * LANES]
        return 0
    lax.fori_loop(0, 4, wo_chunk, 0)

    def gather(buf, ss, rs, fs):
        def blk(slot):
            return buf.at[pl.ds(pl.multiple_of(slot * QR, QR), QR)]

        def cp(slot, sem, dev):
            return pltpu.make_async_remote_copy(blk(slot), blk(slot), sem, rs.at[slot], device_id={"kv": dev}, device_id_type=MESH)

        def send(i, _):
            cp(me, ss.at[i], peer(lax.rem(chip + i, chips))).start()
            return 0
        cp(me, ss.at[0], partner).start()
        lax.fori_loop(1, chips, send, 0)

        def fwd(i, _):
            slot = peer(lax.rem(chip + chips - i, chips))
            cp(slot, ss.at[0], partner).wait_recv()
            cp(slot, fs.at[i], partner).start()
            return 0
        lax.fori_loop(1, chips, fwd, 0)

        def other(i, _):
            slot = lax.rem(chip + chips - i, chips) * CORES + (1 - c)
            cp(slot, ss.at[0], partner).wait_recv()
            return 0
        lax.fori_loop(0, chips, other, 0)

        def drain():
            cp(me, ss.at[0], partner).wait_send()

            def dr(i, _):
                cp(me, ss.at[i], partner).wait_send()
                cp(me, fs.at[i], partner).wait_send()
                return 0
            lax.fori_loop(1, chips, dr, 0)
        return drain

    x_drain = gather(xg, xa_s, xa_r, xf_s)
    for s in range(S):
        for hf in range(CORES):
            for t in range(HH):
                x32[s * B:(s + 1) * B, (hf * HH + t) * LANES:(hf * HH + t + 1) * LANES] = xg[pl.ds(hf * QR + s * HH + t, B, stride=CORES * QR), :]

    for s in range(S):
        layer_norm(s, vg2, vc2)
    logits = lax.dot_general(h[...], vwr[...], NT, preferred_element_type=F32)
    le = iota((B, E), 1)
    diag = iota((B, B), 0) == iota((B, B), 1)
    for s in range(S):
        lg = logits[s * B:(s + 1) * B, :]
        gate = jnp.zeros((B, E), F32)
        for k in range(ei_ref.shape[1]):
            masked = jnp.where(rm_ref[s, :, k, :] == 1, lg, NEG_FILL)
            ex = jnp.exp(masked - jnp.max(masked, axis=1, keepdims=True))
            p = ex / jnp.sum(ex, axis=1, keepdims=True)
            idx = jnp.sum(jnp.where(diag, jnp.broadcast_to(ei_ref[s, k:k + 1, :], (B, B)).astype(F32), 0.0), axis=1, keepdims=True)
            gate = gate + jnp.where(le.astype(F32) == idx, p, 0.0)
        gs[s * B:(s + 1) * B, 0:E] = gate
    g = gs[...]
    step = E
    while step < LANES:
        g = g + pltpu.roll(g, step, 1)
        step *= 2
    moe_copies[0].wait()
    moe_copies[1].wait()
    for t in range(FEP // 256):
        ag = lax.dot_general(h[...], wmoe[0, t * 256:(t + 1) * 256, :], NT, preferred_element_type=F32)
        au = lax.dot_general(h[...], wmoe[1, t * 256:(t + 1) * 256, :], NT, preferred_element_type=F32)
        gg = jnp.concatenate([g] * (256 // LANES), axis=1)
        u = gg * (ag * jax.nn.sigmoid(ag)) * au
        u = jnp.where(iota((R, 256), 1) + t * 256 < FE, u, 0.0)
        ub[:, t * 256:(t + 1) * 256] = u.astype(BF16)
    moe_copies[2].wait()

    def mo_copy(i):
        return pltpu.make_async_remote_copy(mosend.at[i], morecv.at[chip], mo_s.at[i], mo_r.at[chip],
                                            device_id={"kv": peer(i)}, device_id_type=MESH)

    def moe_pair(i, dst, di):
        to_partner(mpsend.at[i], mprecv.at[i], mp_s.at[i], mp_r.at[i]).wait_recv()
        dst[di, :, :] = mine[i] + mprecv[i]

    def moe_step(j, _):
        i = lax.rem(chip + 1 + j, chips)
        pp = round_bf16(jnp.dot(ub[...], wmoe[2, :, pl.ds(pl.multiple_of(i * PC, PC), PC)], preferred_element_type=F32))
        p0, p1 = pp[:, :LANES], pp[:, LANES:]
        mpsend[i, :, :] = jnp.where(c == 0, p1, p0)
        mine[i, :, :] = jnp.where(c == 0, p0, p1)
        to_partner(mpsend.at[i], mprecv.at[i], mp_s.at[i], mp_r.at[i]).start()

        @pl.when(j > 0)
        def _():
            pi = lax.rem(chip + j, chips)
            moe_pair(pi, mosend, pi)
            mo_copy(pi).start()
        return 0
    lax.fori_loop(0, chips, moe_step, 0)
    moe_pair(chip, morecv, chip)

    k_x.wait_recv()
    v_x.wait_recv()
    for src, dst in ((kt, tk_ref), (vt, tv_ref)):
        for hf in range(CORES):
            for t in range(KHH):
                for s in range(S):
                    t32[pl.ds(s * KH + hf * KHH + t, B, stride=S * KH), :] = src[hf, t, s * B:(s + 1) * B, :]
        dst[...] = t32[...].astype(BF16)

    def mo_wait(i, _):
        src = lax.rem(chip + chips - i, chips)
        pltpu.make_async_remote_copy(mosend.at[0], morecv.at[src], mo_s.at[0], mo_r.at[src],
                                     device_id={"kv": peer(src)}, device_id_type=MESH).wait_recv()
        return 0
    lax.fori_loop(1, chips, mo_wait, 0)
    tot = morecv[0]
    for i in range(1, chips):
        tot = tot + morecv[i]
    yg[pl.ds(my_slot, QR), :] = round_bf16(x32[:, pl.ds(pl.multiple_of(me * LANES, LANES), LANES)] + tot)
    y_drain = gather(yg, ya_s, ya_r, yf_s)
    for d in range(chips * CORES):
        for s in range(S):
            out_ref[s, :, d * LANES:(d + 1) * LANES] = yg[d * QR + s * B:d * QR + (s + 1) * B, :].astype(BF16)

    q_x.wait_send()
    k_x.wait_send()
    v_x.wait_send()
    o_x.wait_send()

    def drain(i, _):
        b = lax.rem(chip + i, chips)
        to_partner(psend.at[b], precv.at[b], ps_s.at[b], ps_r.at[b]).wait_send()
        to_partner(mpsend.at[b], mprecv.at[b], mp_s.at[b], mp_r.at[b]).wait_send()

        @pl.when(i > 0)
        def _():
            o_copy(b).wait_send()
            mo_copy(b).wait_send()
        return 0
    lax.fori_loop(0, chips, drain, 0)
    x_drain()
    y_drain()


def solution(mesh):
    n = mesh.shape["kv"]
    chips = n // CORES

    def layer_steps(x_first, next_emb, k_cache, v_cache, seq_len, ln1_gain, ln1_bias, w_q, b_q, w_k, b_k, w_v, b_v, w_o, b_o, ln2_gain, ln2_bias, w_router, w_gate, w_up, w_down, long_factor, expert_idx, route_mask):
        B, T, KH, HD = k_cache.shape
        D = x_first.shape[1]
        H = w_q.shape[1] // HD
        S = next_emb.shape[0] + 1
        E = w_router.shape[1]
        FE = w_gate.shape[0] * w_gate.shape[2]
        FEP = -(-FE // 256) * 256
        R = S * B
        HH, KHH = H // CORES, KH // CORES
        QR = S * HH
        MR = QR + 8
        if B != chips or D != n * LANES or w_q.shape[1] != D or QR != R:
            raise ValueError("unsupported sizes")
        dims = dict(S=S, B=B, D=D, T=T, KH=KH, HD=HD, H=H, E=E, FE=FE, chips=chips)
        half = HD // 2
        power = np.float32(ROPE_BASE) ** (np.arange(half, dtype=np.float32) * np.float32(2.0) / np.float32(HD))
        pw = jnp.asarray(np.concatenate([power, power])[None, :].astype(np.float32))
        lf = jnp.concatenate([long_factor, long_factor])[None, :]
        row = lambda a: a.reshape(1, -1)
        args = (seq_len, expert_idx.transpose(0, 2, 1), route_mask,
                x_first, next_emb, k_cache.reshape(B, T * KH, HD), v_cache.reshape(B, T * KH, HD), row(ln1_gain), row(ln1_bias),
                w_q, row(b_q), w_k, row(b_k), w_v, row(b_v), w_o, row(b_o), row(ln2_gain), row(ln2_bias), w_router.T,
                w_gate.transpose(2, 0, 1).reshape(FE, D), w_up.transpose(2, 0, 1).reshape(FE, D), w_down.transpose(1, 0, 2).reshape(FE, D), lf, pw)
        V = pltpu.VMEM
        DS = pltpu.SemaphoreType.DMA
        scratch = [
            V((4, D, WCOLS), BF16), V((B, T * KH, HD), BF16), V((B, T * KH, HD), BF16), V((3, FEP, D), BF16),
            V((S, B, D), BF16), V((R, D), F32), V((R, D), BF16),
            V((1, D), F32), V((1, D), F32), V((1, D), F32), V((1, D), F32), V((1, D), F32), V((1, w_q.shape[1]), F32),
            V((1, w_k.shape[1]), F32), V((1, w_v.shape[1]), F32), V((1, HD), F32), V((1, HD), F32), V((E, D), BF16),
            V((CORES, B * QR, HD), F32), V((R, HD), F32), V((R, HD), F32), V((CORES, KHH, R, HD), F32), V((CORES, KHH, R, HD), F32), V((2, 16, HD), F32),
            V((B, MR, HD), F32), V((B, MR, HD), F32), V((B, MR, HD), F32), V((B, MR, HD), F32), V((chips + 1, MR, HD), F32),
            V((CORES, QR, HD), F32), V((8, D), F32), V((n * QR, HD), F32), V((R, LANES), F32), V((R, FEP), BF16),
            V((chips, R, LANES), F32), V((chips, R, LANES), F32), V((chips, R, LANES), F32), V((chips, R, LANES), F32), V((chips, R, LANES), F32),
            V((n * QR, LANES), F32), V((B * S * KH, HD), F32),
            DS((10,)), DS((B,)), DS((B,)), DS((3,)), DS((13,)), DS, DS, DS, DS, DS, DS, DS((B,)), DS((B,)), DS((chips,)), DS((chips,)), DS, DS,
            DS((chips,)), DS((n,)), DS((chips,)), DS((chips,)), DS((chips,)), DS((chips,)), DS((chips,)), DS((chips,)), DS((n,)), DS((chips,)),
        ]
        vm = pl.BlockSpec(memory_space=pltpu.VMEM)
        anys = pl.BlockSpec(memory_space=pl.ANY)
        hidden, tk, tv = pl.pallas_call(
            functools.partial(kernel, dims),
            name="decode_layer",
            out_shape=(jax.ShapeDtypeStruct((S, B, D), BF16), jax.ShapeDtypeStruct((B * S * KH, HD), BF16), jax.ShapeDtypeStruct((B * S * KH, HD), BF16)),
            in_specs=[pl.BlockSpec(memory_space=pltpu.SMEM), vm, vm] + [anys] * (len(args) - 3),
            out_specs=(vm, vm, vm),
            scratch_shapes=scratch,
            compiler_params=pltpu.CompilerParams(collective_id=0, has_side_effects=True, vmem_limit_bytes=VMEM_BYTES),
        )(*args)
        return hidden, tk.reshape(B, S, KH, HD), tv.reshape(B, S, KH, HD)

    replicated = P()
    in_specs = (P('dp'), P(None, 'dp'), P('dp', 'kv'), P('dp', 'kv'), P('dp')) + (replicated,) * 13 + (P(None, None, 'kv'), P(None, None, 'kv'), P(None, 'kv'), replicated, P(None, 'dp'), P(None, 'dp'))
    out_specs = (P(None, 'dp'), P('dp'), P('dp'))
    return jax.shard_map(layer_steps, mesh=mesh, in_specs=in_specs, out_specs=out_specs, check_vma=False)
```

```python
import functools
import math

import jax
import jax.numpy as jnp
import numpy as np
from jax import lax
from jax.experimental import pallas as pl
from jax.experimental.pallas import tpu as pltpu
from jax.sharding import PartitionSpec as P

ROPE_BASE = 10000.0
ROPE_MSCALE = math.sqrt(1.0 + math.log(32.0) / math.log(4096.0))
NORM_EPS = 1e-5
NEG_FILL = -1e30
MESH = pl.DeviceIdType.MESH
F32 = jnp.float32
BF16 = jnp.bfloat16
LANES = 128
WCOLS = 512
CORES = 2
VMEM_BYTES = 64 * 1024 * 1024 - 4 * 1024 * 1024
NT = (((1,), (1,)), ((), ()))


def iota(shape, dim):
    return lax.broadcasted_iota(jnp.int32, shape, dim)


def to_row(col):
    rows = col.shape[0]
    pick = iota((rows, LANES), 0) == iota((rows, LANES), 1)
    return jnp.sum(jnp.where(pick, jnp.broadcast_to(col, (rows, LANES)), 0.0), axis=0, keepdims=True)


def to_col(row, rows):
    pick = iota((rows, LANES), 0) == iota((rows, LANES), 1)
    return jnp.sum(jnp.where(pick, jnp.broadcast_to(row, (rows, LANES)), 0.0), axis=1, keepdims=True)


def stat_tile(m_row, l_row):
    r = iota((8, LANES), 0)
    return jnp.where(r == 0, jnp.broadcast_to(m_row, (8, LANES)), jnp.where(r == 1, jnp.broadcast_to(l_row, (8, LANES)), 0.0))


def softmax_part(s_raw, valid, scale):
    s = jnp.where(valid, s_raw * scale, NEG_FILL)
    m = jnp.max(s, axis=1, keepdims=True)
    w = jnp.where(valid, jnp.exp(s - m), 0.0)
    return m, jnp.sum(w, axis=1, keepdims=True), w.astype(BF16)


def round_bf16(x):
    return x.astype(BF16).astype(F32)


def kernel(dims, lens_h, ei_h, rm_h,
           x_first, next_emb, k_hbm, v_hbm, g1, c1, w_q, b_q, w_k, b_k, w_v, b_v, w_o, b_o, g2, c2, w_r, w_g, w_u, w_d, lf, pw,
           out_ref, tk_ref, tv_ref,
           lens_ref, ei_ref, rm_ref, wring, kbuf, vbuf, wmoe, xin, x32, h, vg1, vc1, vg2, vc2, vbo, vbq, vbk, vbv, vlf, vpw, vwr,
           qbuf, cosb, sinb, kt, vt, tkv, kbias, sbuf, wbuf, part, precv, osend, orecv, oxs, lhs, wacc, xg, gs, gt, ut, ub, mine, mpsend, mprecv, mosend, morecv, yg, t32,
           wsem, ksem, vsem, msem, ssem, qx_s, qx_r, kx_s, kx_r, vx_s, vx_r, ps_s, ps_r, os_s, os_r, ox_s, ox_r,
           xa_s, xa_r, xf_s, mp_s, mp_r, mo_s, mo_r, ya_s, ya_r, yf_s):
    S, B, D, T, KH, HD, H, E, FE, chips = (dims[k] for k in ("S", "B", "D", "T", "KH", "HD", "H", "E", "FE", "chips"))
    R = S * B
    HH, KHH = H // CORES, KH // CORES
    half_cols = D // CORES
    QG = H // KH
    QR = S * HH
    MR = QR + 8
    PC = LANES * CORES
    FEP = wmoe.shape[1]
    scale = HD ** -0.5
    me = lax.axis_index("kv")
    chip = me // CORES
    c = lax.rem(me, CORES)
    partner = chip * CORES + (1 - c)

    def peer(ch):
        return ch * CORES + c

    side = math.isqrt(chips)
    cy, cx = chip // side, lax.rem(chip, side)

    def ring(k):
        return side // 2 + ((k + 1) // 2) * (1 - 2 * (k % 2))

    def nth(j):
        return lax.rem(cy + ring(j // side), side) * side + lax.rem(cx + ring(lax.rem(j, side)), side)

    def dist(d):
        return min(d, side - d)
    offsets = sorted([(dy, dx) for dy in range(side) for dx in range(side) if dy or dx], key=lambda o: -(dist(o[0]) + dist(o[1])))

    def ahead(o):
        return lax.rem(cy + o[0], side) * side + lax.rem(cx + o[1], side)

    def behind(o):
        return lax.rem(cy + side - o[0], side) * side + lax.rem(cx + side - o[1], side)

    bar = pltpu.get_barrier_semaphore()
    pl.semaphore_signal(bar, inc=1, device_id={"kv": partner}, device_id_type=MESH)

    def sig(i, _):
        pl.semaphore_signal(bar, inc=1, device_id={"kv": peer(lax.rem(chip + i, chips))}, device_id_type=MESH)
        return 0
    lax.fori_loop(1, chips, sig, 0)

    def wsrc(ci):
        if ci < 4:
            return w_q.at[:, pl.ds(pl.multiple_of(c * half_cols + ci * WCOLS, WCOLS), WCOLS)]
        if ci == 4:
            return w_k.at[:, pl.ds(pl.multiple_of(c * WCOLS, WCOLS), WCOLS)]
        if ci == 5:
            return w_v.at[:, pl.ds(pl.multiple_of(c * WCOLS, WCOLS), WCOLS)]
        return w_o.at[:, pl.ds(pl.multiple_of(c * half_cols + (ci - 6) * WCOLS, WCOLS), WCOLS)]

    def wcopy(ci):
        return pltpu.make_async_copy(wsrc(ci), wring.at[ci % 4], wsem.at[ci])

    smalls = [(x_first, xin.at[0]), (next_emb, xin.at[pl.ds(1, S - 1)]), (g1, vg1), (c1, vc1), (b_q, vbq), (b_k, vbk), (b_v, vbv),
              (lf, vlf), (pw, vpw), (lens_h, lens_ref), (g2, vg2), (c2, vc2), (b_o, vbo), (w_r, vwr), (ei_h, ei_ref), (rm_h, rm_ref)]
    small_copies = [pltpu.make_async_copy(a, b, ssem.at[i]) for i, (a, b) in enumerate(smalls)]
    for cp in small_copies[:10]:
        cp.start()
    for ci in range(4):
        wcopy(ci).start()
    for cp in small_copies[10:]:
        cp.start()

    def kcopy(b):
        return pltpu.make_async_copy(k_hbm.at[b], kbuf.at[b], ksem.at[b])

    def vcopy(b):
        return pltpu.make_async_copy(v_hbm.at[b], vbuf.at[b], vsem.at[b])

    moe_copies = [pltpu.make_async_copy(src, wmoe.at[i, pl.ds(0, FE)], msem.at[i]) for i, src in enumerate((w_g, w_u, w_d))]

    wmoe[2, FE:FEP, :] = jnp.zeros((FEP - FE, D), BF16)
    lhs[...] = jnp.zeros_like(lhs)
    gs[...] = jnp.zeros_like(gs)
    ut[...] = jnp.zeros_like(ut)
    tkv[...] = jnp.zeros_like(tkv)

    def layer_norm(s, gain, bias):
        x = x32[s * B:(s + 1) * B, :]
        mean = jnp.sum(x, axis=1, keepdims=True) / D
        cen = x - mean
        var = jnp.sum(cen * cen, axis=1, keepdims=True) / D
        h[s * B:(s + 1) * B, :] = (cen * lax.rsqrt(var + NORM_EPS) * gain[...] + bias[...]).astype(BF16)

    for cp in small_copies[:10]:
        cp.wait()
    for s in range(S):
        x32[s * B:(s + 1) * B, :] = xin[s].astype(F32)
        layer_norm(s, vg1, vc1)
    hd2 = HD // 2
    row_b = lax.rem(iota((R, hd2), 0), B)
    pos = iota((R, hd2), 0) // B
    for b in range(B):
        pos = pos + jnp.where(row_b == b, lens_ref[b], 0)
    ang = pos.astype(F32) * (1.0 / (vlf[...] * vpw[...]))
    cs = jnp.cos(ang) * ROPE_MSCALE
    sn = jnp.sin(ang) * ROPE_MSCALE
    cosb[:, 0:hd2] = cs
    cosb[:, hd2:HD] = cs
    sinb[:, 0:hd2] = -sn
    sinb[:, hd2:HD] = sn
    kr, kl = iota((CORES * QR, LANES), 0), iota((CORES * QR, LANES), 1)
    kbias[...] = jnp.where((kr // QR) * KHH + lax.rem(kr, HH) // QG == lax.rem(kl, KH), 0.0, NEG_FILL)

    def rotate(x):
        return round_bf16(x * cosb[...] + pltpu.roll(x, HD // 2, 1) * sinb[...])

    def q_chunk(ci, _):
        pltpu.make_async_copy(wsrc(0), wring.at[ci], wsem.at[ci]).wait()
        off = pl.multiple_of(c * half_cols + ci * WCOLS, WCOLS)
        y = jnp.dot(h[...], wring[ci], preferred_element_type=F32) + vbq[:, pl.ds(off, WCOLS)]
        y = round_bf16(y)
        for t in range(WCOLS // HD):
            r = rotate(y[:, t * HD:(t + 1) * HD])
            hh = ci * (WCOLS // HD) + t
            for s in range(S):
                qbuf[c, pl.ds(s * HH + hh, B, stride=QR), :] = r[s * B:(s + 1) * B, :]

        @pl.when(ci == 0)
        def _():
            wcopy(4).start()

        @pl.when(ci == 1)
        def _():
            wcopy(5).start()

            def kv_start(j, _):
                b = nth(j)
                kcopy(b).start()
                vcopy(b).start()
                return 0
            lax.fori_loop(0, B, kv_start, 0)

        @pl.when(ci == 2)
        def _():
            wcopy(6).start()

        @pl.when(ci == 3)
        def _():
            wcopy(7).start()
        return 0
    lax.fori_loop(0, 4, q_chunk, 0)

    pl.semaphore_wait(bar, chips)

    def to_partner(src, dst, ss, rs):
        return pltpu.make_async_remote_copy(src, dst, ss, rs, device_id={"kv": partner}, device_id_type=MESH)

    q_x = to_partner(qbuf.at[c], qbuf.at[c], qx_s, qx_r)
    q_x.start()

    wcopy(4).wait()
    y = round_bf16(jnp.dot(h[...], wring[0], preferred_element_type=F32) + vbk[:, pl.ds(pl.multiple_of(c * WCOLS, WCOLS), WCOLS)])
    for t in range(KHH):
        kt[c, t, :, :] = rotate(y[:, t * HD:(t + 1) * HD])
    wcopy(8).start()
    wcopy(5).wait()
    y = round_bf16(jnp.dot(h[...], wring[1], preferred_element_type=F32) + vbv[:, pl.ds(pl.multiple_of(c * WCOLS, WCOLS), WCOLS)])
    for t in range(KHH):
        vt[c, t, :, :] = y[:, t * HD:(t + 1) * HD]
    wcopy(9).start()
    for cp in moe_copies:
        cp.start()
    k_x = to_partner(kt.at[c], kt.at[c], kx_s, kx_r)
    v_x = to_partner(vt.at[c], vt.at[c], vx_s, vx_r)
    k_x.start()
    v_x.start()

    q_x.wait_recv()
    AR = CORES * QR
    NK = T * KH
    fac = scale * math.log2(math.e)
    lane = iota((AR, LANES), 1)

    def o_copy(b):
        return pltpu.make_async_remote_copy(osend.at[b], orecv.at[chip], os_s.at[b], os_r.at[chip],
                                            device_id={"kv": peer(b)}, device_id_type=MESH)

    def p_copy(b):
        return to_partner(part.at[1 - c, b], precv.at[b], ps_s.at[b], ps_r.at[b])

    def pair_combine(b, dst, di):
        p_copy(b).wait_recv()
        m1, l1 = part[c, b, QR:QR + 1, :], part[c, b, QR + 1:QR + 2, :]
        m2, l2 = precv[b, QR:QR + 1, :], precv[b, QR + 1:QR + 2, :]
        top = jnp.maximum(m1, m2)
        f1, f2 = jnp.exp(m1 - top), jnp.exp(m2 - top)
        dst[di, 0:QR, :] = part[c, b, 0:QR, :] * to_col(f1, QR) + precv[b, 0:QR, :] * to_col(f2, QR)
        dst[di, QR:MR, :] = stat_tile(top, l1 * f1 + l2 * f2)

    def scores(b, u):
        lim = (lens_ref[b] - me * T) * KH
        q0 = qbuf[0, pl.ds(pl.multiple_of(b * QR, QR), QR), :]
        q1 = qbuf[1, pl.ds(pl.multiple_of(b * QR, QR), QR), :]
        qb = jnp.concatenate([q0, q1], axis=0).astype(BF16)
        mx = jnp.full((AR, LANES), NEG_FILL, F32)
        for col in range(NK // 256):
            x = lax.dot_general(qb, kbuf[b, col * 256:(col + 1) * 256, :], NT, preferred_element_type=F32)
            for hc in range(256 // LANES):
                lo = col * 256 + hc * LANES
                xx = jnp.where(lane < lim - lo, x[:, hc * LANES:(hc + 1) * LANES] + kbias[...], NEG_FILL)
                sbuf[u, :, lo:lo + LANES] = xx
                mx = jnp.maximum(mx, xx)
        m = jnp.max(mx, axis=1, keepdims=True)
        mu = jnp.where(lim > 0, m, 0.0)
        return m, mu

    def weigh(b, u, m, mu):
        mub = jnp.broadcast_to(mu, (AR, LANES))
        tot = jnp.zeros((AR, LANES), F32)
        for lo in range(0, NK, LANES):
            w = jnp.exp2((sbuf[u, :, lo:lo + LANES] - mub) * fac)
            tot = tot + w
            wbuf[u, :, lo:lo + LANES] = w.astype(BF16)
        l = jnp.sum(tot, axis=1, keepdims=True)
        o = jnp.dot(wbuf[u], vbuf[b], preferred_element_type=F32)
        ms = m * scale
        for hf in range(CORES):
            part[hf, b, 0:QR, :] = o[hf * QR:(hf + 1) * QR, :]
            part[hf, b, QR:MR, :] = stat_tile(to_row(ms[hf * QR:(hf + 1) * QR, :]), to_row(l[hf * QR:(hf + 1) * QR, :]))

    def attn2(jj):
        bs = [nth(jj * 2 + u) for u in range(2)]
        for b in bs:
            kcopy(b).wait()
            vcopy(b).wait()
        st = [scores(b, u) for u, b in enumerate(bs)]
        for u, b in enumerate(bs):
            weigh(b, u, *st[u])
        for b in bs:
            p_copy(b).start()

    def comb(b):
        pair_combine(b, osend, b)
        o_copy(b).start()

    attn2(0)

    def attn_step(jj, _):
        attn2(jj)
        comb(nth(jj * 2 - 2))
        comb(nth(jj * 2 - 1))
        return 0
    lax.fori_loop(1, B // 2, attn_step, 0)
    comb(nth(B - 2))
    pair_combine(chip, orecv, chip)

    for s in range(S):
        for t in range(KHH):
            tkv[0, s * KHH + t:s * KHH + t + 1, :] = kt[c, t, pl.ds(s * B + chip, 1), :]
            tkv[1, s * KHH + t:s * KHH + t + 1, :] = vt[c, t, pl.ds(s * B + chip, 1), :]
    TR = tkv.shape[1]
    qb = qbuf[c, pl.ds(pl.multiple_of(chip * QR, QR), QR), :].astype(BF16)
    sc = lax.dot_general(qb, tkv[0].astype(BF16), NT, preferred_element_type=F32)
    tr, tl = iota((QR, TR), 0), iota((QR, TR), 1)
    valid = (lax.rem(tl, KHH) == lax.rem(tr, HH) // QG) & (tl // KHH <= tr // HH) & (tl < S * KHH)
    m, l, w = softmax_part(sc, valid, scale)
    orecv[chips, 0:QR, :] = jnp.dot(w, tkv[1].astype(BF16), preferred_element_type=F32)
    orecv[chips, QR:MR, :] = stat_tile(to_row(m), to_row(l))

    def o_wait(i, _):
        src = lax.rem(chip + i, chips)
        pltpu.make_async_remote_copy(osend.at[0], orecv.at[src], os_s.at[0], os_r.at[src],
                                     device_id={"kv": peer(src)}, device_id_type=MESH).wait_recv()
        return 0
    lax.fori_loop(1, chips, o_wait, 0)

    top = orecv[0, QR:QR + 1, :]
    for i in range(1, chips + 1):
        top = jnp.maximum(top, orecv[i, QR:QR + 1, :])
    tot = jnp.zeros((1, LANES), F32)
    acc = jnp.zeros((QR, LANES), F32)
    for i in range(chips + 1):
        f = jnp.exp(orecv[i, QR:QR + 1, :] - top)
        tot = tot + orecv[i, QR + 1:QR + 2, :] * f
        acc = acc + orecv[i, 0:QR, :] * to_col(f, QR)
    oxs[c, :, :] = round_bf16(acc / to_col(tot, QR))
    o_x = to_partner(oxs.at[c], oxs.at[c], ox_s, ox_r)
    o_x.start()
    for cp in small_copies[10:]:
        cp.wait()

    ctiles = WCOLS // LANES
    my_slot = pl.multiple_of(me * QR, QR)
    KROWS = HH * HD

    def fill(hf):
        for hh in range(HH):
            lhs[hf, 0:S, hh * HD:(hh + 1) * HD] = oxs[hf, pl.ds(hh, S, stride=HH), :]

    def wo_dot(hf, jn):
        return jnp.dot(lhs[hf].astype(BF16), wring[lax.rem(jn + 2, 4), pl.ds(pl.multiple_of(hf * KROWS, KROWS), KROWS), :], preferred_element_type=F32)

    fill(c)

    def wo_mine(jn, _):
        pltpu.make_async_copy(wsrc(0), wring.at[lax.rem(jn + 2, 4)], wsem.at[jn + 6]).wait()
        wacc[jn, :, :] = wo_dot(c, jn)
        return 0
    lax.fori_loop(0, 4, wo_mine, 0)
    o_x.wait_recv()
    fill(1 - c)

    def gatherer(buf, pieces, ss, rs, fs):
        PR = QR // pieces

        def cp(p, slot, sem, dev):
            blk = buf.at[pl.ds(pl.multiple_of(slot * QR + p * PR, 8), PR)]
            return pltpu.make_async_remote_copy(blk, blk, sem, rs.at[p, slot], device_id={"kv": dev}, device_id_type=MESH)

        def send(p):
            for i, o in enumerate(offsets):
                cp(p, me, ss.at[p, i], peer(ahead(o))).start()
            cp(p, me, ss.at[p, len(offsets)], partner).start()

        def finish():
            for p in range(pieces):
                for i, o in enumerate(offsets):
                    slot = peer(behind(o))
                    cp(p, slot, ss.at[p, i], partner).wait_recv()
                    cp(p, slot, fs.at[p, i], partner).start()
            for p in range(pieces):
                cp(p, partner, ss.at[p, 0], partner).wait_recv()
                for i, o in enumerate(offsets):
                    cp(p, behind(o) * CORES + (1 - c), ss.at[p, i], partner).wait_recv()

        def drain():
            for p in range(pieces):
                cp(p, me, ss.at[p, len(offsets)], partner).wait_send()
                for i in range(len(offsets)):
                    cp(p, me, ss.at[p, i], partner).wait_send()
                    cp(p, me, fs.at[p, i], partner).wait_send()
        return send, finish, drain

    XP = 2
    XPR = QR // XP
    XT = HH // XP
    x_send, x_finish, x_drain = gatherer(xg, XP, xa_s, xa_r, xf_s)
    for p in range(XP):
        def wo_other(k, _):
            jn = p * (4 // XP) + k
            off = pl.multiple_of(c * half_cols + jn * WCOLS, WCOLS)
            d = wacc[jn] + wo_dot(1 - c, jn)
            for s in range(S):
                v = round_bf16(x32[pl.ds(s * B + chip, 1), pl.ds(off, WCOLS)] + d[s:s + 1, :] + vbo[:, pl.ds(off, WCOLS)])
                for t in range(ctiles):
                    xg[pl.ds(my_slot + p * XPR + s * XT + k * ctiles + t, 1), :] = v[:, t * LANES:(t + 1) * LANES]
            return 0
        lax.fori_loop(0, 4 // XP, wo_other, 0)
        x_send(p)
    x_finish()
    for s in range(S):
        for hf in range(CORES):
            for t in range(HH):
                x32[s * B:(s + 1) * B, (hf * HH + t) * LANES:(hf * HH + t + 1) * LANES] = xg[pl.ds(hf * QR + (t // XT) * XPR + s * XT + t % XT, B, stride=CORES * QR), :]

    for s in range(S):
        layer_norm(s, vg2, vc2)
    logits = lax.dot_general(h[...], vwr[...], NT, preferred_element_type=F32)
    le = iota((B, E), 1)
    diag = iota((B, B), 0) == iota((B, B), 1)
    for s in range(S):
        lg = logits[s * B:(s + 1) * B, :]
        gate = jnp.zeros((B, E), F32)
        for k in range(ei_ref.shape[1]):
            masked = jnp.where(rm_ref[s, :, k, :] == 1, lg, NEG_FILL)
            ex = jnp.exp(masked - jnp.max(masked, axis=1, keepdims=True))
            p = ex / jnp.sum(ex, axis=1, keepdims=True)
            idx = jnp.sum(jnp.where(diag, jnp.broadcast_to(ei_ref[s, k:k + 1, :], (B, B)).astype(F32), 0.0), axis=1, keepdims=True)
            gate = gate + jnp.where(le.astype(F32) == idx, p, 0.0)
        gs[s * B:(s + 1) * B, 0:E] = gate
    gt[...] = jnp.transpose(gs[...])
    g_e = jnp.concatenate([gt[0:E, :]] * (LANES // E), axis=0)[:, 0:R]
    moe_copies[0].wait()
    moe_copies[1].wait()
    UB = 256
    for t in range(FEP // UB):
        ag = lax.dot_general(wmoe[0, t * UB:(t + 1) * UB, :], h[...], NT, preferred_element_type=F32)
        au = lax.dot_general(wmoe[1, t * UB:(t + 1) * UB, :], h[...], NT, preferred_element_type=F32)
        gg = jnp.concatenate([g_e] * (UB // LANES), axis=0)
        u = gg * (ag * jax.nn.sigmoid(ag)) * au
        ut[t * UB:(t + 1) * UB, 0:R] = jnp.where(iota((UB, R), 0) + t * UB < FE, u, 0.0)
    for t in range(FEP // LANES):
        ub[:, t * LANES:(t + 1) * LANES] = jnp.transpose(ut[t * LANES:(t + 1) * LANES, :])[0:R, :].astype(BF16)
    moe_copies[2].wait()

    def mo_copy(i):
        return pltpu.make_async_remote_copy(mosend.at[i], morecv.at[chip], mo_s.at[i], mo_r.at[chip],
                                            device_id={"kv": peer(i)}, device_id_type=MESH)

    def moe_pair(i, dst, di):
        to_partner(mpsend.at[i], mprecv.at[i], mp_s.at[i], mp_r.at[i]).wait_recv()
        dst[di, :, :] = mine[i] + mprecv[i]

    def moe_step(j, _):
        i = nth(j)
        pp = round_bf16(jnp.dot(ub[...], wmoe[2, :, pl.ds(pl.multiple_of(i * PC, PC), PC)], preferred_element_type=F32))
        p0, p1 = pp[:, :LANES], pp[:, LANES:]
        mpsend[i, :, :] = jnp.where(c == 0, p1, p0)
        mine[i, :, :] = jnp.where(c == 0, p0, p1)
        to_partner(mpsend.at[i], mprecv.at[i], mp_s.at[i], mp_r.at[i]).start()
        return 0
    lax.fori_loop(0, chips, moe_step, 0)

    def moe_fwd(j, _):
        i = nth(j)
        moe_pair(i, mosend, i)
        mo_copy(i).start()
        return 0
    lax.fori_loop(0, chips - 1, moe_fwd, 0)
    moe_pair(chip, morecv, chip)

    k_x.wait_recv()
    v_x.wait_recv()
    for src, dst in ((kt, tk_ref), (vt, tv_ref)):
        for hf in range(CORES):
            for t in range(KHH):
                for s in range(S):
                    t32[pl.ds(s * KH + hf * KHH + t, B, stride=S * KH), :] = src[hf, t, s * B:(s + 1) * B, :]
        dst[...] = t32[...].astype(BF16)

    def mo_wait(i, _):
        src = lax.rem(chip + chips - i, chips)
        pltpu.make_async_remote_copy(mosend.at[0], morecv.at[src], mo_s.at[0], mo_r.at[src],
                                     device_id={"kv": peer(src)}, device_id_type=MESH).wait_recv()
        return 0
    lax.fori_loop(1, chips, mo_wait, 0)
    tot = morecv[0]
    for i in range(1, chips):
        tot = tot + morecv[i]
    yg[pl.ds(my_slot, QR), :] = round_bf16(x32[:, pl.ds(pl.multiple_of(me * LANES, LANES), LANES)] + tot)
    y_send, y_finish, y_drain = gatherer(yg, 1, ya_s, ya_r, yf_s)
    y_send(0)
    y_finish()
    for d in range(chips * CORES):
        for s in range(S):
            out_ref[s, :, d * LANES:(d + 1) * LANES] = yg[d * QR + s * B:d * QR + (s + 1) * B, :].astype(BF16)

    q_x.wait_send()
    k_x.wait_send()
    v_x.wait_send()
    o_x.wait_send()

    def drain(i, _):
        b = lax.rem(chip + i, chips)
        p_copy(b).wait_send()
        to_partner(mpsend.at[b], mprecv.at[b], mp_s.at[b], mp_r.at[b]).wait_send()

        @pl.when(i > 0)
        def _():
            o_copy(b).wait_send()
            mo_copy(b).wait_send()
        return 0
    lax.fori_loop(0, chips, drain, 0)
    x_drain()
    y_drain()


def copy_out(a, b, d, oa, ob, od, sem):
    cps = [pltpu.make_async_copy(x, y, sem.at[i]) for i, (x, y) in enumerate(((a, oa), (b, ob), (d, od)))]
    for cp in cps:
        cp.start()
    for cp in cps:
        cp.wait()


def finish(*arrs):
    return pl.pallas_call(
        copy_out,
        name="copy_out",
        out_shape=tuple(jax.ShapeDtypeStruct(a.shape, a.dtype) for a in arrs),
        in_specs=[pl.BlockSpec(memory_space=pltpu.VMEM)] * len(arrs),
        out_specs=(pl.BlockSpec(memory_space=pl.ANY),) * len(arrs),
        scratch_shapes=[pltpu.SemaphoreType.DMA((len(arrs),))],
        compiler_params=pltpu.CompilerParams(vmem_limit_bytes=1 << 20),
    )(*arrs)


def solution(mesh):
    n = mesh.shape["kv"]
    chips = n // CORES

    def layer_steps(x_first, next_emb, k_cache, v_cache, seq_len, ln1_gain, ln1_bias, w_q, b_q, w_k, b_k, w_v, b_v, w_o, b_o, ln2_gain, ln2_bias, w_router, w_gate, w_up, w_down, long_factor, expert_idx, route_mask):
        B, T, KH, HD = k_cache.shape
        D = x_first.shape[1]
        H = w_q.shape[1] // HD
        S = next_emb.shape[0] + 1
        E = w_router.shape[1]
        FE = w_gate.shape[0] * w_gate.shape[2]
        FEP = -(-FE // 256) * 256
        R = S * B
        HH, KHH = H // CORES, KH // CORES
        QR = S * HH
        MR = QR + 8
        if B != chips or D != n * LANES or w_q.shape[1] != D or QR != R:
            raise ValueError("unsupported sizes")
        dims = dict(S=S, B=B, D=D, T=T, KH=KH, HD=HD, H=H, E=E, FE=FE, chips=chips)
        half = HD // 2
        power = np.float32(ROPE_BASE) ** (np.arange(half, dtype=np.float32) * np.float32(2.0) / np.float32(HD))
        pw = jnp.asarray(power[None, :].astype(np.float32))
        lf = long_factor[None, :]
        row = lambda a: a.reshape(1, -1)
        args = (seq_len, expert_idx.transpose(0, 2, 1), route_mask,
                x_first, next_emb, k_cache.reshape(B, T * KH, HD), v_cache.reshape(B, T * KH, HD), row(ln1_gain), row(ln1_bias),
                w_q, row(b_q), w_k, row(b_k), w_v, row(b_v), w_o, row(b_o), row(ln2_gain), row(ln2_bias), w_router.T,
                w_gate.transpose(2, 0, 1).reshape(FE, D), w_up.transpose(2, 0, 1).reshape(FE, D), w_down.transpose(1, 0, 2).reshape(FE, D), lf, pw)
        V = pltpu.VMEM
        DS = pltpu.SemaphoreType.DMA
        scratch = [
            pltpu.SMEM((B,), jnp.int32), V(expert_idx.transpose(0, 2, 1).shape, jnp.int32), V(route_mask.shape, jnp.int32),
            V((4, D, WCOLS), BF16), V((B, T * KH, HD), BF16), V((B, T * KH, HD), BF16), V((3, FEP, D), BF16),
            V((S, B, D), BF16), V((R, D), F32), V((R, D), BF16),
            V((1, D), F32), V((1, D), F32), V((1, D), F32), V((1, D), F32), V((1, D), F32), V((1, w_q.shape[1]), F32),
            V((1, w_k.shape[1]), F32), V((1, w_v.shape[1]), F32), V((1, half), F32), V((1, half), F32), V((E, D), BF16),
            V((CORES, B * QR, HD), F32), V((R, HD), F32), V((R, HD), F32), V((CORES, KHH, R, HD), F32), V((CORES, KHH, R, HD), F32), V((2, 16, HD), F32),
            V((CORES * QR, LANES), F32), V((2, CORES * QR, T * KH), F32), V((2, CORES * QR, T * KH), BF16),
            V((CORES, B, MR, HD), F32), V((B, MR, HD), F32), V((B, MR, HD), F32), V((chips + 1, MR, HD), F32),
            V((CORES, QR, HD), F32), V((CORES, 8, HH * HD), F32), V((4, 8, WCOLS), F32), V((n * QR, HD), F32), V((LANES, LANES), F32), V((LANES, LANES), F32), V((FEP, LANES), F32), V((R, FEP), BF16),
            V((chips, R, LANES), F32), V((chips, R, LANES), F32), V((chips, R, LANES), F32), V((chips, R, LANES), F32), V((chips, R, LANES), F32),
            V((n * QR, LANES), F32), V((B * S * KH, HD), F32),
            DS((10,)), DS((B,)), DS((B,)), DS((3,)), DS((16,)), DS, DS, DS, DS, DS, DS, DS((B,)), DS((B,)), DS((chips,)), DS((chips,)), DS, DS,
            DS((2, chips)), DS((2, n)), DS((2, chips)), DS((chips,)), DS((chips,)), DS((chips,)), DS((chips,)), DS((1, chips)), DS((1, n)), DS((1, chips)),
        ]
        vm = pl.BlockSpec(memory_space=pltpu.VMEM)
        anys = pl.BlockSpec(memory_space=pl.ANY)
        hidden, tk, tv = pl.pallas_call(
            functools.partial(kernel, dims),
            name="decode_layer",
            out_shape=(jax.ShapeDtypeStruct((S, B, D), BF16), jax.ShapeDtypeStruct((B * S * KH, HD), BF16), jax.ShapeDtypeStruct((B * S * KH, HD), BF16)),
            in_specs=[anys] * len(args),
            out_specs=(vm, vm, vm),
            scratch_shapes=scratch,
            compiler_params=pltpu.CompilerParams(collective_id=0, has_side_effects=True, vmem_limit_bytes=VMEM_BYTES),
        )(*args)
        hidden, tk, tv = finish(hidden, tk, tv)
        return hidden, tk.reshape(B, S, KH, HD), tv.reshape(B, S, KH, HD)

    replicated = P()
    in_specs = (P('dp'), P(None, 'dp'), P('dp', 'kv'), P('dp', 'kv'), P('dp')) + (replicated,) * 13 + (P(None, None, 'kv'), P(None, None, 'kv'), P(None, 'kv'), replicated, P(None, 'dp'), P(None, 'dp'))
    out_specs = (P(None, 'dp'), P('dp'), P('dp'))
    return jax.shard_map(layer_steps, mesh=mesh, in_specs=in_specs, out_specs=out_specs, check_vma=False)
```

```python
import functools
import math

import jax
import jax.numpy as jnp
import numpy as np
from jax import lax
from jax.experimental import pallas as pl
from jax.experimental.pallas import tpu as pltpu
from jax.sharding import PartitionSpec as P

ROPE_BASE = 10000.0
ROPE_MSCALE = math.sqrt(1.0 + math.log(32.0) / math.log(4096.0))
NORM_EPS = 1e-5
NEG_FILL = -1e30
MESH = pl.DeviceIdType.MESH
F32 = jnp.float32
BF16 = jnp.bfloat16
LANES = 128
WCOLS = 512
CORES = 2
VMEM_BYTES = 64 * 1024 * 1024 - 4 * 1024 * 1024
NT = (((1,), (1,)), ((), ()))


def iota(shape, dim):
    return lax.broadcasted_iota(jnp.int32, shape, dim)


def to_row(col):
    rows = col.shape[0]
    pick = iota((rows, LANES), 0) == iota((rows, LANES), 1)
    return jnp.sum(jnp.where(pick, jnp.broadcast_to(col, (rows, LANES)), 0.0), axis=0, keepdims=True)


def full_row(full):
    rows = full.shape[0]
    pick = iota((rows, LANES), 0) == iota((rows, LANES), 1)
    return jnp.sum(jnp.where(pick, full, 0.0), axis=0, keepdims=True)


def to_col(row, rows):
    pick = iota((rows, LANES), 0) == iota((rows, LANES), 1)
    return jnp.sum(jnp.where(pick, jnp.broadcast_to(row, (rows, LANES)), 0.0), axis=1, keepdims=True)


def stat_tile(m_row, l_row):
    r = iota((8, LANES), 0)
    return jnp.where(r == 0, jnp.broadcast_to(m_row, (8, LANES)), jnp.where(r == 1, jnp.broadcast_to(l_row, (8, LANES)), 0.0))


def softmax_part(s_raw, valid, scale):
    s = jnp.where(valid, s_raw * scale, NEG_FILL)
    m = jnp.max(s, axis=1, keepdims=True)
    w = jnp.where(valid, jnp.exp(s - m), 0.0)
    return m, jnp.sum(w, axis=1, keepdims=True), w.astype(BF16)


def round_bf16(x):
    return x.astype(BF16).astype(F32)


def kernel(dims, lens_h, ei_h, rm_h,
           x_first, next_emb, k_hbm, v_hbm, g1, c1, w_q, b_q, w_k, b_k, w_v, b_v, w_o, b_o, g2, c2, w_r, w_g, w_u, w_d, lf, pw,
           out_ref, tk_ref, tv_ref,
           lens_ref, ei_ref, rm_ref, wring, kbuf, vbuf, wmoe, xin, x32, h, vg1, vc1, vg2, vc2, vbo, vbq, vbk, vbv, vlf, vpw, vwr,
           qbuf, cosb, sinb, kt, vt, tkv, kbias, sbuf, mbuf, wbuf, part, precv, osend, orecv, oxs, lhs, wacc, xg, gs, gt, ut, ub, mine, mpsend, mprecv, mosend, morecv, yg, t32,
           wsem, ksem, vsem, msem, ssem, qx_s, qx_r, kx_s, kx_r, vx_s, vx_r, ps_s, ps_r, os_s, os_r, ox_s, ox_r,
           xa_s, xa_r, xf_s, mp_s, mp_r, mo_s, mo_r, ya_s, ya_r, yf_s):
    S, B, D, T, KH, HD, H, E, FE, chips = (dims[k] for k in ("S", "B", "D", "T", "KH", "HD", "H", "E", "FE", "chips"))
    R = S * B
    HH, KHH = H // CORES, KH // CORES
    half_cols = D // CORES
    QG = H // KH
    QR = S * HH
    MR = QR + 8
    PC = LANES * CORES
    FEP = wmoe.shape[1]
    scale = HD ** -0.5
    me = lax.axis_index("kv")
    chip = me // CORES
    c = lax.rem(me, CORES)
    partner = chip * CORES + (1 - c)

    def peer(ch):
        return ch * CORES + c

    side = math.isqrt(chips)
    cy, cx = chip // side, lax.rem(chip, side)

    def ring(k):
        return side // 2 + ((k + 1) // 2) * (1 - 2 * (k % 2))

    def nth(j):
        return lax.rem(cy + ring(j // side), side) * side + lax.rem(cx + ring(lax.rem(j, side)), side)

    def dist(d):
        return min(d, side - d)
    offsets = sorted([(dy, dx) for dy in range(side) for dx in range(side) if dy or dx], key=lambda o: -(dist(o[0]) + dist(o[1])))

    def ahead(o):
        return lax.rem(cy + o[0], side) * side + lax.rem(cx + o[1], side)

    def behind(o):
        return lax.rem(cy + side - o[0], side) * side + lax.rem(cx + side - o[1], side)

    bar = pltpu.get_barrier_semaphore()
    pl.semaphore_signal(bar, inc=1, device_id={"kv": partner}, device_id_type=MESH)

    def sig(i, _):
        pl.semaphore_signal(bar, inc=1, device_id={"kv": peer(lax.rem(chip + i, chips))}, device_id_type=MESH)
        return 0
    lax.fori_loop(1, chips, sig, 0)

    def wsrc(ci):
        if ci < 4:
            return w_q.at[:, pl.ds(pl.multiple_of(c * half_cols + ci * WCOLS, WCOLS), WCOLS)]
        if ci == 4:
            return w_k.at[:, pl.ds(pl.multiple_of(c * WCOLS, WCOLS), WCOLS)]
        if ci == 5:
            return w_v.at[:, pl.ds(pl.multiple_of(c * WCOLS, WCOLS), WCOLS)]
        return w_o.at[:, pl.ds(pl.multiple_of(c * half_cols + (ci - 6) * WCOLS, WCOLS), WCOLS)]

    def wcopy(ci):
        return pltpu.make_async_copy(wsrc(ci), wring.at[ci % 4], wsem.at[ci])

    smalls = [(x_first, xin.at[0]), (next_emb, xin.at[pl.ds(1, S - 1)]), (g1, vg1), (c1, vc1), (b_q, vbq), (b_k, vbk), (b_v, vbv),
              (lf, vlf), (pw, vpw), (lens_h, lens_ref), (g2, vg2), (c2, vc2), (b_o, vbo), (w_r, vwr), (ei_h, ei_ref), (rm_h, rm_ref)]
    small_copies = [pltpu.make_async_copy(a, b, ssem.at[i]) for i, (a, b) in enumerate(smalls)]
    for cp in small_copies[:10]:
        cp.start()
    for ci in range(4):
        wcopy(ci).start()
    for cp in small_copies[10:]:
        cp.start()

    def kcopy(b):
        return pltpu.make_async_copy(k_hbm.at[b], kbuf.at[b], ksem.at[b])

    def vcopy(b):
        return pltpu.make_async_copy(v_hbm.at[b], vbuf.at[b], vsem.at[b])

    moe_copies = [pltpu.make_async_copy(src, wmoe.at[i, pl.ds(0, FE)], msem.at[i]) for i, src in enumerate((w_g, w_u, w_d))]

    wmoe[2, FE:FEP, :] = jnp.zeros((FEP - FE, D), BF16)
    lhs[...] = jnp.zeros_like(lhs)
    gs[...] = jnp.zeros_like(gs)
    ut[...] = jnp.zeros_like(ut)
    tkv[...] = jnp.zeros_like(tkv)

    def layer_norm(s, gain, bias):
        x = x32[s * B:(s + 1) * B, :]
        mean = jnp.sum(x, axis=1, keepdims=True) / D
        cen = x - mean
        var = jnp.sum(cen * cen, axis=1, keepdims=True) / D
        h[s * B:(s + 1) * B, :] = (cen * lax.rsqrt(var + NORM_EPS) * gain[...] + bias[...]).astype(BF16)

    for cp in small_copies[:10]:
        cp.wait()
    for s in range(S):
        x32[s * B:(s + 1) * B, :] = xin[s].astype(F32)
        layer_norm(s, vg1, vc1)
    hd2 = HD // 2
    row_b = lax.rem(iota((R, hd2), 0), B)
    pos = iota((R, hd2), 0) // B
    for b in range(B):
        pos = pos + jnp.where(row_b == b, lens_ref[b], 0)
    ang = pos.astype(F32) * (1.0 / (vlf[...] * vpw[...]))
    cs = jnp.cos(ang) * ROPE_MSCALE
    sn = jnp.sin(ang) * ROPE_MSCALE
    cosb[:, 0:hd2] = cs
    cosb[:, hd2:HD] = cs
    sinb[:, 0:hd2] = -sn
    sinb[:, hd2:HD] = sn
    kr, kl = iota((CORES * QR, LANES), 0), iota((CORES * QR, LANES), 1)
    kbias[...] = jnp.where((kr // QR) * KHH + lax.rem(kr, HH) // QG == lax.rem(kl, KH), 0.0, NEG_FILL)

    def rotate(x):
        return round_bf16(x * cosb[...] + pltpu.roll(x, HD // 2, 1) * sinb[...])

    def kv_start(j, _):
        b = nth(j)
        kcopy(b).start()
        vcopy(b).start()
        return 0

    def q_chunk(ci, _):
        pltpu.make_async_copy(wsrc(0), wring.at[ci], wsem.at[ci]).wait()
        off = pl.multiple_of(c * half_cols + ci * WCOLS, WCOLS)
        y = jnp.dot(h[...], wring[ci], preferred_element_type=F32) + vbq[:, pl.ds(off, WCOLS)]
        y = round_bf16(y)
        for t in range(WCOLS // HD):
            r = rotate(y[:, t * HD:(t + 1) * HD])
            hh = ci * (WCOLS // HD) + t
            for s in range(S):
                qbuf[c, pl.ds(s * HH + hh, B, stride=QR), :] = r[s * B:(s + 1) * B, :]

        @pl.when(ci == 0)
        def _():
            wcopy(4).start()

        @pl.when(ci == 1)
        def _():
            wcopy(5).start()

        @pl.when(ci == 2)
        def _():
            lax.fori_loop(0, B // 2, kv_start, 0)

        @pl.when(ci == 3)
        def _():
            lax.fori_loop(B // 2, B, kv_start, 0)
        return 0
    lax.fori_loop(0, 4, q_chunk, 0)

    pl.semaphore_wait(bar, chips)

    def to_partner(src, dst, ss, rs):
        return pltpu.make_async_remote_copy(src, dst, ss, rs, device_id={"kv": partner}, device_id_type=MESH)

    q_x = to_partner(qbuf.at[c], qbuf.at[c], qx_s, qx_r)
    q_x.start()

    wcopy(4).wait()
    y = round_bf16(jnp.dot(h[...], wring[0], preferred_element_type=F32) + vbk[:, pl.ds(pl.multiple_of(c * WCOLS, WCOLS), WCOLS)])
    for t in range(KHH):
        kt[c, t, :, :] = rotate(y[:, t * HD:(t + 1) * HD])
    wcopy(5).wait()
    y = round_bf16(jnp.dot(h[...], wring[1], preferred_element_type=F32) + vbv[:, pl.ds(pl.multiple_of(c * WCOLS, WCOLS), WCOLS)])
    for t in range(KHH):
        vt[c, t, :, :] = y[:, t * HD:(t + 1) * HD]
    k_x = to_partner(kt.at[c], kt.at[c], kx_s, kx_r)
    v_x = to_partner(vt.at[c], vt.at[c], vx_s, vx_r)
    k_x.start()
    v_x.start()

    q_x.wait_recv()
    AR = CORES * QR
    NK = T * KH
    fac = scale * math.log2(math.e)
    lane = iota((AR, LANES), 1)

    def o_copy(b):
        return pltpu.make_async_remote_copy(osend.at[b], orecv.at[chip], os_s.at[b], os_r.at[chip],
                                            device_id={"kv": peer(b)}, device_id_type=MESH)

    def p_copy(b):
        return to_partner(part.at[1 - c, b], precv.at[b], ps_s.at[b], ps_r.at[b])

    def pair_combine(b, dst, di):
        p_copy(b).wait_recv()
        m1, l1 = part[c, b, QR:QR + 1, :], part[c, b, QR + 1:QR + 2, :]
        m2, l2 = precv[b, QR:QR + 1, :], precv[b, QR + 1:QR + 2, :]
        top = jnp.maximum(m1, m2)
        f1, f2 = jnp.exp(m1 - top), jnp.exp(m2 - top)
        dst[di, 0:QR, :] = part[c, b, 0:QR, :] * to_col(f1, QR) + precv[b, 0:QR, :] * to_col(f2, QR)
        dst[di, QR:MR, :] = stat_tile(top, l1 * f1 + l2 * f2)

    def scores(b, u):
        lim = (lens_ref[b] - me * T) * KH
        q0 = qbuf[0, pl.ds(pl.multiple_of(b * QR, QR), QR), :]
        q1 = qbuf[1, pl.ds(pl.multiple_of(b * QR, QR), QR), :]
        qb = jnp.concatenate([q0, q1], axis=0).astype(BF16)
        mx = jnp.full((AR, LANES), NEG_FILL, F32)
        for col in range(NK // 256):
            x = lax.dot_general(qb, kbuf[b, col * 256:(col + 1) * 256, :], NT, preferred_element_type=F32)
            for hc in range(256 // LANES):
                lo = col * 256 + hc * LANES
                xx = jnp.where(lane < lim - lo, x[:, hc * LANES:(hc + 1) * LANES] + kbias[...], NEG_FILL)
                sbuf[u, :, lo:lo + LANES] = xx
                mx = jnp.maximum(mx, xx)
        m = jnp.max(mx, axis=1, keepdims=True)
        mbuf[u, :, :] = jnp.broadcast_to(m, (AR, LANES))

    def weigh(b, u):
        lim = lens_ref[b] - me * T
        mb = mbuf[u]
        mub = jnp.where(lim > 0, mb, 0.0)
        tot = jnp.zeros((AR, LANES), F32)
        for lo in range(0, NK, LANES):
            w = jnp.exp2((sbuf[u, :, lo:lo + LANES] - mub) * fac)
            tot = tot + w
            wbuf[u, :, lo:lo + LANES] = w.astype(BF16)
        l = jnp.sum(tot, axis=1, keepdims=True)
        o = jnp.dot(wbuf[u], vbuf[b], preferred_element_type=F32)
        ms = mb * scale
        for hf in range(CORES):
            part[hf, b, 0:QR, :] = o[hf * QR:(hf + 1) * QR, :]
            part[hf, b, QR:MR, :] = stat_tile(full_row(ms[hf * QR:(hf + 1) * QR, :]), to_row(l[hf * QR:(hf + 1) * QR, :]))

    def comb(b):
        pair_combine(b, osend, b)
        o_copy(b).start()

    LAG = 3

    def stage(j, u, last, lagged):
        kb = nth(j)
        vcopy(kb).wait()
        if not last:
            kcopy(nth(j + 1)).wait()
            scores(nth(j + 1), 1 - u)
        for k, at in enumerate((3, 6, 9, 12)):
            @pl.when(j == at)
            def _():
                wcopy(6 + k).start()
        if last:
            for cp in moe_copies:
                cp.start()
        weigh(kb, u)
        p_copy(kb).start()
        if lagged:
            comb(nth(j - LAG))

    kcopy(nth(0)).wait()
    scores(nth(0), 0)
    for j in range(LAG):
        stage(j, j % 2, False, False)

    def attn_step(j, _):
        for u in range(2):
            @pl.when(lax.rem(j, 2) == u)
            def _():
                stage(j, u, False, True)
        return 0
    lax.fori_loop(LAG, B - 1, attn_step, 0)
    stage(B - 1, (B - 1) % 2, True, True)
    for j in range(B - LAG, B - 1):
        comb(nth(j))
    pair_combine(chip, orecv, chip)

    for s in range(S):
        for t in range(KHH):
            tkv[0, s * KHH + t:s * KHH + t + 1, :] = kt[c, t, pl.ds(s * B + chip, 1), :]
            tkv[1, s * KHH + t:s * KHH + t + 1, :] = vt[c, t, pl.ds(s * B + chip, 1), :]
    TR = tkv.shape[1]
    qb = qbuf[c, pl.ds(pl.multiple_of(chip * QR, QR), QR), :].astype(BF16)
    sc = lax.dot_general(qb, tkv[0].astype(BF16), NT, preferred_element_type=F32)
    tr, tl = iota((QR, TR), 0), iota((QR, TR), 1)
    valid = (lax.rem(tl, KHH) == lax.rem(tr, HH) // QG) & (tl // KHH <= tr // HH) & (tl < S * KHH)
    m, l, w = softmax_part(sc, valid, scale)
    orecv[chips, 0:QR, :] = jnp.dot(w, tkv[1].astype(BF16), preferred_element_type=F32)
    orecv[chips, QR:MR, :] = stat_tile(to_row(m), to_row(l))

    def o_wait(i, _):
        src = lax.rem(chip + i, chips)
        pltpu.make_async_remote_copy(osend.at[0], orecv.at[src], os_s.at[0], os_r.at[src],
                                     device_id={"kv": peer(src)}, device_id_type=MESH).wait_recv()
        return 0
    lax.fori_loop(1, chips, o_wait, 0)

    top = orecv[0, QR:QR + 1, :]
    for i in range(1, chips + 1):
        top = jnp.maximum(top, orecv[i, QR:QR + 1, :])
    tot = jnp.zeros((1, LANES), F32)
    acc = jnp.zeros((QR, LANES), F32)
    for i in range(chips + 1):
        f = jnp.exp(orecv[i, QR:QR + 1, :] - top)
        tot = tot + orecv[i, QR + 1:QR + 2, :] * f
        acc = acc + orecv[i, 0:QR, :] * to_col(f, QR)
    oxs[c, :, :] = round_bf16(acc / to_col(tot, QR))
    o_x = to_partner(oxs.at[c], oxs.at[c], ox_s, ox_r)
    o_x.start()
    for cp in small_copies[10:]:
        cp.wait()

    ctiles = WCOLS // LANES
    my_slot = pl.multiple_of(me * QR, QR)
    KROWS = HH * HD

    def fill(hf):
        for hh in range(HH):
            lhs[hf, 0:S, hh * HD:(hh + 1) * HD] = oxs[hf, pl.ds(hh, S, stride=HH), :]

    def wo_dot(hf, jn):
        return jnp.dot(lhs[hf].astype(BF16), wring[lax.rem(jn + 2, 4), pl.ds(pl.multiple_of(hf * KROWS, KROWS), KROWS), :], preferred_element_type=F32)

    fill(c)

    def wo_mine(jn, _):
        pltpu.make_async_copy(wsrc(0), wring.at[lax.rem(jn + 2, 4)], wsem.at[jn + 6]).wait()
        wacc[jn, :, :] = wo_dot(c, jn)
        return 0
    lax.fori_loop(0, 4, wo_mine, 0)
    o_x.wait_recv()
    fill(1 - c)

    def gatherer(buf, pieces, ss, rs, fs):
        PR = QR // pieces

        def cp(p, slot, sem, dev):
            blk = buf.at[pl.ds(pl.multiple_of(slot * QR + p * PR, 8), PR)]
            return pltpu.make_async_remote_copy(blk, blk, sem, rs.at[p, slot], device_id={"kv": dev}, device_id_type=MESH)

        def send(p):
            for i, o in enumerate(offsets):
                cp(p, me, ss.at[p, i], peer(ahead(o))).start()
            cp(p, me, ss.at[p, len(offsets)], partner).start()

        def finish():
            for p in range(pieces):
                for i, o in enumerate(offsets):
                    slot = peer(behind(o))
                    cp(p, slot, ss.at[p, i], partner).wait_recv()
                    cp(p, slot, fs.at[p, i], partner).start()
            for p in range(pieces):
                cp(p, partner, ss.at[p, 0], partner).wait_recv()
                for i, o in enumerate(offsets):
                    cp(p, behind(o) * CORES + (1 - c), ss.at[p, i], partner).wait_recv()

        def drain():
            for p in range(pieces):
                cp(p, me, ss.at[p, len(offsets)], partner).wait_send()
                for i in range(len(offsets)):
                    cp(p, me, ss.at[p, i], partner).wait_send()
                    cp(p, me, fs.at[p, i], partner).wait_send()
        return send, finish, drain

    XP = 2
    XPR = QR // XP
    XT = HH // XP
    x_send, x_finish, x_drain = gatherer(xg, XP, xa_s, xa_r, xf_s)
    for p in range(XP):
        def wo_other(k, _):
            jn = p * (4 // XP) + k
            off = pl.multiple_of(c * half_cols + jn * WCOLS, WCOLS)
            d = wacc[jn] + wo_dot(1 - c, jn)
            for s in range(S):
                v = round_bf16(x32[pl.ds(s * B + chip, 1), pl.ds(off, WCOLS)] + d[s:s + 1, :] + vbo[:, pl.ds(off, WCOLS)])
                for t in range(ctiles):
                    xg[pl.ds(my_slot + p * XPR + s * XT + k * ctiles + t, 1), :] = v[:, t * LANES:(t + 1) * LANES]
            return 0
        lax.fori_loop(0, 4 // XP, wo_other, 0)
        x_send(p)
    x_finish()
    for s in range(S):
        for hf in range(CORES):
            for t in range(HH):
                x32[s * B:(s + 1) * B, (hf * HH + t) * LANES:(hf * HH + t + 1) * LANES] = xg[pl.ds(hf * QR + (t // XT) * XPR + s * XT + t % XT, B, stride=CORES * QR), :]

    for cp in moe_copies:
        cp.wait()

    for s in range(S):
        layer_norm(s, vg2, vc2)
    logits = lax.dot_general(h[...], vwr[...], NT, preferred_element_type=F32)
    le = iota((B, E), 1)
    diag = iota((B, B), 0) == iota((B, B), 1)
    for s in range(S):
        lg = logits[s * B:(s + 1) * B, :]
        gate = jnp.zeros((B, E), F32)
        for k in range(ei_ref.shape[1]):
            masked = jnp.where(rm_ref[s, :, k, :] == 1, lg, NEG_FILL)
            ex = jnp.exp(masked - jnp.max(masked, axis=1, keepdims=True))
            p = ex / jnp.sum(ex, axis=1, keepdims=True)
            idx = jnp.sum(jnp.where(diag, jnp.broadcast_to(ei_ref[s, k:k + 1, :], (B, B)).astype(F32), 0.0), axis=1, keepdims=True)
            gate = gate + jnp.where(le.astype(F32) == idx, p, 0.0)
        gs[s * B:(s + 1) * B, 0:E] = gate
    gt[...] = jnp.transpose(gs[...])
    g_e = jnp.concatenate([gt[0:E, :]] * (LANES // E), axis=0)[:, 0:R]
    UB = 256
    for t in range(FEP // UB):
        ag = lax.dot_general(wmoe[0, t * UB:(t + 1) * UB, :], h[...], NT, preferred_element_type=F32)
        au = lax.dot_general(wmoe[1, t * UB:(t + 1) * UB, :], h[...], NT, preferred_element_type=F32)
        gg = jnp.concatenate([g_e] * (UB // LANES), axis=0)
        u = gg * (ag * jax.nn.sigmoid(ag)) * au
        ut[t * UB:(t + 1) * UB, 0:R] = jnp.where(iota((UB, R), 0) + t * UB < FE, u, 0.0)
    for t in range(FEP // LANES):
        ub[:, t * LANES:(t + 1) * LANES] = jnp.transpose(ut[t * LANES:(t + 1) * LANES, :])[0:R, :].astype(BF16)

    def mo_copy(i):
        return pltpu.make_async_remote_copy(mosend.at[i], morecv.at[chip], mo_s.at[i], mo_r.at[chip],
                                            device_id={"kv": peer(i)}, device_id_type=MESH)

    def moe_pair(i, dst, di):
        to_partner(mpsend.at[i], mprecv.at[i], mp_s.at[i], mp_r.at[i]).wait_recv()
        dst[di, :, :] = mine[i] + mprecv[i]

    GRP = 4

    def moe_out(g, _):
        for k in range(GRP):
            i = nth(g * GRP + k)
            pp = round_bf16(jnp.dot(ub[...], wmoe[2, :, pl.ds(pl.multiple_of(i * PC, PC), PC)], preferred_element_type=F32))
            p0, p1 = pp[:, :LANES], pp[:, LANES:]
            mpsend[i, :, :] = jnp.where(c == 0, p1, p0)
            mine[i, :, :] = jnp.where(c == 0, p0, p1)
        for k in range(GRP):
            i = nth(g * GRP + k)
            to_partner(mpsend.at[i], mprecv.at[i], mp_s.at[i], mp_r.at[i]).start()
        return 0

    def moe_fwd(j, _):
        i = nth(j)
        moe_pair(i, mosend, i)
        mo_copy(i).start()
        return 0
    lax.fori_loop(0, 2, moe_out, 0)

    def moe_both(g, _):
        moe_out(g, 0)
        lax.fori_loop((g - 2) * GRP, (g - 1) * GRP, moe_fwd, 0)
        return 0
    lax.fori_loop(2, chips // GRP, moe_both, 0)
    lax.fori_loop(chips - 2 * GRP, chips - 1, moe_fwd, 0)
    moe_pair(chip, morecv, chip)

    k_x.wait_recv()
    v_x.wait_recv()
    for src, dst in ((kt, tk_ref), (vt, tv_ref)):
        for hf in range(CORES):
            for t in range(KHH):
                for s in range(S):
                    t32[pl.ds(s * KH + hf * KHH + t, B, stride=S * KH), :] = src[hf, t, s * B:(s + 1) * B, :]
        dst[...] = t32[...].astype(BF16)

    def mo_wait(i, _):
        src = lax.rem(chip + chips - i, chips)
        pltpu.make_async_remote_copy(mosend.at[0], morecv.at[src], mo_s.at[0], mo_r.at[src],
                                     device_id={"kv": peer(src)}, device_id_type=MESH).wait_recv()
        return 0
    lax.fori_loop(1, chips, mo_wait, 0)
    tot = morecv[0]
    for i in range(1, chips):
        tot = tot + morecv[i]
    yg[pl.ds(my_slot, QR), :] = round_bf16(x32[:, pl.ds(pl.multiple_of(me * LANES, LANES), LANES)] + tot)
    y_send, y_finish, y_drain = gatherer(yg, 1, ya_s, ya_r, yf_s)
    y_send(0)
    y_finish()
    for d in range(chips * CORES):
        for s in range(S):
            out_ref[s, :, d * LANES:(d + 1) * LANES] = yg[d * QR + s * B:d * QR + (s + 1) * B, :].astype(BF16)

    q_x.wait_send()
    k_x.wait_send()
    v_x.wait_send()
    o_x.wait_send()

    def drain(i, _):
        b = lax.rem(chip + i, chips)
        p_copy(b).wait_send()
        to_partner(mpsend.at[b], mprecv.at[b], mp_s.at[b], mp_r.at[b]).wait_send()

        @pl.when(i > 0)
        def _():
            o_copy(b).wait_send()
            mo_copy(b).wait_send()
        return 0
    lax.fori_loop(0, chips, drain, 0)
    x_drain()
    y_drain()


def copy_out(a, b, d, oa, ob, od, sem):
    cps = [pltpu.make_async_copy(x, y, sem.at[i]) for i, (x, y) in enumerate(((a, oa), (b, ob), (d, od)))]
    for cp in cps:
        cp.start()
    for cp in cps:
        cp.wait()


def finish(*arrs):
    return pl.pallas_call(
        copy_out,
        name="copy_out",
        out_shape=tuple(jax.ShapeDtypeStruct(a.shape, a.dtype) for a in arrs),
        in_specs=[pl.BlockSpec(memory_space=pltpu.VMEM)] * len(arrs),
        out_specs=(pl.BlockSpec(memory_space=pl.ANY),) * len(arrs),
        scratch_shapes=[pltpu.SemaphoreType.DMA((len(arrs),))],
        compiler_params=pltpu.CompilerParams(vmem_limit_bytes=1 << 20),
    )(*arrs)


def solution(mesh):
    n = mesh.shape["kv"]
    chips = n // CORES

    def layer_steps(x_first, next_emb, k_cache, v_cache, seq_len, ln1_gain, ln1_bias, w_q, b_q, w_k, b_k, w_v, b_v, w_o, b_o, ln2_gain, ln2_bias, w_router, w_gate, w_up, w_down, long_factor, expert_idx, route_mask):
        B, T, KH, HD = k_cache.shape
        D = x_first.shape[1]
        H = w_q.shape[1] // HD
        S = next_emb.shape[0] + 1
        E = w_router.shape[1]
        FE = w_gate.shape[0] * w_gate.shape[2]
        FEP = -(-FE // 256) * 256
        R = S * B
        HH, KHH = H // CORES, KH // CORES
        QR = S * HH
        MR = QR + 8
        if B != chips or D != n * LANES or w_q.shape[1] != D or QR != R:
            raise ValueError("unsupported sizes")
        dims = dict(S=S, B=B, D=D, T=T, KH=KH, HD=HD, H=H, E=E, FE=FE, chips=chips)
        half = HD // 2
        power = np.float32(ROPE_BASE) ** (np.arange(half, dtype=np.float32) * np.float32(2.0) / np.float32(HD))
        pw = jnp.asarray(power[None, :].astype(np.float32))
        lf = long_factor[None, :]
        row = lambda a: a.reshape(1, -1)
        args = (seq_len, expert_idx.transpose(0, 2, 1), route_mask,
                x_first, next_emb, k_cache.reshape(B, T * KH, HD), v_cache.reshape(B, T * KH, HD), row(ln1_gain), row(ln1_bias),
                w_q, row(b_q), w_k, row(b_k), w_v, row(b_v), w_o, row(b_o), row(ln2_gain), row(ln2_bias), w_router.T,
                w_gate.transpose(2, 0, 1).reshape(FE, D), w_up.transpose(2, 0, 1).reshape(FE, D), w_down.transpose(1, 0, 2).reshape(FE, D), lf, pw)
        V = pltpu.VMEM
        DS = pltpu.SemaphoreType.DMA
        scratch = [
            pltpu.SMEM((B,), jnp.int32), V(expert_idx.transpose(0, 2, 1).shape, jnp.int32), V(route_mask.shape, jnp.int32),
            V((4, D, WCOLS), BF16), V((B, T * KH, HD), BF16), V((B, T * KH, HD), BF16), V((3, FEP, D), BF16),
            V((S, B, D), BF16), V((R, D), F32), V((R, D), BF16),
            V((1, D), F32), V((1, D), F32), V((1, D), F32), V((1, D), F32), V((1, D), F32), V((1, w_q.shape[1]), F32),
            V((1, w_k.shape[1]), F32), V((1, w_v.shape[1]), F32), V((1, half), F32), V((1, half), F32), V((E, D), BF16),
            V((CORES, B * QR, HD), F32), V((R, HD), F32), V((R, HD), F32), V((CORES, KHH, R, HD), F32), V((CORES, KHH, R, HD), F32), V((2, 16, HD), F32),
            V((CORES * QR, LANES), F32), V((2, CORES * QR, T * KH), F32), V((2, CORES * QR, LANES), F32), V((2, CORES * QR, T * KH), BF16),
            V((CORES, B, MR, HD), F32), V((B, MR, HD), F32), V((B, MR, HD), F32), V((chips + 1, MR, HD), F32),
            V((CORES, QR, HD), F32), V((CORES, 8, HH * HD), F32), V((4, 8, WCOLS), F32), V((n * QR, HD), F32), V((LANES, LANES), F32), V((LANES, LANES), F32), V((FEP, LANES), F32), V((R, FEP), BF16),
            V((chips, R, LANES), F32), V((chips, R, LANES), F32), V((chips, R, LANES), F32), V((chips, R, LANES), F32), V((chips, R, LANES), F32),
            V((n * QR, LANES), F32), V((B * S * KH, HD), F32),
            DS((10,)), DS((B,)), DS((B,)), DS((3,)), DS((16,)), DS, DS, DS, DS, DS, DS, DS((B,)), DS((B,)), DS((chips,)), DS((chips,)), DS, DS,
            DS((2, chips)), DS((2, n)), DS((2, chips)), DS((chips,)), DS((chips,)), DS((chips,)), DS((chips,)), DS((2, chips)), DS((2, n)), DS((2, chips)),
        ]
        vm = pl.BlockSpec(memory_space=pltpu.VMEM)
        anys = pl.BlockSpec(memory_space=pl.ANY)
        hidden, tk, tv = pl.pallas_call(
            functools.partial(kernel, dims),
            name="decode_layer",
            out_shape=(V((S, B, D), BF16), V((B * S * KH, HD), BF16), V((B * S * KH, HD), BF16)),
            in_specs=[anys] * len(args),
            out_specs=(vm, vm, vm),
            scratch_shapes=scratch,
            compiler_params=pltpu.CompilerParams(collective_id=0, has_side_effects=True, vmem_limit_bytes=VMEM_BYTES),
        )(*args)
        hidden, tk, tv = finish(hidden, tk, tv)
        return hidden, tk.reshape(B, S, KH, HD), tv.reshape(B, S, KH, HD)

    replicated = P()
    in_specs = (P('dp'), P(None, 'dp'), P('dp', 'kv'), P('dp', 'kv'), P('dp')) + (replicated,) * 13 + (P(None, None, 'kv'), P(None, None, 'kv'), P(None, 'kv'), replicated, P(None, 'dp'), P(None, 'dp'))
    out_specs = (P(None, 'dp'), P('dp'), P('dp'))
    return jax.shard_map(layer_steps, mesh=mesh, in_specs=in_specs, out_specs=out_specs, check_vma=False)
```

```python
import functools
import math

import jax
import jax.numpy as jnp
import numpy as np
from jax import lax
from jax.experimental import pallas as pl
from jax.experimental.pallas import tpu as pltpu
from jax.sharding import PartitionSpec as P

ROPE_BASE = 10000.0
ROPE_MSCALE = math.sqrt(1.0 + math.log(32.0) / math.log(4096.0))
NORM_EPS = 1e-5
NEG_FILL = -1e30
MESH = pl.DeviceIdType.MESH
F32 = jnp.float32
BF16 = jnp.bfloat16
LANES = 128
WCOLS = 512
CORES = 2
VMEM_BYTES = 64 * 1024 * 1024 - 4 * 1024 * 1024
NT = (((1,), (1,)), ((), ()))


def iota(shape, dim):
    return lax.broadcasted_iota(jnp.int32, shape, dim)


def to_row(col):
    rows = col.shape[0]
    pick = iota((rows, LANES), 0) == iota((rows, LANES), 1)
    return jnp.sum(jnp.where(pick, jnp.broadcast_to(col, (rows, LANES)), 0.0), axis=0, keepdims=True)


def full_row(full):
    rows = full.shape[0]
    pick = iota((rows, LANES), 0) == iota((rows, LANES), 1)
    return jnp.sum(jnp.where(pick, full, 0.0), axis=0, keepdims=True)


def to_col(row, rows):
    pick = iota((rows, LANES), 0) == iota((rows, LANES), 1)
    return jnp.sum(jnp.where(pick, jnp.broadcast_to(row, (rows, LANES)), 0.0), axis=1, keepdims=True)


def stat_tile(m_row, l_row):
    r = iota((8, LANES), 0)
    return jnp.where(r == 0, jnp.broadcast_to(m_row, (8, LANES)), jnp.where(r == 1, jnp.broadcast_to(l_row, (8, LANES)), 0.0))


def softmax_part(s_raw, valid, scale):
    s = jnp.where(valid, s_raw * scale, NEG_FILL)
    m = jnp.max(s, axis=1, keepdims=True)
    w = jnp.where(valid, jnp.exp(s - m), 0.0)
    return m, jnp.sum(w, axis=1, keepdims=True), w.astype(BF16)


def round_bf16(x):
    return x.astype(BF16).astype(F32)


def kernel(dims, lens_h, ei_h, rm_h,
           x_first, next_emb, k_hbm, v_hbm, g1, c1, w_q, b_q, w_k, b_k, w_v, b_v, w_o, b_o, g2, c2, w_r, w_g, w_u, w_d, lf, pw,
           out_ref, tk_ref, tv_ref,
           lens_ref, ei_ref, rm_ref, wring, kbuf, vbuf, wmoe, xin, x32, h, vg1, vc1, vg2, vc2, vbo, vbq, vbk, vbv, vlf, vpw, vwr,
           qbuf, cosb, sinb, kt, vt, tkv, kbias, sb0, sb1, mbuf, part, precv, osend, orecv, oxs, lhs, wacc, xg, gs, gt, ut, ub, mine, mpsend, mprecv, mosend, morecv, yg, t32,
           wsem, ksem, vsem, msem, ssem, qx_s, qx_r, kx_s, kx_r, vx_s, vx_r, ps_s, ps_r, os_s, os_r, ox_s, ox_r,
           xa_s, xa_r, xa_o, mp_s, mp_r, mo_s, mo_r, ya_s, ya_r, ya_o):
    S, B, D, T, KH, HD, H, E, FE, chips = (dims[k] for k in ("S", "B", "D", "T", "KH", "HD", "H", "E", "FE", "chips"))
    R = S * B
    HH, KHH = H // CORES, KH // CORES
    half_cols = D // CORES
    QG = H // KH
    QR = S * HH
    MR = QR + 8
    PC = LANES * CORES
    FEP = wmoe.shape[1]
    scale = HD ** -0.5
    me = lax.axis_index("kv")
    chip = me // CORES
    c = lax.rem(me, CORES)
    partner = chip * CORES + (1 - c)

    def peer(ch):
        return ch * CORES + c

    side = math.isqrt(chips)
    cy, cx = chip // side, lax.rem(chip, side)

    def ring(k):
        return side // 2 + ((k + 1) // 2) * (1 - 2 * (k % 2))

    def nth(j):
        return lax.rem(cy + ring(j // side), side) * side + lax.rem(cx + ring(lax.rem(j, side)), side)

    def dist(d):
        return min(d, side - d)
    offsets = sorted([(dy, dx) for dy in range(side) for dx in range(side) if dy or dx], key=lambda o: -(dist(o[0]) + dist(o[1])))

    def ahead(o):
        return lax.rem(cy + o[0], side) * side + lax.rem(cx + o[1], side)

    def behind(o):
        return lax.rem(cy + side - o[0], side) * side + lax.rem(cx + side - o[1], side)

    bar = pltpu.get_barrier_semaphore()
    pl.semaphore_signal(bar, inc=1, device_id={"kv": partner}, device_id_type=MESH)

    def sig(i, _):
        pl.semaphore_signal(bar, inc=1, device_id={"kv": peer(lax.rem(chip + i, chips))}, device_id_type=MESH)
        return 0
    lax.fori_loop(1, chips, sig, 0)

    def wsrc(ci):
        if ci < 4:
            return w_q.at[:, pl.ds(pl.multiple_of(c * half_cols + ci * WCOLS, WCOLS), WCOLS)]
        if ci == 4:
            return w_k.at[:, pl.ds(pl.multiple_of(c * WCOLS, WCOLS), WCOLS)]
        if ci == 5:
            return w_v.at[:, pl.ds(pl.multiple_of(c * WCOLS, WCOLS), WCOLS)]
        return w_o.at[:, pl.ds(pl.multiple_of(c * half_cols + (ci - 6) * WCOLS, WCOLS), WCOLS)]

    def wcopy(ci):
        return pltpu.make_async_copy(wsrc(ci), wring.at[ci % 4], wsem.at[ci])

    smalls = [(x_first, xin.at[0]), (next_emb, xin.at[pl.ds(1, S - 1)]), (g1, vg1), (c1, vc1), (b_q, vbq), (b_k, vbk), (b_v, vbv),
              (lf, vlf), (pw, vpw), (lens_h, lens_ref), (g2, vg2), (c2, vc2), (b_o, vbo), (w_r, vwr), (ei_h, ei_ref), (rm_h, rm_ref)]
    small_copies = [pltpu.make_async_copy(a, b, ssem.at[i]) for i, (a, b) in enumerate(smalls)]
    for cp in small_copies[:10]:
        cp.start()
    for ci in range(4):
        wcopy(ci).start()
    for cp in small_copies[10:]:
        cp.start()

    def kcopy(b):
        return pltpu.make_async_copy(k_hbm.at[b], kbuf.at[b], ksem.at[b])

    def vcopy(b):
        return pltpu.make_async_copy(v_hbm.at[b], vbuf.at[b], vsem.at[b])

    moe_copies = [pltpu.make_async_copy(src, wmoe.at[i, pl.ds(0, FE)], msem.at[i]) for i, src in enumerate((w_g, w_u, w_d))]

    wmoe[2, FE:FEP, :] = jnp.zeros((FEP - FE, D), BF16)
    lhs[...] = jnp.zeros_like(lhs)
    gs[...] = jnp.zeros_like(gs)
    ut[...] = jnp.zeros_like(ut)
    tkv[...] = jnp.zeros_like(tkv)

    def layer_norm(s, gain, bias):
        x = x32[s * B:(s + 1) * B, :]
        mean = jnp.sum(x, axis=1, keepdims=True) / D
        cen = x - mean
        var = jnp.sum(cen * cen, axis=1, keepdims=True) / D
        h[s * B:(s + 1) * B, :] = (cen * lax.rsqrt(var + NORM_EPS) * gain[...] + bias[...]).astype(BF16)

    for cp in small_copies[:10]:
        cp.wait()
    for s in range(S):
        x32[s * B:(s + 1) * B, :] = xin[s].astype(F32)
        layer_norm(s, vg1, vc1)
    hd2 = HD // 2
    row_b = lax.rem(iota((R, hd2), 0), B)
    pos = iota((R, hd2), 0) // B
    for b in range(B):
        pos = pos + jnp.where(row_b == b, lens_ref[b], 0)
    ang = pos.astype(F32) * (1.0 / (vlf[...] * vpw[...]))
    cs = jnp.cos(ang) * ROPE_MSCALE
    sn = jnp.sin(ang) * ROPE_MSCALE
    cosb[:, 0:hd2] = cs
    cosb[:, hd2:HD] = cs
    sinb[:, 0:hd2] = -sn
    sinb[:, hd2:HD] = sn
    kr, kl = iota((CORES * QR, LANES), 0), iota((CORES * QR, LANES), 1)
    kbias[...] = jnp.where((kr // QR) * KHH + lax.rem(kr, HH) // QG == lax.rem(kl, KH), 0.0, NEG_FILL)

    def rotate(x):
        return round_bf16(x * cosb[...] + pltpu.roll(x, HD // 2, 1) * sinb[...])

    def kv_start(j, _):
        b = nth(j)
        kcopy(b).start()
        vcopy(b).start()
        return 0

    def q_chunk(ci, _):
        pltpu.make_async_copy(wsrc(0), wring.at[ci], wsem.at[ci]).wait()
        off = pl.multiple_of(c * half_cols + ci * WCOLS, WCOLS)
        y = jnp.dot(h[...], wring[ci], preferred_element_type=F32) + vbq[:, pl.ds(off, WCOLS)]
        y = round_bf16(y)
        for t in range(WCOLS // HD):
            r = rotate(y[:, t * HD:(t + 1) * HD])
            hh = ci * (WCOLS // HD) + t
            for s in range(S):
                qbuf[c, pl.ds(s * HH + hh, B, stride=QR), :] = r[s * B:(s + 1) * B, :]

        @pl.when(ci == 0)
        def _():
            wcopy(4).start()

        @pl.when(ci == 1)
        def _():
            wcopy(5).start()

        @pl.when(ci == 2)
        def _():
            lax.fori_loop(0, B // 2, kv_start, 0)

        @pl.when(ci == 3)
        def _():
            lax.fori_loop(B // 2, B, kv_start, 0)
        return 0
    lax.fori_loop(0, 4, q_chunk, 0)

    pl.semaphore_wait(bar, chips)

    def to_partner(src, dst, ss, rs):
        return pltpu.make_async_remote_copy(src, dst, ss, rs, device_id={"kv": partner}, device_id_type=MESH)

    q_x = to_partner(qbuf.at[c], qbuf.at[c], qx_s, qx_r)
    q_x.start()

    wcopy(4).wait()
    y = round_bf16(jnp.dot(h[...], wring[0], preferred_element_type=F32) + vbk[:, pl.ds(pl.multiple_of(c * WCOLS, WCOLS), WCOLS)])
    for t in range(KHH):
        kt[c, t, :, :] = rotate(y[:, t * HD:(t + 1) * HD])
    wcopy(5).wait()
    y = round_bf16(jnp.dot(h[...], wring[1], preferred_element_type=F32) + vbv[:, pl.ds(pl.multiple_of(c * WCOLS, WCOLS), WCOLS)])
    for t in range(KHH):
        vt[c, t, :, :] = y[:, t * HD:(t + 1) * HD]
    k_x = to_partner(kt.at[c], kt.at[c], kx_s, kx_r)
    v_x = to_partner(vt.at[c], vt.at[c], vx_s, vx_r)
    k_x.start()
    v_x.start()

    q_x.wait_recv()
    AR = CORES * QR
    sbufs = (sb0, sb1)
    NK = T * KH
    fac = scale * math.log2(math.e)
    lane = iota((AR, LANES), 1)

    def o_copy(b):
        return pltpu.make_async_remote_copy(osend.at[b], orecv.at[chip], os_s.at[b], os_r.at[chip],
                                            device_id={"kv": peer(b)}, device_id_type=MESH)

    def p_copy(b):
        return to_partner(part.at[1 - c, b], precv.at[b], ps_s.at[b], ps_r.at[b])

    def pair_combine(b, dst, di):
        p_copy(b).wait_recv()
        m1, l1 = part[c, b, QR:QR + 1, :], part[c, b, QR + 1:QR + 2, :]
        m2, l2 = precv[b, QR:QR + 1, :], precv[b, QR + 1:QR + 2, :]
        top = jnp.maximum(m1, m2)
        f1, f2 = jnp.exp(m1 - top), jnp.exp(m2 - top)
        dst[di, 0:QR, :] = part[c, b, 0:QR, :] * to_col(f1, QR) + precv[b, 0:QR, :] * to_col(f2, QR)
        dst[di, QR:MR, :] = stat_tile(top, l1 * f1 + l2 * f2)

    def queries(b):
        q0 = qbuf[0, pl.ds(pl.multiple_of(b * QR, QR), QR), :]
        q1 = qbuf[1, pl.ds(pl.multiple_of(b * QR, QR), QR), :]
        return jnp.concatenate([q0, q1], axis=0).astype(BF16)

    def work(sb, su, wb, wu):
        CK = 256
        if sb is not None:
            lim = (lens_ref[sb] - me * T) * KH
            qb = queries(sb)
            mx = jnp.full((AR, LANES), NEG_FILL, F32)
        if wb is not None:
            mb = mbuf[wu]
            mub = jnp.where(lens_ref[wb] > me * T, mb, 0.0)
            tot = jnp.zeros((AR, LANES), F32)
            o = jnp.zeros((AR, HD), F32)
        for col in range(NK // CK):
            if sb is not None:
                x = lax.dot_general(qb, kbuf[sb, col * CK:(col + 1) * CK, :], NT, preferred_element_type=F32)
            if wb is not None:
                ws = []
                for hc in range(CK // LANES):
                    lo = col * CK + hc * LANES
                    w = jnp.exp2((sbufs[wu][:, lo:lo + LANES] - mub) * fac)
                    tot = tot + w
                    ws.append(w.astype(BF16))
                o = o + jnp.dot(jnp.concatenate(ws, axis=1), vbuf[wb, col * CK:(col + 1) * CK, :], preferred_element_type=F32)
            if sb is not None:
                for hc in range(CK // LANES):
                    lo = col * CK + hc * LANES
                    xx = jnp.where(lane < lim - lo, x[:, hc * LANES:(hc + 1) * LANES] + kbias[...], NEG_FILL)
                    sbufs[su][:, lo:lo + LANES] = xx
                    mx = jnp.maximum(mx, xx)
        if sb is not None:
            mbuf[su, :, :] = jnp.broadcast_to(jnp.max(mx, axis=1, keepdims=True), (AR, LANES))
        if wb is not None:
            l = jnp.sum(tot, axis=1, keepdims=True)
            ms = mb * scale
            for hf in range(CORES):
                part[hf, wb, 0:QR, :] = o[hf * QR:(hf + 1) * QR, :]
                part[hf, wb, QR:MR, :] = stat_tile(full_row(ms[hf * QR:(hf + 1) * QR, :]), to_row(l[hf * QR:(hf + 1) * QR, :]))

    def comb(b):
        pair_combine(b, osend, b)
        o_copy(b).start()

    LAG = 3

    def stage(j, u, last, lagged):
        kb = nth(j)
        vcopy(kb).wait()
        if not last:
            kcopy(nth(j + 1)).wait()
        for k, at in enumerate((3, 6, 9, 12)):
            @pl.when(j == at)
            def _():
                wcopy(6 + k).start()
        if last:
            for cp in moe_copies:
                cp.start()
        work(None if last else nth(j + 1), 1 - u, kb, u)
        p_copy(kb).start()
        if lagged:
            comb(nth(j - LAG))

    kcopy(nth(0)).wait()
    work(nth(0), 0, None, 0)
    for j in range(LAG):
        stage(j, j % 2, False, False)

    def attn_step(j, _):
        for u in range(2):
            @pl.when(lax.rem(j, 2) == u)
            def _():
                stage(j, u, False, True)
        return 0
    lax.fori_loop(LAG, B - 1, attn_step, 0)
    stage(B - 1, (B - 1) % 2, True, True)
    for j in range(B - LAG, B - 1):
        comb(nth(j))
    pair_combine(chip, orecv, chip)

    for s in range(S):
        for t in range(KHH):
            tkv[0, s * KHH + t:s * KHH + t + 1, :] = kt[c, t, pl.ds(s * B + chip, 1), :]
            tkv[1, s * KHH + t:s * KHH + t + 1, :] = vt[c, t, pl.ds(s * B + chip, 1), :]
    TR = tkv.shape[1]
    qb = qbuf[c, pl.ds(pl.multiple_of(chip * QR, QR), QR), :].astype(BF16)
    sc = lax.dot_general(qb, tkv[0].astype(BF16), NT, preferred_element_type=F32)
    tr, tl = iota((QR, TR), 0), iota((QR, TR), 1)
    valid = (lax.rem(tl, KHH) == lax.rem(tr, HH) // QG) & (tl // KHH <= tr // HH) & (tl < S * KHH)
    m, l, w = softmax_part(sc, valid, scale)
    orecv[chips, 0:QR, :] = jnp.dot(w, tkv[1].astype(BF16), preferred_element_type=F32)
    orecv[chips, QR:MR, :] = stat_tile(to_row(m), to_row(l))

    def o_wait(i, _):
        src = lax.rem(chip + i, chips)
        pltpu.make_async_remote_copy(osend.at[0], orecv.at[src], os_s.at[0], os_r.at[src],
                                     device_id={"kv": peer(src)}, device_id_type=MESH).wait_recv()
        return 0
    lax.fori_loop(1, chips, o_wait, 0)

    top = orecv[0, QR:QR + 1, :]
    for i in range(1, chips + 1):
        top = jnp.maximum(top, orecv[i, QR:QR + 1, :])
    tot = jnp.zeros((1, LANES), F32)
    acc = jnp.zeros((QR, LANES), F32)
    for i in range(chips + 1):
        f = jnp.exp(orecv[i, QR:QR + 1, :] - top)
        tot = tot + orecv[i, QR + 1:QR + 2, :] * f
        acc = acc + orecv[i, 0:QR, :] * to_col(f, QR)
    oxs[c, :, :] = round_bf16(acc / to_col(tot, QR))
    o_x = to_partner(oxs.at[c], oxs.at[c], ox_s, ox_r)
    o_x.start()
    for cp in small_copies[10:]:
        cp.wait()

    ctiles = WCOLS // LANES
    my_slot = pl.multiple_of(me * QR, QR)
    KROWS = HH * HD

    def fill(hf):
        for hh in range(HH):
            lhs[hf, 0:S, hh * HD:(hh + 1) * HD] = oxs[hf, pl.ds(hh, S, stride=HH), :]

    def wo_dot(hf, jn):
        return jnp.dot(lhs[hf].astype(BF16), wring[lax.rem(jn + 2, 4), pl.ds(pl.multiple_of(hf * KROWS, KROWS), KROWS), :], preferred_element_type=F32)

    fill(c)

    def wo_mine(jn, _):
        pltpu.make_async_copy(wsrc(0), wring.at[lax.rem(jn + 2, 4)], wsem.at[jn + 6]).wait()
        wacc[jn, :, :] = wo_dot(c, jn)
        return 0
    lax.fori_loop(0, 4, wo_mine, 0)
    o_x.wait_recv()
    fill(1 - c)

    GROUPS = 3
    GSIZE = -(-len(offsets) // GROUPS)

    def gatherer(buf, pieces, ss, rs, ro):
        PR = QR // pieces

        def cp(p, slot, rsem, dev):
            blk = buf.at[pl.ds(pl.multiple_of(slot * QR + p * PR, 8), PR)]
            return pltpu.make_async_remote_copy(blk, blk, ss.at[p], rsem, device_id={"kv": dev}, device_id_type=MESH)

        def all_of(count, p, rsem):
            blk = buf.at[pl.ds(0, count * PR)]
            return pltpu.make_async_remote_copy(blk, blk, ss.at[p], rsem, device_id={"kv": partner}, device_id_type=MESH)

        def send(p):
            for i, o in enumerate(offsets):
                cp(p, me, rs.at[p, i // GSIZE], peer(ahead(o))).start()
            cp(p, me, ro.at[p], partner).start()

        def finish():
            for p in range(pieces):
                for g in range(GROUPS):
                    mem = offsets[g * GSIZE:(g + 1) * GSIZE]
                    all_of(len(mem), p, rs.at[p, g]).wait_recv()
                    for o in mem:
                        cp(p, peer(behind(o)), ro.at[p], partner).start()
            for p in range(pieces):
                all_of(chips, p, ro.at[p]).wait_recv()

        def drain():
            for p in range(pieces):
                all_of(2 * chips - 1, p, ro.at[p]).wait_send()
        return send, finish, drain

    XP = 2
    XPR = QR // XP
    XT = HH // XP
    x_send, x_finish, x_drain = gatherer(xg, XP, xa_s, xa_r, xa_o)
    for p in range(XP):
        def wo_other(k, _):
            jn = p * (4 // XP) + k
            off = pl.multiple_of(c * half_cols + jn * WCOLS, WCOLS)
            d = wacc[jn] + wo_dot(1 - c, jn)
            for s in range(S):
                v = round_bf16(x32[pl.ds(s * B + chip, 1), pl.ds(off, WCOLS)] + d[s:s + 1, :] + vbo[:, pl.ds(off, WCOLS)])
                for t in range(ctiles):
                    xg[pl.ds(my_slot + p * XPR + s * XT + k * ctiles + t, 1), :] = v[:, t * LANES:(t + 1) * LANES]
            return 0
        lax.fori_loop(0, 4 // XP, wo_other, 0)
        x_send(p)
    x_finish()
    for s in range(S):
        for hf in range(CORES):
            for t in range(HH):
                x32[s * B:(s + 1) * B, (hf * HH + t) * LANES:(hf * HH + t + 1) * LANES] = xg[pl.ds(hf * QR + (t // XT) * XPR + s * XT + t % XT, B, stride=CORES * QR), :]

    for cp in moe_copies:
        cp.wait()

    for s in range(S):
        layer_norm(s, vg2, vc2)
    logits = lax.dot_general(h[...], vwr[...], NT, preferred_element_type=F32)
    le = iota((B, E), 1)
    diag = iota((B, B), 0) == iota((B, B), 1)
    for s in range(S):
        lg = logits[s * B:(s + 1) * B, :]
        gate = jnp.zeros((B, E), F32)
        for k in range(ei_ref.shape[1]):
            masked = jnp.where(rm_ref[s, :, k, :] == 1, lg, NEG_FILL)
            ex = jnp.exp(masked - jnp.max(masked, axis=1, keepdims=True))
            p = ex / jnp.sum(ex, axis=1, keepdims=True)
            idx = jnp.sum(jnp.where(diag, jnp.broadcast_to(ei_ref[s, k:k + 1, :], (B, B)).astype(F32), 0.0), axis=1, keepdims=True)
            gate = gate + jnp.where(le.astype(F32) == idx, p, 0.0)
        gs[s * B:(s + 1) * B, 0:E] = gate
    gt[...] = jnp.transpose(gs[...])
    g_e = jnp.concatenate([gt[0:E, :]] * (LANES // E), axis=0)[:, 0:R]
    UB = 256
    for t in range(FEP // UB):
        ag = lax.dot_general(wmoe[0, t * UB:(t + 1) * UB, :], h[...], NT, preferred_element_type=F32)
        au = lax.dot_general(wmoe[1, t * UB:(t + 1) * UB, :], h[...], NT, preferred_element_type=F32)
        gg = jnp.concatenate([g_e] * (UB // LANES), axis=0)
        u = gg * (ag * jax.nn.sigmoid(ag)) * au
        ut[t * UB:(t + 1) * UB, 0:R] = jnp.where(iota((UB, R), 0) + t * UB < FE, u, 0.0)
    for t in range(FEP // LANES):
        ub[:, t * LANES:(t + 1) * LANES] = jnp.transpose(ut[t * LANES:(t + 1) * LANES, :])[0:R, :].astype(BF16)

    MP = 2
    MPR = R // MP

    def mo_copy(i, p):
        return pltpu.make_async_remote_copy(mosend.at[p, i], morecv.at[p, chip], mo_s.at[p, i], mo_r.at[p, chip],
                                            device_id={"kv": peer(i)}, device_id_type=MESH)

    def moe_pair(i, dst, di):
        to_partner(mpsend.at[i], mprecv.at[i], mp_s.at[i], mp_r.at[i]).wait_recv()
        for p in range(MP):
            dst[p, di, :, :] = mine[i, p * MPR:(p + 1) * MPR, :] + mprecv[i, p * MPR:(p + 1) * MPR, :]

    GRP = 4

    def moe_out(g, _):
        for k in range(GRP):
            i = nth(g * GRP + k)
            pp = round_bf16(jnp.dot(ub[...], wmoe[2, :, pl.ds(pl.multiple_of(i * PC, PC), PC)], preferred_element_type=F32))
            p0, p1 = pp[:, :LANES], pp[:, LANES:]
            mpsend[i, :, :] = jnp.where(c == 0, p1, p0)
            mine[i, :, :] = jnp.where(c == 0, p0, p1)
        for k in range(GRP):
            i = nth(g * GRP + k)
            to_partner(mpsend.at[i], mprecv.at[i], mp_s.at[i], mp_r.at[i]).start()
        return 0

    def moe_fwd(j, _):
        i = nth(j)
        moe_pair(i, mosend, i)
        mo_copy(i, 0).start()
        return 0
    lax.fori_loop(0, 2, moe_out, 0)

    def moe_both(g, _):
        moe_out(g, 0)
        lax.fori_loop((g - 2) * GRP, (g - 1) * GRP, moe_fwd, 0)
        return 0
    lax.fori_loop(2, chips // GRP, moe_both, 0)
    lax.fori_loop(chips - 2 * GRP, chips - 1, moe_fwd, 0)

    def mo_rest(j, _):
        for p in range(1, MP):
            mo_copy(nth(j), p).start()
        return 0
    lax.fori_loop(0, chips - 1, mo_rest, 0)
    moe_pair(chip, morecv, chip)

    k_x.wait_recv()
    v_x.wait_recv()
    for src, dst in ((kt, tk_ref), (vt, tv_ref)):
        for hf in range(CORES):
            for t in range(KHH):
                for s in range(S):
                    t32[pl.ds(s * KH + hf * KHH + t, B, stride=S * KH), :] = src[hf, t, s * B:(s + 1) * B, :]
        dst[...] = t32[...].astype(BF16)

    y_send, y_finish, y_drain = gatherer(yg, MP, ya_s, ya_r, ya_o)
    for p in range(MP):
        def mo_wait(i, _):
            src = lax.rem(chip + i, chips)
            pltpu.make_async_remote_copy(mosend.at[p, 0], morecv.at[p, src], mo_s.at[p, 0], mo_r.at[p, src],
                                         device_id={"kv": peer(src)}, device_id_type=MESH).wait_recv()
            return 0
        lax.fori_loop(1, chips, mo_wait, 0)
        tot = morecv[p, 0]
        for i in range(1, chips):
            tot = tot + morecv[p, i]
        yg[pl.ds(my_slot + p * MPR, MPR), :] = round_bf16(x32[p * MPR:(p + 1) * MPR, pl.ds(pl.multiple_of(me * LANES, LANES), LANES)] + tot)
        y_send(p)
    y_finish()
    for d in range(chips * CORES):
        for s in range(S):
            out_ref[s, :, d * LANES:(d + 1) * LANES] = yg[d * QR + s * B:d * QR + (s + 1) * B, :].astype(BF16)

    q_x.wait_send()
    k_x.wait_send()
    v_x.wait_send()
    o_x.wait_send()

    def drain(i, _):
        b = lax.rem(chip + i, chips)
        p_copy(b).wait_send()
        to_partner(mpsend.at[b], mprecv.at[b], mp_s.at[b], mp_r.at[b]).wait_send()

        @pl.when(i > 0)
        def _():
            o_copy(b).wait_send()
            for p in range(MP):
                mo_copy(b, p).wait_send()
        return 0
    lax.fori_loop(0, chips, drain, 0)
    x_drain()
    y_drain()


def copy_out(a, b, d, oa, ob, od, sem):
    cps = [pltpu.make_async_copy(x, y, sem.at[i]) for i, (x, y) in enumerate(((a, oa), (b, ob), (d, od)))]
    for cp in cps:
        cp.start()
    for cp in cps:
        cp.wait()


def finish(*arrs):
    return pl.pallas_call(
        copy_out,
        name="copy_out",
        out_shape=tuple(jax.ShapeDtypeStruct(a.shape, a.dtype) for a in arrs),
        in_specs=[pl.BlockSpec(memory_space=pltpu.VMEM)] * len(arrs),
        out_specs=(pl.BlockSpec(memory_space=pl.ANY),) * len(arrs),
        scratch_shapes=[pltpu.SemaphoreType.DMA((len(arrs),))],
        compiler_params=pltpu.CompilerParams(vmem_limit_bytes=1 << 20),
    )(*arrs)


def solution(mesh):
    n = mesh.shape["kv"]
    chips = n // CORES

    def layer_steps(x_first, next_emb, k_cache, v_cache, seq_len, ln1_gain, ln1_bias, w_q, b_q, w_k, b_k, w_v, b_v, w_o, b_o, ln2_gain, ln2_bias, w_router, w_gate, w_up, w_down, long_factor, expert_idx, route_mask):
        B, T, KH, HD = k_cache.shape
        D = x_first.shape[1]
        H = w_q.shape[1] // HD
        S = next_emb.shape[0] + 1
        E = w_router.shape[1]
        FE = w_gate.shape[0] * w_gate.shape[2]
        FEP = -(-FE // 256) * 256
        R = S * B
        HH, KHH = H // CORES, KH // CORES
        QR = S * HH
        MR = QR + 8
        if B != chips or D != n * LANES or w_q.shape[1] != D or QR != R:
            raise ValueError("unsupported sizes")
        dims = dict(S=S, B=B, D=D, T=T, KH=KH, HD=HD, H=H, E=E, FE=FE, chips=chips)
        half = HD // 2
        power = np.float32(ROPE_BASE) ** (np.arange(half, dtype=np.float32) * np.float32(2.0) / np.float32(HD))
        pw = jnp.asarray(power[None, :].astype(np.float32))
        lf = long_factor[None, :]
        row = lambda a: a.reshape(1, -1)
        args = (seq_len, expert_idx.transpose(0, 2, 1), route_mask,
                x_first, next_emb, k_cache.reshape(B, T * KH, HD), v_cache.reshape(B, T * KH, HD), row(ln1_gain), row(ln1_bias),
                w_q, row(b_q), w_k, row(b_k), w_v, row(b_v), w_o, row(b_o), row(ln2_gain), row(ln2_bias), w_router.T,
                w_gate.transpose(2, 0, 1).reshape(FE, D), w_up.transpose(2, 0, 1).reshape(FE, D), w_down.transpose(1, 0, 2).reshape(FE, D), lf, pw)
        V = pltpu.VMEM
        DS = pltpu.SemaphoreType.DMA
        scratch = [
            pltpu.SMEM((B,), jnp.int32), V(expert_idx.transpose(0, 2, 1).shape, jnp.int32), V(route_mask.shape, jnp.int32),
            V((4, D, WCOLS), BF16), V((B, T * KH, HD), BF16), V((B, T * KH, HD), BF16), V((3, FEP, D), BF16),
            V((S, B, D), BF16), V((R, D), F32), V((R, D), BF16),
            V((1, D), F32), V((1, D), F32), V((1, D), F32), V((1, D), F32), V((1, D), F32), V((1, w_q.shape[1]), F32),
            V((1, w_k.shape[1]), F32), V((1, w_v.shape[1]), F32), V((1, half), F32), V((1, half), F32), V((E, D), BF16),
            V((CORES, B * QR, HD), F32), V((R, HD), F32), V((R, HD), F32), V((CORES, KHH, R, HD), F32), V((CORES, KHH, R, HD), F32), V((2, 16, HD), F32),
            V((CORES * QR, LANES), F32), V((CORES * QR, T * KH), F32), V((CORES * QR, T * KH), F32), V((2, CORES * QR, LANES), F32),
            V((CORES, B, MR, HD), F32), V((B, MR, HD), F32), V((B, MR, HD), F32), V((chips + 1, MR, HD), F32),
            V((CORES, QR, HD), F32), V((CORES, 8, HH * HD), F32), V((4, 8, WCOLS), F32), V((n * QR, HD), F32), V((LANES, LANES), F32), V((LANES, LANES), F32), V((FEP, LANES), F32), V((R, FEP), BF16),
            V((chips, R, LANES), F32), V((chips, R, LANES), F32), V((chips, R, LANES), F32), V((2, chips, R // 2, LANES), F32), V((2, chips, R // 2, LANES), F32),
            V((n * QR, LANES), F32), V((B * S * KH, HD), F32),
            DS((10,)), DS((B,)), DS((B,)), DS((3,)), DS((16,)), DS, DS, DS, DS, DS, DS, DS((B,)), DS((B,)), DS((chips,)), DS((chips,)), DS, DS,
            DS((2,)), DS((2, 3)), DS((2,)), DS((chips,)), DS((chips,)), DS((2, chips)), DS((2, chips)), DS((2,)), DS((2, 3)), DS((2,)),
        ]
        vm = pl.BlockSpec(memory_space=pltpu.VMEM)
        anys = pl.BlockSpec(memory_space=pl.ANY)
        hidden, tk, tv = pl.pallas_call(
            functools.partial(kernel, dims),
            name="decode_layer",
            out_shape=(V((S, B, D), BF16), V((B * S * KH, HD), BF16), V((B * S * KH, HD), BF16)),
            in_specs=[anys] * len(args),
            out_specs=(vm, vm, vm),
            scratch_shapes=scratch,
            compiler_params=pltpu.CompilerParams(collective_id=0, has_side_effects=True, vmem_limit_bytes=VMEM_BYTES),
        )(*args)
        hidden, tk, tv = finish(hidden, tk, tv)
        return hidden, tk.reshape(B, S, KH, HD), tv.reshape(B, S, KH, HD)

    replicated = P()
    in_specs = (P('dp'), P(None, 'dp'), P('dp', 'kv'), P('dp', 'kv'), P('dp')) + (replicated,) * 13 + (P(None, None, 'kv'), P(None, None, 'kv'), P(None, 'kv'), replicated, P(None, 'dp'), P(None, 'dp'))
    out_specs = (P(None, 'dp'), P('dp'), P('dp'))
    return jax.shard_map(layer_steps, mesh=mesh, in_specs=in_specs, out_specs=out_specs, check_vma=False)
```

```python
import functools
import math

import jax
import jax.numpy as jnp
import numpy as np
from jax import lax
from jax.experimental import pallas as pl
from jax.experimental.pallas import tpu as pltpu
from jax.sharding import PartitionSpec as P

ROPE_BASE = 10000.0
ROPE_MSCALE = math.sqrt(1.0 + math.log(32.0) / math.log(4096.0))
NORM_EPS = 1e-5
NEG_FILL = -1e30
MESH = pl.DeviceIdType.MESH
F32 = jnp.float32
BF16 = jnp.bfloat16
LANES = 128
WCOLS = 512
CORES = 2
VMEM_BYTES = 64 * 1024 * 1024 - 4 * 1024 * 1024
NT = (((1,), (1,)), ((), ()))


def iota(shape, dim):
    return lax.broadcasted_iota(jnp.int32, shape, dim)


def to_row(col):
    rows = col.shape[0]
    pick = iota((rows, LANES), 0) == iota((rows, LANES), 1)
    return jnp.sum(jnp.where(pick, jnp.broadcast_to(col, (rows, LANES)), 0.0), axis=0, keepdims=True)


def full_row(full):
    rows = full.shape[0]
    pick = iota((rows, LANES), 0) == iota((rows, LANES), 1)
    return jnp.sum(jnp.where(pick, full, 0.0), axis=0, keepdims=True)


def to_col(row, rows):
    pick = iota((rows, LANES), 0) == iota((rows, LANES), 1)
    return jnp.sum(jnp.where(pick, jnp.broadcast_to(row, (rows, LANES)), 0.0), axis=1, keepdims=True)


def stat_tile(m_row, l_row):
    r = iota((8, LANES), 0)
    return jnp.where(r == 0, jnp.broadcast_to(m_row, (8, LANES)), jnp.where(r == 1, jnp.broadcast_to(l_row, (8, LANES)), 0.0))


def softmax_part(s_raw, valid, scale):
    s = jnp.where(valid, s_raw * scale, NEG_FILL)
    m = jnp.max(s, axis=1, keepdims=True)
    w = jnp.where(valid, jnp.exp(s - m), 0.0)
    return m, jnp.sum(w, axis=1, keepdims=True), w.astype(BF16)


def round_bf16(x):
    return x.astype(BF16).astype(F32)


def kernel(dims, lens_h, ei_h, rm_h,
           x_first, next_emb, k_hbm, v_hbm, g1, c1, w_q, b_q, w_k, b_k, w_v, b_v, w_o, b_o, g2, c2, w_r, w_g, w_u, w_d, lf, pw,
           out_ref, tk_ref, tv_ref,
           lens_ref, ei_ref, rm_ref, wring, kbuf, vbuf, wmoe, xin, x32, h, vg1, vc1, vg2, vc2, vbo, vbq, vbk, vbv, vlf, vpw, vwr,
           qbuf, cosb, sinb, kt, vt, tkv, kbias, sb0, sb1, mbuf, part, precv, osend, orecv, oxs, lhs, wacc, xg, gs, gt, ut, ub, mine, mpsend, mprecv, mosend, morecv, yg, t32,
           wsem, ksem, vsem, msem, ssem, qx_s, qx_r, kx_s, kx_r, vx_s, vx_r, ps_s, ps_r, os_s, os_r, ox_s, ox_r,
           xa_s, xa_r, xa_o, mo_s, mo_r, ya_s, ya_r, ya_o):
    S, B, D, T, KH, HD, H, E, FE, chips = (dims[k] for k in ("S", "B", "D", "T", "KH", "HD", "H", "E", "FE", "chips"))
    R = S * B
    HH, KHH = H // CORES, KH // CORES
    half_cols = D // CORES
    QG = H // KH
    QR = S * HH
    MR = QR + 8
    PC = LANES * CORES
    FEP = wmoe.shape[1]
    scale = HD ** -0.5
    me = lax.axis_index("kv")
    chip = lax.div(me, CORES)
    c = lax.rem(me, CORES)
    partner = chip * CORES + (1 - c)

    def peer(ch):
        return ch * CORES + c

    side = math.isqrt(chips)
    cy, cx = lax.div(chip, side), lax.rem(chip, side)

    def ring(k):
        return side // 2 + lax.div(k + 1, 2) * (1 - 2 * lax.rem(k, 2))

    def nth(j):
        j = jnp.int32(j)
        return lax.rem(cy + ring(lax.div(j, side)), side) * side + lax.rem(cx + ring(lax.rem(j, side)), side)

    def dist(d):
        return min(d, side - d)
    offsets = sorted([(dy, dx) for dy in range(side) for dx in range(side) if dy or dx], key=lambda o: -(dist(o[0]) + dist(o[1])))

    def ahead(o):
        return lax.rem(cy + o[0], side) * side + lax.rem(cx + o[1], side)

    def behind(o):
        return lax.rem(cy + side - o[0], side) * side + lax.rem(cx + side - o[1], side)

    bar = pltpu.get_barrier_semaphore()
    pl.semaphore_signal(bar, inc=1, device_id={"kv": partner}, device_id_type=MESH)

    def sig(i, _):
        pl.semaphore_signal(bar, inc=1, device_id={"kv": peer(lax.rem(chip + i, chips))}, device_id_type=MESH)
        return 0
    lax.fori_loop(1, chips, sig, 0)

    def wsrc(ci):
        if ci < 4:
            return w_q.at[:, pl.ds(pl.multiple_of(c * half_cols + ci * WCOLS, WCOLS), WCOLS)]
        if ci == 4:
            return w_k.at[:, pl.ds(pl.multiple_of(c * WCOLS, WCOLS), WCOLS)]
        if ci == 5:
            return w_v.at[:, pl.ds(pl.multiple_of(c * WCOLS, WCOLS), WCOLS)]
        return w_o.at[:, pl.ds(pl.multiple_of(c * half_cols + (ci - 6) * WCOLS, WCOLS), WCOLS)]

    def wcopy(ci):
        return pltpu.make_async_copy(wsrc(ci), wring.at[ci % 4], wsem.at[ci])

    smalls = [(x_first, xin.at[0]), (next_emb, xin.at[pl.ds(1, S - 1)]), (g1, vg1), (c1, vc1), (b_q, vbq), (b_k, vbk), (b_v, vbv),
              (lf, vlf), (pw, vpw), (lens_h, lens_ref), (g2, vg2), (c2, vc2), (b_o, vbo), (w_r, vwr), (ei_h, ei_ref), (rm_h, rm_ref)]
    small_copies = [pltpu.make_async_copy(a, b, ssem.at[i]) for i, (a, b) in enumerate(smalls)]
    for cp in small_copies[:10]:
        cp.start()
    for ci in range(4):
        wcopy(ci).start()
    for cp in small_copies[10:]:
        cp.start()

    def kcopy(b):
        return pltpu.make_async_copy(k_hbm.at[b], kbuf.at[b], ksem.at[b])

    def vcopy(b):
        return pltpu.make_async_copy(v_hbm.at[b], vbuf.at[b], vsem.at[b])

    moe_copies = [pltpu.make_async_copy(src, wmoe.at[i, pl.ds(0, FE)], msem.at[i]) for i, src in enumerate((w_g, w_u, w_d))]

    wmoe[2, FE:FEP, :] = jnp.zeros((FEP - FE, D), BF16)
    lhs[...] = jnp.zeros_like(lhs)
    gs[...] = jnp.zeros_like(gs)
    ut[...] = jnp.zeros_like(ut)
    tkv[...] = jnp.zeros_like(tkv)

    def layer_norm(s, gain, bias):
        x = x32[s * B:(s + 1) * B, :]
        mean = jnp.sum(x, axis=1, keepdims=True) / D
        cen = x - mean
        var = jnp.sum(cen * cen, axis=1, keepdims=True) / D
        h[s * B:(s + 1) * B, :] = (cen * lax.rsqrt(var + NORM_EPS) * gain[...] + bias[...]).astype(BF16)

    for cp in small_copies[:10]:
        cp.wait()
    for s in range(S):
        x32[s * B:(s + 1) * B, :] = xin[s].astype(F32)
        layer_norm(s, vg1, vc1)
    hd2 = HD // 2
    row_b = lax.rem(iota((R, hd2), 0), B)
    pos = iota((R, hd2), 0) // B
    for b in range(B):
        pos = pos + jnp.where(row_b == b, lens_ref[b], 0)
    ang = pos.astype(F32) * (1.0 / (vlf[...] * vpw[...]))
    cs = jnp.cos(ang) * ROPE_MSCALE
    sn = jnp.sin(ang) * ROPE_MSCALE
    cosb[:, 0:hd2] = cs
    cosb[:, hd2:HD] = cs
    sinb[:, 0:hd2] = -sn
    sinb[:, hd2:HD] = sn
    kr, kl = iota((CORES * QR, LANES), 0), iota((CORES * QR, LANES), 1)
    kbias[...] = jnp.where((kr // QR) * KHH + lax.rem(kr, HH) // QG == lax.rem(kl, KH), 0.0, NEG_FILL)

    def rotate(x):
        return round_bf16(x * cosb[...] + pltpu.roll(x, HD // 2, 1) * sinb[...])

    def kv_start(j, _):
        b = nth(j)
        kcopy(b).start()
        vcopy(b).start()
        return 0

    def q_chunk(ci, _):
        pltpu.make_async_copy(wsrc(0), wring.at[ci], wsem.at[ci]).wait()
        off = pl.multiple_of(c * half_cols + ci * WCOLS, WCOLS)
        y = jnp.dot(h[...], wring[ci], preferred_element_type=F32) + vbq[:, pl.ds(off, WCOLS)]
        y = round_bf16(y)
        for t in range(WCOLS // HD):
            r = rotate(y[:, t * HD:(t + 1) * HD])
            hh = ci * (WCOLS // HD) + t
            for s in range(S):
                qbuf[c, pl.ds(s * HH + hh, B, stride=QR), :] = r[s * B:(s + 1) * B, :]

        @pl.when(ci == 0)
        def _():
            wcopy(4).start()

        @pl.when(ci == 1)
        def _():
            wcopy(5).start()

        @pl.when(ci == 2)
        def _():
            lax.fori_loop(0, B // 2, kv_start, 0)

        @pl.when(ci == 3)
        def _():
            lax.fori_loop(B // 2, B, kv_start, 0)
        return 0
    lax.fori_loop(0, 4, q_chunk, 0)

    pl.semaphore_wait(bar, chips)

    def to_partner(src, dst, ss, rs):
        return pltpu.make_async_remote_copy(src, dst, ss, rs, device_id={"kv": partner}, device_id_type=MESH)

    q_x = to_partner(qbuf.at[c], qbuf.at[c], qx_s, qx_r)
    q_x.start()

    wcopy(4).wait()
    y = round_bf16(jnp.dot(h[...], wring[0], preferred_element_type=F32) + vbk[:, pl.ds(pl.multiple_of(c * WCOLS, WCOLS), WCOLS)])
    for t in range(KHH):
        kt[c, t, :, :] = rotate(y[:, t * HD:(t + 1) * HD])
    wcopy(5).wait()
    y = round_bf16(jnp.dot(h[...], wring[1], preferred_element_type=F32) + vbv[:, pl.ds(pl.multiple_of(c * WCOLS, WCOLS), WCOLS)])
    for t in range(KHH):
        vt[c, t, :, :] = y[:, t * HD:(t + 1) * HD]
    k_x = to_partner(kt.at[c], kt.at[c], kx_s, kx_r)
    v_x = to_partner(vt.at[c], vt.at[c], vx_s, vx_r)
    k_x.start()
    v_x.start()

    q_x.wait_recv()
    AR = CORES * QR
    sbufs = (sb0, sb1)
    NK = T * KH
    fac = scale * math.log2(math.e)
    lane = iota((AR, LANES), 1)

    def o_copy(b):
        return pltpu.make_async_remote_copy(osend.at[b], orecv.at[chip], os_s.at[b], os_r.at[chip],
                                            device_id={"kv": peer(b)}, device_id_type=MESH)

    def p_copy(b):
        return to_partner(part.at[1 - c, b], precv.at[b], ps_s.at[b], ps_r.at[b])

    def pair_combine(b, dst, di):
        p_copy(b).wait_recv()
        m1, l1 = part[c, b, QR:QR + 1, :], part[c, b, QR + 1:QR + 2, :]
        m2, l2 = precv[b, QR:QR + 1, :], precv[b, QR + 1:QR + 2, :]
        top = jnp.maximum(m1, m2)
        f1, f2 = jnp.exp(m1 - top), jnp.exp(m2 - top)
        dst[di, 0:QR, :] = part[c, b, 0:QR, :] * to_col(f1, QR) + precv[b, 0:QR, :] * to_col(f2, QR)
        dst[di, QR:MR, :] = stat_tile(top, l1 * f1 + l2 * f2)

    def queries(b):
        q0 = qbuf[0, pl.ds(pl.multiple_of(b * QR, QR), QR), :]
        q1 = qbuf[1, pl.ds(pl.multiple_of(b * QR, QR), QR), :]
        return jnp.concatenate([q0, q1], axis=0).astype(BF16)

    def work(sb, su, wb, wu):
        CK = 256
        if sb is not None:
            lim = (lens_ref[sb] - me * T) * KH
            qb = queries(sb)
            mx = jnp.full((AR, LANES), NEG_FILL, F32)
        if wb is not None:
            mb = mbuf[wu]
            mub = jnp.where(lens_ref[wb] > me * T, mb, 0.0)
            tot = jnp.zeros((AR, LANES), F32)
            o = jnp.zeros((AR, HD), F32)
        for col in range(NK // CK):
            if sb is not None:
                x = lax.dot_general(qb, kbuf[sb, col * CK:(col + 1) * CK, :], NT, preferred_element_type=F32)
            if wb is not None:
                ws = []
                for hc in range(CK // LANES):
                    lo = col * CK + hc * LANES
                    w = jnp.exp2((sbufs[wu][:, lo:lo + LANES] - mub) * fac)
                    tot = tot + w
                    ws.append(w.astype(BF16))
                o = o + jnp.dot(jnp.concatenate(ws, axis=1), vbuf[wb, col * CK:(col + 1) * CK, :], preferred_element_type=F32)
            if sb is not None:
                for hc in range(CK // LANES):
                    lo = col * CK + hc * LANES
                    xx = jnp.where(lane < lim - lo, x[:, hc * LANES:(hc + 1) * LANES] + kbias[...], NEG_FILL)
                    sbufs[su][:, lo:lo + LANES] = xx
                    mx = jnp.maximum(mx, xx)
        if sb is not None:
            mbuf[su, :, :] = jnp.broadcast_to(jnp.max(mx, axis=1, keepdims=True), (AR, LANES))
        if wb is not None:
            l = jnp.sum(tot, axis=1, keepdims=True)
            ms = mb * scale
            for hf in range(CORES):
                part[hf, wb, 0:QR, :] = o[hf * QR:(hf + 1) * QR, :]
                part[hf, wb, QR:MR, :] = stat_tile(full_row(ms[hf * QR:(hf + 1) * QR, :]), to_row(l[hf * QR:(hf + 1) * QR, :]))

    def comb(b):
        pair_combine(b, osend, b)
        o_copy(b).start()

    LAG = 2

    def stage(j, u, last, lagged):
        kb = nth(j)
        vcopy(kb).wait()
        if not last:
            kcopy(nth(j + 1)).wait()
        for k, at in enumerate((3, 6, 9, 12)):
            @pl.when(j == at)
            def _():
                wcopy(6 + k).start()
        if last:
            for cp in moe_copies:
                cp.start()
        work(None if last else nth(j + 1), 1 - u, kb, u)
        p_copy(kb).start()
        if lagged:
            comb(nth(j - LAG))

    kcopy(nth(0)).wait()
    work(nth(0), 0, None, 0)
    for j in range(LAG):
        stage(j, j % 2, False, False)

    def attn_step(j, _):
        for u in range(2):
            @pl.when(lax.rem(j, 2) == u)
            def _():
                stage(j, u, False, True)
        return 0
    lax.fori_loop(LAG, B - 1, attn_step, 0)
    stage(B - 1, (B - 1) % 2, True, True)
    for j in range(B - LAG, B - 1):
        comb(nth(j))
    pair_combine(chip, orecv, chip)

    for s in range(S):
        for t in range(KHH):
            tkv[0, s * KHH + t:s * KHH + t + 1, :] = kt[c, t, pl.ds(s * B + chip, 1), :]
            tkv[1, s * KHH + t:s * KHH + t + 1, :] = vt[c, t, pl.ds(s * B + chip, 1), :]
    TR = tkv.shape[1]
    qb = qbuf[c, pl.ds(pl.multiple_of(chip * QR, QR), QR), :].astype(BF16)
    sc = lax.dot_general(qb, tkv[0].astype(BF16), NT, preferred_element_type=F32)
    tr, tl = iota((QR, TR), 0), iota((QR, TR), 1)
    valid = (lax.rem(tl, KHH) == lax.rem(tr, HH) // QG) & (tl // KHH <= tr // HH) & (tl < S * KHH)
    m, l, w = softmax_part(sc, valid, scale)
    orecv[chips, 0:QR, :] = jnp.dot(w, tkv[1].astype(BF16), preferred_element_type=F32)
    orecv[chips, QR:MR, :] = stat_tile(to_row(m), to_row(l))

    def o_wait(i, _):
        src = lax.rem(chip + i, chips)
        pltpu.make_async_remote_copy(osend.at[0], orecv.at[src], os_s.at[0], os_r.at[src],
                                     device_id={"kv": peer(src)}, device_id_type=MESH).wait_recv()
        return 0
    lax.fori_loop(1, chips, o_wait, 0)

    top = orecv[0, QR:QR + 1, :]
    for i in range(1, chips + 1):
        top = jnp.maximum(top, orecv[i, QR:QR + 1, :])
    tot = jnp.zeros((1, LANES), F32)
    acc = jnp.zeros((QR, LANES), F32)
    for i in range(chips + 1):
        f = jnp.exp(orecv[i, QR:QR + 1, :] - top)
        tot = tot + orecv[i, QR + 1:QR + 2, :] * f
        acc = acc + orecv[i, 0:QR, :] * to_col(f, QR)
    oxs[c, :, :] = round_bf16(acc / to_col(tot, QR))
    o_x = to_partner(oxs.at[c], oxs.at[c], ox_s, ox_r)
    o_x.start()
    for cp in small_copies[10:]:
        cp.wait()

    ctiles = WCOLS // LANES
    my_slot = pl.multiple_of(me * QR, QR)
    KROWS = HH * HD

    def fill(hf):
        for hh in range(HH):
            lhs[hf, 0:S, hh * HD:(hh + 1) * HD] = oxs[hf, pl.ds(hh, S, stride=HH), :]

    def wo_dot(hf, jn):
        return jnp.dot(lhs[hf].astype(BF16), wring[lax.rem(jn + 2, 4), pl.ds(pl.multiple_of(hf * KROWS, KROWS), KROWS), :], preferred_element_type=F32)

    fill(c)

    def wo_mine(jn, _):
        pltpu.make_async_copy(wsrc(0), wring.at[lax.rem(jn + 2, 4)], wsem.at[jn + 6]).wait()
        wacc[jn, :, :] = wo_dot(c, jn)
        return 0
    lax.fori_loop(0, 4, wo_mine, 0)
    o_x.wait_recv()
    fill(1 - c)

    GROUPS = 3
    GSIZE = -(-len(offsets) // GROUPS)

    def gatherer(buf, pieces, ss, rs, ro):
        PR = QR // pieces

        def cp(p, slot, rsem, dev):
            blk = buf.at[pl.ds(pl.multiple_of(slot * QR + p * PR, 8), PR)]
            return pltpu.make_async_remote_copy(blk, blk, ss.at[p], rsem, device_id={"kv": dev}, device_id_type=MESH)

        def all_of(count, p, rsem):
            blk = buf.at[pl.ds(0, count * PR)]
            return pltpu.make_async_remote_copy(blk, blk, ss.at[p], rsem, device_id={"kv": partner}, device_id_type=MESH)

        def send(p):
            for i, o in enumerate(offsets):
                cp(p, me, rs.at[p, i // GSIZE], peer(ahead(o))).start()
            cp(p, me, ro.at[p], partner).start()

        def finish():
            for p in range(pieces):
                for g in range(GROUPS):
                    mem = offsets[g * GSIZE:(g + 1) * GSIZE]
                    all_of(len(mem), p, rs.at[p, g]).wait_recv()
                    for o in mem:
                        cp(p, peer(behind(o)), ro.at[p], partner).start()
            for p in range(pieces):
                all_of(chips, p, ro.at[p]).wait_recv()

        def drain():
            for p in range(pieces):
                all_of(2 * chips - 1, p, ro.at[p]).wait_send()
        return send, finish, drain

    XP = 2
    XPR = QR // XP
    XT = HH // XP
    x_send, x_finish, x_drain = gatherer(xg, XP, xa_s, xa_r, xa_o)
    for p in range(XP):
        def wo_other(k, _):
            jn = p * (4 // XP) + k
            off = pl.multiple_of(c * half_cols + jn * WCOLS, WCOLS)
            d = wacc[jn] + wo_dot(1 - c, jn)
            for s in range(S):
                v = round_bf16(x32[pl.ds(s * B + chip, 1), pl.ds(off, WCOLS)] + d[s:s + 1, :] + vbo[:, pl.ds(off, WCOLS)])
                for t in range(ctiles):
                    xg[pl.ds(my_slot + p * XPR + s * XT + k * ctiles + t, 1), :] = v[:, t * LANES:(t + 1) * LANES]
            return 0
        lax.fori_loop(0, 4 // XP, wo_other, 0)
        x_send(p)

    def o_drain(i, _):
        b = lax.rem(chip + i, chips)
        p_copy(b).wait_send()

        @pl.when(i > 0)
        def _():
            o_copy(b).wait_send()
        return 0
    lax.fori_loop(0, chips, o_drain, 0)
    x_finish()
    for s in range(S):
        for hf in range(CORES):
            for t in range(HH):
                x32[s * B:(s + 1) * B, (hf * HH + t) * LANES:(hf * HH + t + 1) * LANES] = xg[pl.ds(hf * QR + (t // XT) * XPR + s * XT + t % XT, B, stride=CORES * QR), :]

    for cp in moe_copies:
        cp.wait()

    for s in range(S):
        layer_norm(s, vg2, vc2)
    logits = lax.dot_general(h[...], vwr[...], NT, preferred_element_type=F32)
    le = iota((B, E), 1)
    diag = iota((B, B), 0) == iota((B, B), 1)
    for s in range(S):
        lg = logits[s * B:(s + 1) * B, :]
        gate = jnp.zeros((B, E), F32)
        for k in range(ei_ref.shape[1]):
            masked = jnp.where(rm_ref[s, :, k, :] == 1, lg, NEG_FILL)
            ex = jnp.exp(masked - jnp.max(masked, axis=1, keepdims=True))
            p = ex / jnp.sum(ex, axis=1, keepdims=True)
            idx = jnp.sum(jnp.where(diag, jnp.broadcast_to(ei_ref[s, k:k + 1, :], (B, B)).astype(F32), 0.0), axis=1, keepdims=True)
            gate = gate + jnp.where(le.astype(F32) == idx, p, 0.0)
        gs[s * B:(s + 1) * B, 0:E] = gate
    gt[...] = jnp.transpose(gs[...])
    g_e = jnp.concatenate([gt[0:E, :]] * (LANES // E), axis=0)[:, 0:R]
    UB = 256
    for t in range(FEP // UB):
        ag = lax.dot_general(wmoe[0, t * UB:(t + 1) * UB, :], h[...], NT, preferred_element_type=F32)
        au = lax.dot_general(wmoe[1, t * UB:(t + 1) * UB, :], h[...], NT, preferred_element_type=F32)
        gg = jnp.concatenate([g_e] * (UB // LANES), axis=0)
        u = gg * (ag * jax.nn.sigmoid(ag)) * au
        ut[t * UB:(t + 1) * UB, 0:R] = jnp.where(iota((UB, R), 0) + t * UB < FE, u, 0.0)
    for t in range(FEP // LANES):
        ub[:, t * LANES:(t + 1) * LANES] = jnp.transpose(ut[t * LANES:(t + 1) * LANES, :])[0:R, :].astype(BF16)

    MP = 2
    MPR = R // MP

    def mo_copy(i, p):
        return pltpu.make_async_remote_copy(mosend.at[p, i], morecv.at[p, chip], mo_s.at[p, i], mo_r.at[p, chip],
                                            device_id={"kv": peer(i)}, device_id_type=MESH)

    def moe_pair(i, dst, di):
        to_partner(mpsend.at[i], mprecv.at[i], ps_s.at[i], ps_r.at[i]).wait_recv()
        for p in range(MP):
            dst[p, di, :, :] = mine[i, p * MPR:(p + 1) * MPR, :] + mprecv[i, p * MPR:(p + 1) * MPR, :]

    GRP = 4

    def moe_out(g, _):
        for k in range(GRP):
            i = nth(g * GRP + k)
            pp = round_bf16(jnp.dot(ub[...], wmoe[2, :, pl.ds(pl.multiple_of(i * PC, PC), PC)], preferred_element_type=F32))
            p0, p1 = pp[:, :LANES], pp[:, LANES:]
            mpsend[i, :, :] = jnp.where(c == 0, p1, p0)
            mine[i, :, :] = jnp.where(c == 0, p0, p1)
        for k in range(GRP):
            i = nth(g * GRP + k)
            to_partner(mpsend.at[i], mprecv.at[i], ps_s.at[i], ps_r.at[i]).start()
        return 0

    def moe_fwd(j, _):
        i = nth(j)
        moe_pair(i, mosend, i)
        mo_copy(i, 0).start()
        return 0
    lax.fori_loop(0, 2, moe_out, 0)

    def moe_both(g, _):
        moe_out(g, 0)
        lax.fori_loop((g - 2) * GRP, (g - 1) * GRP, moe_fwd, 0)
        return 0
    lax.fori_loop(2, chips // GRP, moe_both, 0)
    lax.fori_loop(chips - 2 * GRP, chips - 1, moe_fwd, 0)

    def mo_rest(j, _):
        for p in range(1, MP):
            mo_copy(nth(j), p).start()
        return 0
    lax.fori_loop(0, chips - 1, mo_rest, 0)
    moe_pair(chip, morecv, chip)

    k_x.wait_recv()
    v_x.wait_recv()
    for src, dst in ((kt, tk_ref), (vt, tv_ref)):
        for hf in range(CORES):
            for t in range(KHH):
                for s in range(S):
                    t32[pl.ds(s * KH + hf * KHH + t, B, stride=S * KH), :] = src[hf, t, s * B:(s + 1) * B, :]
        dst[...] = t32[...].astype(BF16)

    y_send, y_finish, y_drain = gatherer(yg, MP, ya_s, ya_r, ya_o)
    for p in range(MP):
        def mo_wait(i, _):
            src = lax.rem(chip + i, chips)
            pltpu.make_async_remote_copy(mosend.at[p, 0], morecv.at[p, src], mo_s.at[p, 0], mo_r.at[p, src],
                                         device_id={"kv": peer(src)}, device_id_type=MESH).wait_recv()
            return 0
        lax.fori_loop(1, chips, mo_wait, 0)
        tot = morecv[p, 0]
        for i in range(1, chips):
            tot = tot + morecv[p, i]
        yg[pl.ds(my_slot + p * MPR, MPR), :] = round_bf16(x32[p * MPR:(p + 1) * MPR, pl.ds(pl.multiple_of(me * LANES, LANES), LANES)] + tot)
        y_send(p)
    y_finish()
    for d in range(chips * CORES):
        for s in range(S):
            out_ref[s, :, d * LANES:(d + 1) * LANES] = yg[d * QR + s * B:d * QR + (s + 1) * B, :].astype(BF16)

    q_x.wait_send()
    k_x.wait_send()
    v_x.wait_send()
    o_x.wait_send()

    def drain(i, _):
        b = lax.rem(chip + i, chips)
        to_partner(mpsend.at[b], mprecv.at[b], ps_s.at[b], ps_r.at[b]).wait_send()

        @pl.when(i > 0)
        def _():
            for p in range(MP):
                mo_copy(b, p).wait_send()
        return 0
    lax.fori_loop(0, chips, drain, 0)
    x_drain()
    y_drain()


def copy_out(a, b, d, oa, ob, od, sem):
    cps = [pltpu.make_async_copy(x, y, sem.at[i]) for i, (x, y) in enumerate(((a, oa), (b, ob), (d, od)))]
    for cp in cps:
        cp.start()
    for cp in cps:
        cp.wait()


def finish(*arrs):
    return pl.pallas_call(
        copy_out,
        name="copy_out",
        out_shape=tuple(jax.ShapeDtypeStruct(a.shape, a.dtype) for a in arrs),
        in_specs=[pl.BlockSpec(memory_space=pltpu.VMEM)] * len(arrs),
        out_specs=(pl.BlockSpec(memory_space=pl.ANY),) * len(arrs),
        scratch_shapes=[pltpu.SemaphoreType.DMA((len(arrs),))],
        compiler_params=pltpu.CompilerParams(vmem_limit_bytes=1 << 20),
    )(*arrs)


def solution(mesh):
    n = mesh.shape["kv"]
    chips = n // CORES

    def layer_steps(x_first, next_emb, k_cache, v_cache, seq_len, ln1_gain, ln1_bias, w_q, b_q, w_k, b_k, w_v, b_v, w_o, b_o, ln2_gain, ln2_bias, w_router, w_gate, w_up, w_down, long_factor, expert_idx, route_mask):
        B, T, KH, HD = k_cache.shape
        D = x_first.shape[1]
        H = w_q.shape[1] // HD
        S = next_emb.shape[0] + 1
        E = w_router.shape[1]
        FE = w_gate.shape[0] * w_gate.shape[2]
        FEP = -(-FE // 256) * 256
        R = S * B
        HH, KHH = H // CORES, KH // CORES
        QR = S * HH
        MR = QR + 8
        if B != chips or D != n * LANES or w_q.shape[1] != D or QR != R:
            raise ValueError("unsupported sizes")
        dims = dict(S=S, B=B, D=D, T=T, KH=KH, HD=HD, H=H, E=E, FE=FE, chips=chips)
        half = HD // 2
        power = np.float32(ROPE_BASE) ** (np.arange(half, dtype=np.float32) * np.float32(2.0) / np.float32(HD))
        pw = jnp.asarray(power[None, :].astype(np.float32))
        lf = long_factor[None, :]
        row = lambda a: a.reshape(1, -1)
        args = (seq_len, expert_idx.transpose(0, 2, 1), route_mask,
                x_first, next_emb, k_cache.reshape(B, T * KH, HD), v_cache.reshape(B, T * KH, HD), row(ln1_gain), row(ln1_bias),
                w_q, row(b_q), w_k, row(b_k), w_v, row(b_v), w_o, row(b_o), row(ln2_gain), row(ln2_bias), w_router.T,
                w_gate.transpose(2, 0, 1).reshape(FE, D), w_up.transpose(2, 0, 1).reshape(FE, D), w_down.transpose(1, 0, 2).reshape(FE, D), lf, pw)
        V = pltpu.VMEM
        DS = pltpu.SemaphoreType.DMA
        scratch = [
            pltpu.SMEM((B,), jnp.int32), V(expert_idx.transpose(0, 2, 1).shape, jnp.int32), V(route_mask.shape, jnp.int32),
            V((4, D, WCOLS), BF16), V((B, T * KH, HD), BF16), V((B, T * KH, HD), BF16), V((3, FEP, D), BF16),
            V((S, B, D), BF16), V((R, D), F32), V((R, D), BF16),
            V((1, D), F32), V((1, D), F32), V((1, D), F32), V((1, D), F32), V((1, D), F32), V((1, w_q.shape[1]), F32),
            V((1, w_k.shape[1]), F32), V((1, w_v.shape[1]), F32), V((1, half), F32), V((1, half), F32), V((E, D), BF16),
            V((CORES, B * QR, HD), F32), V((R, HD), F32), V((R, HD), F32), V((CORES, KHH, R, HD), F32), V((CORES, KHH, R, HD), F32), V((2, 16, HD), F32),
            V((CORES * QR, LANES), F32), V((CORES * QR, T * KH), F32), V((CORES * QR, T * KH), F32), V((2, CORES * QR, LANES), F32),
            V((CORES, B, MR, HD), F32), V((B, MR, HD), F32), V((B, MR, HD), F32), V((chips + 1, MR, HD), F32),
            V((CORES, QR, HD), F32), V((CORES, 8, HH * HD), F32), V((4, 8, WCOLS), F32), V((n * QR, HD), F32), V((LANES, LANES), F32), V((LANES, LANES), F32), V((FEP, LANES), F32), V((R, FEP), BF16),
            V((chips, R, LANES), F32), V((chips, R, LANES), F32), V((chips, R, LANES), F32), V((2, chips, R // 2, LANES), F32), V((2, chips, R // 2, LANES), F32),
            V((n * QR, LANES), F32), V((B * S * KH, HD), F32),
            DS((10,)), DS((B,)), DS((B,)), DS((3,)), DS((16,)), DS, DS, DS, DS, DS, DS, DS((B,)), DS((B,)), DS((chips,)), DS((chips,)), DS, DS,
            DS((2,)), DS((2, 3)), DS((2,)), DS((2, chips)), DS((2, chips)), DS((2,)), DS((2, 3)), DS((2,)),
        ]
        vm = pl.BlockSpec(memory_space=pltpu.VMEM)
        anys = pl.BlockSpec(memory_space=pl.ANY)
        hidden, tk, tv = pl.pallas_call(
            functools.partial(kernel, dims),
            name="decode_layer",
            out_shape=(V((S, B, D), BF16), V((B * S * KH, HD), BF16), V((B * S * KH, HD), BF16)),
            in_specs=[anys] * len(args),
            out_specs=(vm, vm, vm),
            scratch_shapes=scratch,
            compiler_params=pltpu.CompilerParams(collective_id=0, has_side_effects=True, vmem_limit_bytes=VMEM_BYTES),
        )(*args)
        hidden, tk, tv = finish(hidden, tk, tv)
        return hidden, tk.reshape(B, S, KH, HD), tv.reshape(B, S, KH, HD)

    replicated = P()
    in_specs = (P('dp'), P(None, 'dp'), P('dp', 'kv'), P('dp', 'kv'), P('dp')) + (replicated,) * 13 + (P(None, None, 'kv'), P(None, None, 'kv'), P(None, 'kv'), replicated, P(None, 'dp'), P(None, 'dp'))
    out_specs = (P(None, 'dp'), P('dp'), P('dp'))
    return jax.shard_map(layer_steps, mesh=mesh, in_specs=in_specs, out_specs=out_specs, check_vma=False)
```

```python
import functools
import math

import jax
import jax.numpy as jnp
import numpy as np
from jax import lax
from jax.experimental import pallas as pl
from jax.experimental.pallas import tpu as pltpu
from jax.sharding import PartitionSpec as P

ROPE_BASE = 10000.0
ROPE_MSCALE = math.sqrt(1.0 + math.log(32.0) / math.log(4096.0))
NORM_EPS = 1e-5
NEG_FILL = -1e30
MESH = pl.DeviceIdType.MESH
F32 = jnp.float32
BF16 = jnp.bfloat16
LANES = 128
WCOLS = 512
CORES = 2
VMEM_BYTES = 64 * 1024 * 1024 - 4 * 1024 * 1024
NT = (((1,), (1,)), ((), ()))


def iota(shape, dim):
    return lax.broadcasted_iota(jnp.int32, shape, dim)


def to_row(col):
    rows = col.shape[0]
    pick = iota((rows, LANES), 0) == iota((rows, LANES), 1)
    return jnp.sum(jnp.where(pick, jnp.broadcast_to(col, (rows, LANES)), 0.0), axis=0, keepdims=True)


def full_row(full):
    rows = full.shape[0]
    pick = iota((rows, LANES), 0) == iota((rows, LANES), 1)
    return jnp.sum(jnp.where(pick, full, 0.0), axis=0, keepdims=True)


def to_col(row, rows):
    pick = iota((rows, LANES), 0) == iota((rows, LANES), 1)
    return jnp.sum(jnp.where(pick, jnp.broadcast_to(row, (rows, LANES)), 0.0), axis=1, keepdims=True)


def stat_tile(m_row, l_row):
    r = iota((8, LANES), 0)
    return jnp.where(r == 0, jnp.broadcast_to(m_row, (8, LANES)), jnp.where(r == 1, jnp.broadcast_to(l_row, (8, LANES)), 0.0))


def softmax_part(s_raw, valid, scale):
    s = jnp.where(valid, s_raw * scale, NEG_FILL)
    m = jnp.max(s, axis=1, keepdims=True)
    w = jnp.where(valid, jnp.exp(s - m), 0.0)
    return m, jnp.sum(w, axis=1, keepdims=True), w.astype(BF16)


def round_bf16(x):
    return x.astype(BF16).astype(F32)


def kernel(dims, lens_h, ei_h, rm_h,
           x_first, next_emb, k_hbm, v_hbm, g1, c1, w_q, b_q, w_k, b_k, w_v, b_v, w_o, b_o, g2, c2, w_r, w_g, w_u, w_d, lf, pw,
           out_ref, tk_ref, tv_ref,
           lens_ref, ei_ref, rm_ref, wring, kbuf, vbuf, wmoe, xin, x32, h, vg1, vc1, vg2, vc2, vbo, vbq, vbk, vbv, vlf, vpw, vwr,
           qbuf, cosb, sinb, kt, vt, tkv, kbias, sb0, sb1, mbuf, part, precv, osend, orecv, oxs, lhs, wacc, xg, gs, gt, ut, ub, mine, mpsend, mprecv, mosend, morecv, yg, t32,
           wsem, ksem, vsem, msem, ssem, qx_s, qx_r, kx_s, kx_r, vx_s, vx_r, ps_s, ps_r, os_s, os_r, ox_s, ox_r,
           xa_s, xa_r, xa_o, mo_s, mo_r, ya_s, ya_r, ya_o):
    S, B, D, T, KH, HD, H, E, FE, chips = (dims[k] for k in ("S", "B", "D", "T", "KH", "HD", "H", "E", "FE", "chips"))
    R = S * B
    HH, KHH = H // CORES, KH // CORES
    half_cols = D // CORES
    QG = H // KH
    QR = S * HH
    MR = QR + 8
    PC = LANES * CORES
    FEP = wmoe.shape[1]
    scale = HD ** -0.5
    me = lax.axis_index("kv")
    chip = lax.div(me, CORES)
    c = lax.rem(me, CORES)
    partner = chip * CORES + (1 - c)

    def peer(ch):
        return ch * CORES + c

    side = math.isqrt(chips)
    cy, cx = lax.div(chip, side), lax.rem(chip, side)

    def ring(k):
        return side // 2 + lax.div(k + 1, 2) * (1 - 2 * lax.rem(k, 2))

    def nth(j):
        j = jnp.int32(j)
        return lax.rem(cy + ring(lax.div(j, side)), side) * side + lax.rem(cx + ring(lax.rem(j, side)), side)

    def dist(d):
        return min(d, side - d)
    offsets = sorted([(dy, dx) for dy in range(side) for dx in range(side) if dy or dx], key=lambda o: -(dist(o[0]) + dist(o[1])))

    def ahead(o):
        return lax.rem(cy + o[0], side) * side + lax.rem(cx + o[1], side)

    def behind(o):
        return lax.rem(cy + side - o[0], side) * side + lax.rem(cx + side - o[1], side)

    bar = pltpu.get_barrier_semaphore()
    pl.semaphore_signal(bar, inc=1, device_id={"kv": partner}, device_id_type=MESH)

    def sig(i, _):
        pl.semaphore_signal(bar, inc=1, device_id={"kv": peer(lax.rem(chip + i, chips))}, device_id_type=MESH)
        return 0
    lax.fori_loop(1, chips, sig, 0)

    def wsrc(ci):
        if ci < 4:
            return w_q.at[:, pl.ds(pl.multiple_of(c * half_cols + ci * WCOLS, WCOLS), WCOLS)]
        if ci == 4:
            return w_k.at[:, pl.ds(pl.multiple_of(c * WCOLS, WCOLS), WCOLS)]
        if ci == 5:
            return w_v.at[:, pl.ds(pl.multiple_of(c * WCOLS, WCOLS), WCOLS)]
        return w_o.at[:, pl.ds(pl.multiple_of(c * half_cols + (ci - 6) * WCOLS, WCOLS), WCOLS)]

    def wcopy(ci):
        return pltpu.make_async_copy(wsrc(ci), wring.at[ci % 4], wsem.at[ci])

    smalls = [(x_first, xin.at[0]), (next_emb, xin.at[pl.ds(1, S - 1)]), (g1, vg1), (c1, vc1), (b_q, vbq), (b_k, vbk), (b_v, vbv),
              (lf, vlf), (pw, vpw), (lens_h, lens_ref), (g2, vg2), (c2, vc2), (b_o, vbo), (w_r, vwr), (ei_h, ei_ref), (rm_h, rm_ref)]
    small_copies = [pltpu.make_async_copy(a, b, ssem.at[i]) for i, (a, b) in enumerate(smalls)]
    for cp in small_copies[:10]:
        cp.start()
    for ci in range(4):
        wcopy(ci).start()
    for cp in small_copies[10:]:
        cp.start()

    def kcopy(b):
        return pltpu.make_async_copy(k_hbm.at[b], kbuf.at[b], ksem.at[b])

    def vcopy(b):
        return pltpu.make_async_copy(v_hbm.at[b], vbuf.at[b], vsem.at[b])

    moe_copies = [pltpu.make_async_copy(src, wmoe.at[i, pl.ds(0, FE)], msem.at[i]) for i, src in enumerate((w_g, w_u, w_d))]

    wmoe[2, FE:FEP, :] = jnp.zeros((FEP - FE, D), BF16)
    lhs[...] = jnp.zeros_like(lhs)
    gs[...] = jnp.zeros_like(gs)
    ut[...] = jnp.zeros_like(ut)
    tkv[...] = jnp.zeros_like(tkv)

    def layer_norm(s, gain, bias):
        x = x32[s * B:(s + 1) * B, :]
        mean = jnp.sum(x, axis=1, keepdims=True) / D
        cen = x - mean
        var = jnp.sum(cen * cen, axis=1, keepdims=True) / D
        h[s * B:(s + 1) * B, :] = (cen * lax.rsqrt(var + NORM_EPS) * gain[...] + bias[...]).astype(BF16)

    for cp in small_copies[:10]:
        cp.wait()
    for s in range(S):
        x32[s * B:(s + 1) * B, :] = xin[s].astype(F32)
        layer_norm(s, vg1, vc1)
    hd2 = HD // 2
    row_b = lax.rem(iota((R, hd2), 0), B)
    pos = iota((R, hd2), 0) // B
    for b in range(B):
        pos = pos + jnp.where(row_b == b, lens_ref[b], 0)
    ang = pos.astype(F32) * (1.0 / (vlf[...] * vpw[...]))
    cs = jnp.cos(ang) * ROPE_MSCALE
    sn = jnp.sin(ang) * ROPE_MSCALE
    cosb[:, 0:hd2] = cs
    cosb[:, hd2:HD] = cs
    sinb[:, 0:hd2] = -sn
    sinb[:, hd2:HD] = sn
    kr, kl = iota((CORES * QR, LANES), 0), iota((CORES * QR, LANES), 1)
    kbias[...] = jnp.where((kr // QR) * KHH + lax.rem(kr, HH) // QG == lax.rem(kl, KH), float(jnp.finfo(F32).max), NEG_FILL)

    def rotate(x):
        return round_bf16(x * cosb[...] + pltpu.roll(x, HD // 2, 1) * sinb[...])

    def kv_start(j, _):
        b = nth(j)
        kcopy(b).start()
        vcopy(b).start()
        return 0

    def q_chunk(ci, _):
        pltpu.make_async_copy(wsrc(0), wring.at[ci], wsem.at[ci]).wait()
        off = pl.multiple_of(c * half_cols + ci * WCOLS, WCOLS)
        y = jnp.dot(h[...], wring[ci], preferred_element_type=F32) + vbq[:, pl.ds(off, WCOLS)]
        y = round_bf16(y)
        for t in range(WCOLS // HD):
            r = rotate(y[:, t * HD:(t + 1) * HD])
            hh = ci * (WCOLS // HD) + t
            for s in range(S):
                qbuf[c, pl.ds(s * HH + hh, B, stride=QR), :] = r[s * B:(s + 1) * B, :]

        @pl.when(ci == 0)
        def _():
            wcopy(4).start()

        @pl.when(ci == 1)
        def _():
            wcopy(5).start()

        @pl.when(ci == 2)
        def _():
            lax.fori_loop(0, B // 2, kv_start, 0)

        @pl.when(ci == 3)
        def _():
            lax.fori_loop(B // 2, B, kv_start, 0)
        return 0
    lax.fori_loop(0, 4, q_chunk, 0)

    pl.semaphore_wait(bar, chips)

    def to_partner(src, dst, ss, rs):
        return pltpu.make_async_remote_copy(src, dst, ss, rs, device_id={"kv": partner}, device_id_type=MESH)

    q_x = to_partner(qbuf.at[c], qbuf.at[c], qx_s, qx_r)
    q_x.start()

    wcopy(4).wait()
    y = round_bf16(jnp.dot(h[...], wring[0], preferred_element_type=F32) + vbk[:, pl.ds(pl.multiple_of(c * WCOLS, WCOLS), WCOLS)])
    for t in range(KHH):
        kt[c, t, :, :] = rotate(y[:, t * HD:(t + 1) * HD])
    wcopy(5).wait()
    y = round_bf16(jnp.dot(h[...], wring[1], preferred_element_type=F32) + vbv[:, pl.ds(pl.multiple_of(c * WCOLS, WCOLS), WCOLS)])
    for t in range(KHH):
        vt[c, t, :, :] = y[:, t * HD:(t + 1) * HD]
    k_x = to_partner(kt.at[c], kt.at[c], kx_s, kx_r)
    v_x = to_partner(vt.at[c], vt.at[c], vx_s, vx_r)
    k_x.start()
    v_x.start()

    q_x.wait_recv()
    AR = CORES * QR
    sbufs = (sb0, sb1)
    NK = T * KH
    fac = scale * math.log2(math.e)
    lane = iota((AR, LANES), 1)

    def o_copy(b):
        return pltpu.make_async_remote_copy(osend.at[b], orecv.at[chip], os_s.at[b], os_r.at[chip],
                                            device_id={"kv": peer(b)}, device_id_type=MESH)

    def p_copy(b):
        return to_partner(part.at[1 - c, b], precv.at[b], ps_s.at[b], ps_r.at[b])

    def pair_combine(b, dst, di):
        p_copy(b).wait_recv()
        m1, l1 = part[c, b, QR:QR + 1, :], part[c, b, QR + 1:QR + 2, :]
        m2, l2 = precv[b, QR:QR + 1, :], precv[b, QR + 1:QR + 2, :]
        top = jnp.maximum(m1, m2)
        f1, f2 = jnp.exp(m1 - top), jnp.exp(m2 - top)
        dst[di, 0:QR, :] = part[c, b, 0:QR, :] * to_col(f1, QR) + precv[b, 0:QR, :] * to_col(f2, QR)
        dst[di, QR:MR, :] = stat_tile(top, l1 * f1 + l2 * f2)

    def queries(b):
        q0 = qbuf[0, pl.ds(pl.multiple_of(b * QR, QR), QR), :]
        q1 = qbuf[1, pl.ds(pl.multiple_of(b * QR, QR), QR), :]
        return jnp.concatenate([q0, q1], axis=0).astype(BF16)

    def work(sb, su, wb, wu):
        CK = 256
        if sb is not None:
            lim = (lens_ref[sb] - me * T) * KH
            qb = queries(sb)
            mx = jnp.full((AR, LANES), NEG_FILL, F32)
        if wb is not None:
            mb = mbuf[wu]
            mub = jnp.where(lens_ref[wb] > me * T, mb, 0.0)
            tot = jnp.zeros((AR, LANES), F32)
            o = jnp.zeros((AR, HD), F32)
        for col in range(NK // CK):
            if sb is not None:
                x = lax.dot_general(qb, kbuf[sb, col * CK:(col + 1) * CK, :], NT, preferred_element_type=F32)
            if wb is not None:
                ws = []
                for hc in range(CK // LANES):
                    lo = col * CK + hc * LANES
                    w = jnp.exp2((sbufs[wu][:, lo:lo + LANES] - mub) * fac)
                    tot = tot + w
                    ws.append(w.astype(BF16))
                o = o + jnp.dot(jnp.concatenate(ws, axis=1), vbuf[wb, col * CK:(col + 1) * CK, :], preferred_element_type=F32)
            if sb is not None:
                for hc in range(CK // LANES):
                    lo = col * CK + hc * LANES
                    xx = jnp.where(lane < lim - lo, jnp.minimum(x[:, hc * LANES:(hc + 1) * LANES], kbias[...]), NEG_FILL)
                    sbufs[su][:, lo:lo + LANES] = xx
                    mx = jnp.maximum(mx, xx)
        if sb is not None:
            mbuf[su, :, :] = jnp.broadcast_to(jnp.max(mx, axis=1, keepdims=True), (AR, LANES))
        if wb is not None:
            l = jnp.sum(tot, axis=1, keepdims=True)
            ms = mb * scale
            for hf in range(CORES):
                part[hf, wb, 0:QR, :] = o[hf * QR:(hf + 1) * QR, :]
                part[hf, wb, QR:MR, :] = stat_tile(full_row(ms[hf * QR:(hf + 1) * QR, :]), to_row(l[hf * QR:(hf + 1) * QR, :]))

    def comb(b):
        pair_combine(b, osend, b)
        o_copy(b).start()

    LAG = 2

    def stage(j, u, last, lagged):
        kb = nth(j)
        vcopy(kb).wait()
        if not last:
            kcopy(nth(j + 1)).wait()
        for k, at in enumerate((3, 6, 9, 12)):
            @pl.when(j == at)
            def _():
                wcopy(6 + k).start()
        if last:
            for cp in moe_copies:
                cp.start()
        work(None if last else nth(j + 1), 1 - u, kb, u)
        p_copy(kb).start()
        if lagged:
            comb(nth(j - LAG))

    kcopy(nth(0)).wait()
    work(nth(0), 0, None, 0)
    for j in range(LAG):
        stage(j, j % 2, False, False)

    def attn_step(j, _):
        for u in range(2):
            @pl.when(lax.rem(j, 2) == u)
            def _():
                stage(j, u, False, True)
        return 0
    lax.fori_loop(LAG, B - 1, attn_step, 0)
    stage(B - 1, (B - 1) % 2, True, True)
    for j in range(B - LAG, B - 1):
        comb(nth(j))
    pair_combine(chip, orecv, chip)

    for s in range(S):
        for t in range(KHH):
            tkv[0, s * KHH + t:s * KHH + t + 1, :] = kt[c, t, pl.ds(s * B + chip, 1), :]
            tkv[1, s * KHH + t:s * KHH + t + 1, :] = vt[c, t, pl.ds(s * B + chip, 1), :]
    TR = tkv.shape[1]
    qb = qbuf[c, pl.ds(pl.multiple_of(chip * QR, QR), QR), :].astype(BF16)
    sc = lax.dot_general(qb, tkv[0].astype(BF16), NT, preferred_element_type=F32)
    tr, tl = iota((QR, TR), 0), iota((QR, TR), 1)
    valid = (lax.rem(tl, KHH) == lax.rem(tr, HH) // QG) & (tl // KHH <= tr // HH) & (tl < S * KHH)
    m, l, w = softmax_part(sc, valid, scale)
    orecv[chips, 0:QR, :] = jnp.dot(w, tkv[1].astype(BF16), preferred_element_type=F32)
    orecv[chips, QR:MR, :] = stat_tile(to_row(m), to_row(l))

    def o_wait(i, _):
        src = lax.rem(chip + i, chips)
        pltpu.make_async_remote_copy(osend.at[0], orecv.at[src], os_s.at[0], os_r.at[src],
                                     device_id={"kv": peer(src)}, device_id_type=MESH).wait_recv()
        return 0
    lax.fori_loop(1, chips, o_wait, 0)

    top = orecv[0, QR:QR + 1, :]
    for i in range(1, chips + 1):
        top = jnp.maximum(top, orecv[i, QR:QR + 1, :])
    tot = jnp.zeros((1, LANES), F32)
    acc = jnp.zeros((QR, LANES), F32)
    for i in range(chips + 1):
        f = jnp.exp(orecv[i, QR:QR + 1, :] - top)
        tot = tot + orecv[i, QR + 1:QR + 2, :] * f
        acc = acc + orecv[i, 0:QR, :] * to_col(f, QR)
    oxs[c, :, :] = round_bf16(acc / to_col(tot, QR))
    o_x = to_partner(oxs.at[c], oxs.at[c], ox_s, ox_r)
    o_x.start()
    for cp in small_copies[10:]:
        cp.wait()

    ctiles = WCOLS // LANES
    my_slot = pl.multiple_of(me * QR, QR)
    KROWS = HH * HD

    def fill(hf):
        for hh in range(HH):
            lhs[hf, 0:S, hh * HD:(hh + 1) * HD] = oxs[hf, pl.ds(hh, S, stride=HH), :]

    def wo_dot(hf, jn):
        return jnp.dot(lhs[hf].astype(BF16), wring[lax.rem(jn + 2, 4), pl.ds(pl.multiple_of(hf * KROWS, KROWS), KROWS), :], preferred_element_type=F32)

    fill(c)

    def wo_mine(jn, _):
        pltpu.make_async_copy(wsrc(0), wring.at[lax.rem(jn + 2, 4)], wsem.at[jn + 6]).wait()
        wacc[jn, :, :] = wo_dot(c, jn)
        return 0
    lax.fori_loop(0, 4, wo_mine, 0)
    o_x.wait_recv()
    fill(1 - c)

    GROUPS = 3
    GSIZE = -(-len(offsets) // GROUPS)

    def gatherer(buf, pieces, ss, rs, ro):
        PR = QR // pieces

        def cp(p, slot, rsem, dev):
            blk = buf.at[pl.ds(pl.multiple_of(slot * QR + p * PR, 8), PR)]
            return pltpu.make_async_remote_copy(blk, blk, ss.at[p], rsem, device_id={"kv": dev}, device_id_type=MESH)

        def all_of(count, p, rsem):
            blk = buf.at[pl.ds(0, count * PR)]
            return pltpu.make_async_remote_copy(blk, blk, ss.at[p], rsem, device_id={"kv": partner}, device_id_type=MESH)

        def send(p):
            for i, o in enumerate(offsets):
                cp(p, me, rs.at[p, i // GSIZE], peer(ahead(o))).start()
            cp(p, me, ro.at[p], partner).start()

        def finish():
            for p in range(pieces):
                for g in range(GROUPS):
                    mem = offsets[g * GSIZE:(g + 1) * GSIZE]
                    all_of(len(mem), p, rs.at[p, g]).wait_recv()
                    for o in mem:
                        cp(p, peer(behind(o)), ro.at[p], partner).start()
            for p in range(pieces):
                all_of(chips, p, ro.at[p]).wait_recv()

        def drain():
            for p in range(pieces):
                all_of(2 * chips - 1, p, ro.at[p]).wait_send()
        return send, finish, drain

    XP = 2
    XPR = QR // XP
    XT = HH // XP
    x_send, x_finish, x_drain = gatherer(xg, XP, xa_s, xa_r, xa_o)
    for p in range(XP):
        def wo_other(k, _):
            jn = p * (4 // XP) + k
            off = pl.multiple_of(c * half_cols + jn * WCOLS, WCOLS)
            d = wacc[jn] + wo_dot(1 - c, jn)
            for s in range(S):
                v = round_bf16(x32[pl.ds(s * B + chip, 1), pl.ds(off, WCOLS)] + d[s:s + 1, :] + vbo[:, pl.ds(off, WCOLS)])
                for t in range(ctiles):
                    xg[pl.ds(my_slot + p * XPR + s * XT + k * ctiles + t, 1), :] = v[:, t * LANES:(t + 1) * LANES]
            return 0
        lax.fori_loop(0, 4 // XP, wo_other, 0)
        x_send(p)

    def o_drain(i, _):
        b = lax.rem(chip + i, chips)
        p_copy(b).wait_send()

        @pl.when(i > 0)
        def _():
            o_copy(b).wait_send()
        return 0
    lax.fori_loop(0, chips, o_drain, 0)
    x_finish()
    for s in range(S):
        for hf in range(CORES):
            for t in range(HH):
                x32[s * B:(s + 1) * B, (hf * HH + t) * LANES:(hf * HH + t + 1) * LANES] = xg[pl.ds(hf * QR + (t // XT) * XPR + s * XT + t % XT, B, stride=CORES * QR), :]

    for cp in moe_copies:
        cp.wait()

    for s in range(S):
        layer_norm(s, vg2, vc2)
    logits = lax.dot_general(h[...], vwr[...], NT, preferred_element_type=F32)
    le = iota((B, E), 1)
    diag = iota((B, B), 0) == iota((B, B), 1)
    for s in range(S):
        lg = logits[s * B:(s + 1) * B, :]
        gate = jnp.zeros((B, E), F32)
        for k in range(ei_ref.shape[1]):
            masked = jnp.where(rm_ref[s, :, k, :] == 1, lg, NEG_FILL)
            ex = jnp.exp(masked - jnp.max(masked, axis=1, keepdims=True))
            p = ex / jnp.sum(ex, axis=1, keepdims=True)
            idx = jnp.sum(jnp.where(diag, jnp.broadcast_to(ei_ref[s, k:k + 1, :], (B, B)).astype(F32), 0.0), axis=1, keepdims=True)
            gate = gate + jnp.where(le.astype(F32) == idx, p, 0.0)
        gs[s * B:(s + 1) * B, 0:E] = gate
    gt[...] = jnp.transpose(gs[...])
    g_e = jnp.concatenate([gt[0:E, :]] * (LANES // E), axis=0)[:, 0:R]
    UB = 256
    for t in range(FEP // UB):
        ag = lax.dot_general(wmoe[0, t * UB:(t + 1) * UB, :], h[...], NT, preferred_element_type=F32)
        au = lax.dot_general(wmoe[1, t * UB:(t + 1) * UB, :], h[...], NT, preferred_element_type=F32)
        gg = jnp.concatenate([g_e] * (UB // LANES), axis=0)
        u = gg * (ag * jax.nn.sigmoid(ag)) * au
        ut[t * UB:(t + 1) * UB, 0:R] = jnp.where(iota((UB, R), 0) + t * UB < FE, u, 0.0)
    for t in range(FEP // LANES):
        ub[:, t * LANES:(t + 1) * LANES] = jnp.transpose(ut[t * LANES:(t + 1) * LANES, :])[0:R, :].astype(BF16)

    MP = 2
    MPR = R // MP

    def mo_copy(i, p):
        return pltpu.make_async_remote_copy(mosend.at[p, i], morecv.at[p, chip], mo_s.at[p, i], mo_r.at[p, chip],
                                            device_id={"kv": peer(i)}, device_id_type=MESH)

    def moe_pair(i, dst, di):
        to_partner(mpsend.at[i], mprecv.at[i], ps_s.at[i], ps_r.at[i]).wait_recv()
        for p in range(MP):
            dst[p, di, :, :] = mine[i, p * MPR:(p + 1) * MPR, :] + mprecv[i, p * MPR:(p + 1) * MPR, :]

    GRP = 4

    def moe_out(g, _):
        for k in range(GRP):
            i = nth(g * GRP + k)
            pp = round_bf16(jnp.dot(ub[...], wmoe[2, :, pl.ds(pl.multiple_of(i * PC, PC), PC)], preferred_element_type=F32))
            p0, p1 = pp[:, :LANES], pp[:, LANES:]
            mpsend[i, :, :] = jnp.where(c == 0, p1, p0)
            mine[i, :, :] = jnp.where(c == 0, p0, p1)
        for k in range(GRP):
            i = nth(g * GRP + k)
            to_partner(mpsend.at[i], mprecv.at[i], ps_s.at[i], ps_r.at[i]).start()
        return 0

    def moe_fwd(j, _):
        i = nth(j)
        moe_pair(i, mosend, i)
        mo_copy(i, 0).start()
        return 0
    lax.fori_loop(0, 2, moe_out, 0)

    def moe_both(g, _):
        moe_out(g, 0)
        lax.fori_loop((g - 2) * GRP, (g - 1) * GRP, moe_fwd, 0)
        return 0
    lax.fori_loop(2, chips // GRP, moe_both, 0)
    lax.fori_loop(chips - 2 * GRP, chips - 1, moe_fwd, 0)

    def mo_rest(j, _):
        for p in range(1, MP):
            mo_copy(nth(j), p).start()
        return 0
    lax.fori_loop(0, chips - 1, mo_rest, 0)
    moe_pair(chip, morecv, chip)

    k_x.wait_recv()
    v_x.wait_recv()
    for src, dst in ((kt, tk_ref), (vt, tv_ref)):
        for hf in range(CORES):
            for t in range(KHH):
                for s in range(S):
                    t32[pl.ds(s * KH + hf * KHH + t, B, stride=S * KH), :] = src[hf, t, s * B:(s + 1) * B, :]
        dst[...] = t32[...].astype(BF16)

    y_send, y_finish, y_drain = gatherer(yg, MP, ya_s, ya_r, ya_o)
    for p in range(MP):
        def mo_wait(i, _):
            src = lax.rem(chip + i, chips)
            pltpu.make_async_remote_copy(mosend.at[p, 0], morecv.at[p, src], mo_s.at[p, 0], mo_r.at[p, src],
                                         device_id={"kv": peer(src)}, device_id_type=MESH).wait_recv()
            return 0
        lax.fori_loop(1, chips, mo_wait, 0)
        tot = morecv[p, 0]
        for i in range(1, chips):
            tot = tot + morecv[p, i]
        yg[pl.ds(my_slot + p * MPR, MPR), :] = round_bf16(x32[p * MPR:(p + 1) * MPR, pl.ds(pl.multiple_of(me * LANES, LANES), LANES)] + tot)
        y_send(p)
    y_finish()
    for d in range(chips * CORES):
        for s in range(S):
            out_ref[s, :, d * LANES:(d + 1) * LANES] = yg[d * QR + s * B:d * QR + (s + 1) * B, :].astype(BF16)

    q_x.wait_send()
    k_x.wait_send()
    v_x.wait_send()
    o_x.wait_send()

    def drain(i, _):
        b = lax.rem(chip + i, chips)
        to_partner(mpsend.at[b], mprecv.at[b], ps_s.at[b], ps_r.at[b]).wait_send()

        @pl.when(i > 0)
        def _():
            for p in range(MP):
                mo_copy(b, p).wait_send()
        return 0
    lax.fori_loop(0, chips, drain, 0)
    x_drain()
    y_drain()


def copy_out(a, b, d, oa, ob, od, sem):
    cps = [pltpu.make_async_copy(x, y, sem.at[i]) for i, (x, y) in enumerate(((a, oa), (b, ob), (d, od)))]
    for cp in cps:
        cp.start()
    for cp in cps:
        cp.wait()


def finish(*arrs):
    return pl.pallas_call(
        copy_out,
        name="copy_out",
        out_shape=tuple(jax.ShapeDtypeStruct(a.shape, a.dtype) for a in arrs),
        in_specs=[pl.BlockSpec(memory_space=pltpu.VMEM)] * len(arrs),
        out_specs=(pl.BlockSpec(memory_space=pl.ANY),) * len(arrs),
        scratch_shapes=[pltpu.SemaphoreType.DMA((len(arrs),))],
        compiler_params=pltpu.CompilerParams(vmem_limit_bytes=1 << 20),
    )(*arrs)


def solution(mesh):
    n = mesh.shape["kv"]
    chips = n // CORES

    def layer_steps(x_first, next_emb, k_cache, v_cache, seq_len, ln1_gain, ln1_bias, w_q, b_q, w_k, b_k, w_v, b_v, w_o, b_o, ln2_gain, ln2_bias, w_router, w_gate, w_up, w_down, long_factor, expert_idx, route_mask):
        B, T, KH, HD = k_cache.shape
        D = x_first.shape[1]
        H = w_q.shape[1] // HD
        S = next_emb.shape[0] + 1
        E = w_router.shape[1]
        FE = w_gate.shape[0] * w_gate.shape[2]
        FEP = -(-FE // 256) * 256
        R = S * B
        HH, KHH = H // CORES, KH // CORES
        QR = S * HH
        MR = QR + 8
        if B != chips or D != n * LANES or w_q.shape[1] != D or QR != R:
            raise ValueError("unsupported sizes")
        dims = dict(S=S, B=B, D=D, T=T, KH=KH, HD=HD, H=H, E=E, FE=FE, chips=chips)
        half = HD // 2
        power = np.float32(ROPE_BASE) ** (np.arange(half, dtype=np.float32) * np.float32(2.0) / np.float32(HD))
        pw = jnp.asarray(power[None, :].astype(np.float32))
        lf = long_factor[None, :]
        row = lambda a: a.reshape(1, -1)
        args = (seq_len, expert_idx.transpose(0, 2, 1), route_mask,
                x_first, next_emb, k_cache.reshape(B, T * KH, HD), v_cache.reshape(B, T * KH, HD), row(ln1_gain), row(ln1_bias),
                w_q, row(b_q), w_k, row(b_k), w_v, row(b_v), w_o, row(b_o), row(ln2_gain), row(ln2_bias), w_router.T,
                w_gate.transpose(2, 0, 1).reshape(FE, D), w_up.transpose(2, 0, 1).reshape(FE, D), w_down.transpose(1, 0, 2).reshape(FE, D), lf, pw)
        V = pltpu.VMEM
        DS = pltpu.SemaphoreType.DMA
        scratch = [
            pltpu.SMEM((B,), jnp.int32), V(expert_idx.transpose(0, 2, 1).shape, jnp.int32), V(route_mask.shape, jnp.int32),
            V((4, D, WCOLS), BF16), V((B, T * KH, HD), BF16), V((B, T * KH, HD), BF16), V((3, FEP, D), BF16),
            V((S, B, D), BF16), V((R, D), F32), V((R, D), BF16),
            V((1, D), F32), V((1, D), F32), V((1, D), F32), V((1, D), F32), V((1, D), F32), V((1, w_q.shape[1]), F32),
            V((1, w_k.shape[1]), F32), V((1, w_v.shape[1]), F32), V((1, half), F32), V((1, half), F32), V((E, D), BF16),
            V((CORES, B * QR, HD), F32), V((R, HD), F32), V((R, HD), F32), V((CORES, KHH, R, HD), F32), V((CORES, KHH, R, HD), F32), V((2, 16, HD), F32),
            V((CORES * QR, LANES), F32), V((CORES * QR, T * KH), F32), V((CORES * QR, T * KH), F32), V((2, CORES * QR, LANES), F32),
            V((CORES, B, MR, HD), F32), V((B, MR, HD), F32), V((B, MR, HD), F32), V((chips + 1, MR, HD), F32),
            V((CORES, QR, HD), F32), V((CORES, 8, HH * HD), F32), V((4, 8, WCOLS), F32), V((n * QR, HD), F32), V((LANES, LANES), F32), V((LANES, LANES), F32), V((FEP, LANES), F32), V((R, FEP), BF16),
            V((chips, R, LANES), F32), V((chips, R, LANES), F32), V((chips, R, LANES), F32), V((2, chips, R // 2, LANES), F32), V((2, chips, R // 2, LANES), F32),
            V((n * QR, LANES), F32), V((B * S * KH, HD), F32),
            DS((10,)), DS((B,)), DS((B,)), DS((3,)), DS((16,)), DS, DS, DS, DS, DS, DS, DS((B,)), DS((B,)), DS((chips,)), DS((chips,)), DS, DS,
            DS((2,)), DS((2, 3)), DS((2,)), DS((2, chips)), DS((2, chips)), DS((2,)), DS((2, 3)), DS((2,)),
        ]
        vm = pl.BlockSpec(memory_space=pltpu.VMEM)
        anys = pl.BlockSpec(memory_space=pl.ANY)
        hidden, tk, tv = pl.pallas_call(
            functools.partial(kernel, dims),
            name="decode_layer",
            out_shape=(V((S, B, D), BF16), V((B * S * KH, HD), BF16), V((B * S * KH, HD), BF16)),
            in_specs=[anys] * len(args),
            out_specs=(vm, vm, vm),
            scratch_shapes=scratch,
            compiler_params=pltpu.CompilerParams(collective_id=0, has_side_effects=True, vmem_limit_bytes=VMEM_BYTES),
        )(*args)
        hidden, tk, tv = finish(hidden, tk, tv)
        return hidden, tk.reshape(B, S, KH, HD), tv.reshape(B, S, KH, HD)

    replicated = P()
    in_specs = (P('dp'), P(None, 'dp'), P('dp', 'kv'), P('dp', 'kv'), P('dp')) + (replicated,) * 13 + (P(None, None, 'kv'), P(None, None, 'kv'), P(None, 'kv'), replicated, P(None, 'dp'), P(None, 'dp'))
    out_specs = (P(None, 'dp'), P('dp'), P('dp'))
    return jax.shard_map(layer_steps, mesh=mesh, in_specs=in_specs, out_specs=out_specs, check_vma=False)
```
